128 devices in a mesh: model: 16 (over z, y), data: 8 (over x, core).
Axes of the slice: x: 4, y: 4, z: 4, core: 2. Of those that a mesh axis runs over, the one named last changes fastest.
Arguments:
- x_tokens: bfloat16 [16384, 2048], P('data')
- dy_tokens: bfloat16 [16384, 2048], P('data')
- w_col: bfloat16 [2, 2048, 2048], P(None, None, 'model')
- w_row: bfloat16 [2, 2048, 2048], P(None, 'model')
- a_old_col: float32 [2, 2048, 2048], replicated
- s_old_col: float32 [2, 2048, 128], P(None, 'model')
- a_old_row: float32 [2, 2048, 128], P(None, 'model')
- s_old_row: float32 [2, 2048, 2048], replicated
- a_inv_col: float32 [2, 2048, 2048], replicated
- s_inv_col: float32 [2, 2048, 128], P(None, 'model')
- a_inv_row: float32 [2, 2048, 128], P(None, 'model')
- s_inv_row: float32 [2, 2048, 2048], replicated
Outputs:
- output 1: float32 [2, 2048, 2048], P(None, None, 'model')
- output 2: float32 [2, 2048, 2048], P(None, 'model')
- output 3: float32 [2, 2048, 2048], replicated
- output 4: float32 [2, 2048, 128], P(None, 'model')
- output 5: float32 [2, 2048, 128], P(None, 'model')
- output 6: float32 [2, 2048, 2048], replicated
All inputs are finite; a program needn't handle non-finite values.
Results may differ from the reference program's by a relative error of at most 0.0075489.
Values are sent between devices in bfloat16 or wider.
A program may use at most 1 GiB of HBM per device.

```python
import math
import jax
import jax.numpy as jnp
from jax import lax

HIDDEN = 2048
TOKENS_DEV = 2048
DATA_WAYS = 8
MODEL_WAYS = 16
BATCH_ROWS = TOKENS_DEV * DATA_WAYS
BLOCK_DIM = HIDDEN // MODEL_WAYS
FACTOR_DECAY = 0.8
GELU_SCALE = math.sqrt(2.0 / math.pi)
GELU_CUBIC = 0.044715
EXACT = lax.Precision.HIGHEST


def gelu_value(pre_act):
    tanh_arg = GELU_SCALE * (pre_act + GELU_CUBIC * pre_act * pre_act * pre_act)
    return 0.5 * pre_act * (1.0 + jnp.tanh(tanh_arg))


def gelu_slope(pre_act):
    tanh_arg = GELU_SCALE * (pre_act + GELU_CUBIC * pre_act * pre_act * pre_act)
    tanh_val = jnp.tanh(tanh_arg)
    return 0.5 * (1.0 + tanh_val) + 0.5 * pre_act * (1.0 - tanh_val * tanh_val) * GELU_SCALE * (1.0 + 3.0 * GELU_CUBIC * pre_act * pre_act)


def activate(pre_act):
    return gelu_value(pre_act.astype(jnp.float32)).astype(jnp.bfloat16)


def back_gate(grad_act, pre_act):
    return (grad_act.astype(jnp.float32) * gelu_slope(pre_act.astype(jnp.float32))).astype(jnp.bfloat16)


def sym_draw(rand_key, lead_count, mat_dim, spread):
    diag_key, noise_key = jax.random.split(rand_key)
    diag_vals = jax.random.uniform(diag_key, (lead_count, mat_dim), jnp.float32, 0.5, 1.5)
    sym_noise = jax.random.normal(noise_key, (lead_count, mat_dim, mat_dim), jnp.float32)
    sym_noise = (sym_noise + jnp.swapaxes(sym_noise, 1, 2)) * (spread / math.sqrt(2.0 * mat_dim))
    return sym_noise + diag_vals[:, :, None] * jnp.eye(mat_dim, dtype=jnp.float32)


def block_draw(rand_key, spread):
    return sym_draw(rand_key, 2 * MODEL_WAYS, BLOCK_DIM, spread).reshape(2, HIDDEN, BLOCK_DIM)


def token_draw(rand_key):
    mean_key, scale_key, base_key = jax.random.split(rand_key, 3)
    shard_mean = jax.random.normal(mean_key, (DATA_WAYS, 1, HIDDEN), jnp.float32) * (0.5 * HIDDEN ** -0.25)
    shard_scale = jnp.exp2(jax.random.uniform(scale_key, (DATA_WAYS, 1, 1), jnp.float32, -1.0, 1.0))
    base_vals = jax.random.normal(base_key, (DATA_WAYS, TOKENS_DEV, HIDDEN), jnp.float32)
    return (base_vals * shard_scale + shard_mean).reshape(BATCH_ROWS, HIDDEN).astype(jnp.bfloat16)


def setup_inputs(seed: int = 0) -> dict:
    key_list = jax.random.split(jax.random.key(seed), 12)
    weight_scale = HIDDEN ** -0.5
    return {
        'x_tokens': token_draw(key_list[0]),
        'dy_tokens': token_draw(key_list[1]),
        'w_col': (jax.random.normal(key_list[2], (2, HIDDEN, HIDDEN), jnp.float32) * weight_scale).astype(jnp.bfloat16),
        'w_row': (jax.random.normal(key_list[3], (2, HIDDEN, HIDDEN), jnp.float32) * weight_scale).astype(jnp.bfloat16),
        'a_old_col': sym_draw(key_list[4], 2, HIDDEN, 0.3),
        's_old_col': block_draw(key_list[5], 0.3),
        'a_old_row': block_draw(key_list[6], 0.3),
        's_old_row': sym_draw(key_list[7], 2, HIDDEN, 0.3),
        'a_inv_col': sym_draw(key_list[8], 2, HIDDEN, 0.2),
        's_inv_col': block_draw(key_list[9], 0.2),
        'a_inv_row': block_draw(key_list[10], 0.2),
        's_inv_row': sym_draw(key_list[11], 2, HIDDEN, 0.2),
    }


def gram_mat(left_mat, right_mat):
    return jnp.dot(left_mat.T, right_mat, preferred_element_type=jnp.float32) / BATCH_ROWS


def block_gram(left_mat, right_mat):
    left_blocks = jnp.swapaxes(left_mat.reshape(BATCH_ROWS, MODEL_WAYS, BLOCK_DIM), 0, 1)
    right_blocks = jnp.swapaxes(right_mat.reshape(BATCH_ROWS, MODEL_WAYS, BLOCK_DIM), 0, 1)
    blocks = lax.map(lambda block_pair: jnp.dot(block_pair[0].T, block_pair[1], preferred_element_type=jnp.float32), (left_blocks, right_blocks))
    return blocks.reshape(HIDDEN, BLOCK_DIM) / BATCH_ROWS


def precondition_col(a_inv, grad_mat, s_inv_blocks):
    left_done = jnp.dot(a_inv, grad_mat, precision=EXACT).reshape(HIDDEN, MODEL_WAYS, BLOCK_DIM)
    right_blocks = s_inv_blocks.reshape(MODEL_WAYS, BLOCK_DIM, BLOCK_DIM)
    return jnp.einsum('dmi,mij->dmj', left_done, right_blocks, precision=EXACT).reshape(HIDDEN, HIDDEN)


def precondition_row(a_inv_blocks, grad_mat, s_inv):
    left_blocks = a_inv_blocks.reshape(MODEL_WAYS, BLOCK_DIM, BLOCK_DIM)
    left_done = jnp.einsum('mij,mjk->mik', left_blocks, grad_mat.reshape(MODEL_WAYS, BLOCK_DIM, HIDDEN), precision=EXACT).reshape(HIDDEN, HIDDEN)
    return jnp.dot(left_done, s_inv, precision=EXACT)


def blend_factor(old_mats, first_new, second_new):
    return FACTOR_DECAY * old_mats + (1.0 - FACTOR_DECAY) * jnp.stack([first_new, second_new])


def reference(x_tokens, dy_tokens, w_col, w_row, a_old_col, s_old_col, a_old_row, s_old_row, a_inv_col, s_inv_col, a_inv_row, s_inv_row):
    z_one = jnp.dot(x_tokens, w_col[0], preferred_element_type=jnp.float32).astype(jnp.bfloat16)
    h_one = activate(z_one)
    z_two = jnp.dot(h_one, w_row[0], preferred_element_type=jnp.float32).astype(jnp.bfloat16)
    h_two = activate(z_two)
    z_three = jnp.dot(h_two, w_col[1], preferred_element_type=jnp.float32).astype(jnp.bfloat16)
    h_three = activate(z_three)
    g_three = back_gate(jnp.dot(dy_tokens, w_row[1].T, preferred_element_type=jnp.float32).astype(jnp.bfloat16), z_three)
    g_two = back_gate(jnp.dot(g_three, w_col[1].T, preferred_element_type=jnp.float32).astype(jnp.bfloat16), z_two)
    g_one = back_gate(jnp.dot(g_two, w_row[0].T, preferred_element_type=jnp.float32).astype(jnp.bfloat16), z_one)
    u_col = jnp.stack([
        precondition_col(a_inv_col[0], gram_mat(x_tokens, g_one), s_inv_col[0]),
        precondition_col(a_inv_col[1], gram_mat(h_two, g_three), s_inv_col[1]),
    ])
    u_row = jnp.stack([
        precondition_row(a_inv_row[0], gram_mat(h_one, g_two), s_inv_row[0]),
        precondition_row(a_inv_row[1], gram_mat(h_three, dy_tokens), s_inv_row[1]),
    ])
    a_new_col = blend_factor(a_old_col, gram_mat(x_tokens, x_tokens), gram_mat(h_two, h_two))
    s_new_col = blend_factor(s_old_col, block_gram(g_one, g_one), block_gram(g_three, g_three))
    a_new_row = blend_factor(a_old_row, block_gram(h_one, h_one), block_gram(h_three, h_three))
    s_new_row = blend_factor(s_old_row, gram_mat(g_two, g_two), gram_mat(dy_tokens, dy_tokens))
    return (u_col, u_row, a_new_col, s_new_col, a_new_row, s_new_row)
```

```python
import functools
import math
import jax
import jax.numpy as jnp
from jax import lax
from jax.experimental import pallas as pl
from jax.experimental.pallas import tpu as pltpu
from jax.sharding import PartitionSpec as P

FACTOR_DECAY = 0.8
GELU_SCALE = math.sqrt(2.0 / math.pi)
GELU_CUBIC = 0.044715
EXACT = lax.Precision.HIGHEST
TN_DIMS = (((0,), (0,)), ((), ()))
NT_DIMS = (((1,), (1,)), ((), ()))


def gelu_value(pre_act):
    tanh_arg = GELU_SCALE * (pre_act + GELU_CUBIC * pre_act * pre_act * pre_act)
    return 0.5 * pre_act * (1.0 + jnp.tanh(tanh_arg))


def gelu_slope(pre_act):
    tanh_arg = GELU_SCALE * (pre_act + GELU_CUBIC * pre_act * pre_act * pre_act)
    tanh_val = jnp.tanh(tanh_arg)
    return 0.5 * (1.0 + tanh_val) + 0.5 * pre_act * (1.0 - tanh_val * tanh_val) * GELU_SCALE * (1.0 + 3.0 * GELU_CUBIC * pre_act * pre_act)


def activate(pre_act):
    return gelu_value(pre_act.astype(jnp.float32)).astype(jnp.bfloat16)


def back_gate(grad_act, pre_act):
    return (grad_act.astype(jnp.float32) * gelu_slope(pre_act.astype(jnp.float32))).astype(jnp.bfloat16)


def matmul(left_mat, right_mat):
    return jnp.dot(left_mat, right_mat, preferred_element_type=jnp.float32)


def matmul_tn(left_mat, right_mat):
    return lax.dot_general(left_mat, right_mat, TN_DIMS, preferred_element_type=jnp.float32)


def matmul_nt(left_mat, right_mat):
    return lax.dot_general(left_mat, right_mat, NT_DIMS, preferred_element_type=jnp.float32)


def exact_dot(left_mat, right_mat):
    return jnp.dot(left_mat, right_mat, precision=EXACT, preferred_element_type=jnp.float32)


def precondition(a_inv, grad_mat, s_inv):
    return exact_dot(exact_dot(a_inv, grad_mat), s_inv)


def blend_factor(old_mats, first_new, second_new, inv_rows):
    return FACTOR_DECAY * old_mats + (1.0 - FACTOR_DECAY) * inv_rows * jnp.stack([first_new, second_new])


MESH = pl.DeviceIdType.MESH
SIDE = 4
PLANE = 16


def plane_peer(model_id, z_step, y_step):
    z_pos, y_pos = lax.rem(lax.div(model_id, SIDE) + z_step + SIDE, SIDE), lax.rem(lax.rem(model_id, SIDE) + y_step + SIDE, SIDE)
    return z_pos * SIDE + y_pos


class Copies:
    def __init__(self, send_sems, recv_sems):
        self.send_sems, self.recv_sems = send_sems, recv_sems
        self.index, self.sent = {}, []

    def slot(self, name):
        return self.index.setdefault(name, len(self.index))

    def make(self, name, src, dst, device):
        num = self.slot(name)
        return pltpu.make_async_remote_copy(src_ref=src, dst_ref=dst, send_sem=self.send_sems.at[num], recv_sem=self.recv_sems.at[num], device_id=device, device_id_type=MESH)

    def start(self, name, src, dst, device):
        copy = self.make(name, src, dst, device)
        copy.start()
        self.sent.append(copy)

    def wait(self, name, dst, device):
        self.make(name, dst, dst, device).wait_recv()

    def finish(self):
        for copy in self.sent:
            copy.wait_send()
        self.sent = []


def greet(devices):
    barrier = pltpu.get_barrier_semaphore()
    for device in devices:
        pl.semaphore_signal(barrier, inc=1, device_id=device, device_id_type=MESH)
    pl.semaphore_wait(barrier, len(devices))


def plane_gather(copies, tag, region, on_piece=None):
    model_id = lax.axis_index('model')

    def peer(order, first, second):
        return plane_peer(model_id, second, first) if order == 0 else plane_peer(model_id, first, second)

    def dev(order, first, second):
        return {'model': peer(order, first, second)}

    def send(order, name, owner, part, first, second):
        ref = region(owner, order, *part)
        copies.start((tag, order) + name, ref, ref, dev(order, first, second))

    def recv(order, name, owner, part):
        copies.wait((tag, order) + name, region(owner, order, *part), dev(order, 0, 1))

    whole, low, high = (0, 2), (0, 1), (1, 2)

    def spread(order, k):
        owner = peer(order, k, 0)
        send(order, ('b', k, -1), owner, whole, 0, 1)
        send(order, ('b', k, 1), owner, whole, 0, -1)

    def done(order, first, second):
        if on_piece is not None:
            on_piece(peer(order, first, second), order, (first, second))

    for order in (0, 1):
        owner = peer(order, 0, 0)
        send(order, ('a', -1), owner, whole, 1, 0)
        send(order, ('a', 1), owner, whole, -1, 0)
    for order in (0, 1):
        spread(order, 0)
    yield
    for order in (0, 1):
        for step, part in ((-1, low), (1, high)):
            owner = peer(order, step, 0)
            recv(order, ('a', step), owner, whole)
            send(order, ('a', 2 * step), owner, part, -step, 0)
            spread(order, step)
            done(order, step, 0)
        yield
    def pass_on(order, k):
        for step, part in ((-1, low), (1, high)):
            owner = peer(order, k, step)
            recv(order, ('b', k, step), owner, whole)
            send(order, ('b', k, 2 * step), owner, part, 0, -step)
            done(order, k, step)
    for order in (0, 1):
        pass_on(order, 0)
        yield
    for order in (0, 1):
        owner = peer(order, 2, 0)
        recv(order, ('a', -2), owner, low)
        recv(order, ('a', 2), owner, high)
        spread(order, 2)
        done(order, 2, 0)
        yield
    for k in (-1, 1, 2):
        for order in (0, 1):
            pass_on(order, k)
            yield
    for k in (0, -1, 1, 2):
        for order in (0, 1):
            owner = peer(order, k, 2)
            recv(order, ('b', k, -2), owner, low)
            recv(order, ('b', k, 2), owner, high)
            done(order, k, 2)
        yield


def neighbours():
    model_id = lax.axis_index('model')
    return [{'model': plane_peer(model_id, a, b)} for a, b in ((0, 1), (0, -1), (1, 0), (-1, 0))]


def partner():
    data_id = lax.axis_index('data')
    return {'data': data_id + 1 - 2 * lax.rem(data_id, 2)}


def gather_rows_kernel(rows, piece_ref, out_ref, local_sem, send_sems, recv_sems):
    model_id = lax.axis_index('model')
    copies = Copies(send_sems, recv_sems)
    out_ref[pl.ds(pl.multiple_of(model_id * rows, rows), rows), :] = piece_ref[...]
    greet(neighbours())

    def region(owner, order, lo, hi):
        start = owner * rows + order * (rows // 2) + lo * (rows // 4)
        return out_ref.at[pl.ds(pl.multiple_of(start, rows // 4), (hi - lo) * (rows // 4)), :]

    for _ in plane_gather(copies, 'g', region):
        pass
    copies.finish()


def gather_rows(piece, collective_id):
    rows, width = piece.shape
    return pl.pallas_call(
        functools.partial(gather_rows_kernel, rows),
        out_shape=jax.ShapeDtypeStruct((PLANE * rows, width), piece.dtype),
        in_specs=[pl.BlockSpec(memory_space=pltpu.VMEM)],
        out_specs=pl.BlockSpec(memory_space=pltpu.VMEM),
        scratch_shapes=[pltpu.SemaphoreType.DMA, pltpu.SemaphoreType.DMA((40,)), pltpu.SemaphoreType.DMA((40,))],
        compiler_params=pltpu.CompilerParams(collective_id=collective_id, has_side_effects=True),
    )(piece)


def gather_shared_kernel(rows, piece_ref, out_ref, send_sems, recv_sems):
    model_id = lax.axis_index('model')
    core = lax.rem(lax.axis_index('data'), 2)
    copies = Copies(send_sems, recv_sems)
    mate = partner()
    out_ref[pl.ds(pl.multiple_of(model_id * rows, rows), rows), :] = piece_ref[...]
    greet(neighbours() + [mate])
    half = rows // 2

    def region_of(which, owner, order, lo, hi):
        start = owner * rows + which * half + order * (half // 2) + lo * (half // 4)
        return out_ref.at[pl.ds(pl.multiple_of(start, half // 4), (hi - lo) * (half // 4)), :]

    handed = []
    def hand(owner, order, key):
        ref = region_of(core, owner, order, 0, 2)
        copies.start(('mate', order) + key, ref, ref, mate)
        handed.append((owner, order, key))

    for _ in plane_gather(copies, 'g', functools.partial(region_of, core), hand):
        pass
    for owner, order, key in handed:
        copies.wait(('mate', order) + key, region_of(1 - core, owner, order, 0, 2), mate)
    copies.finish()


def gather_shared(piece, collective_id):
    rows, width = piece.shape
    return pl.pallas_call(
        functools.partial(gather_shared_kernel, rows),
        out_shape=jax.ShapeDtypeStruct((PLANE * rows, width), piece.dtype),
        in_specs=[pl.BlockSpec(memory_space=pltpu.VMEM)],
        out_specs=pl.BlockSpec(memory_space=pltpu.VMEM),
        scratch_shapes=[pltpu.SemaphoreType.DMA((70,)), pltpu.SemaphoreType.DMA((70,))],
        compiler_params=pltpu.CompilerParams(collective_id=collective_id, has_side_effects=True),
    )(piece)


STEPS = [(a, b) for a in range(4) for b in range(4) if (a, b) != (0, 0)]


def swap_kernel(cols_ref, out_ref, send_sems, recv_sems):
    model_id = lax.axis_index('model')
    rows, width = out_ref.shape[0], cols_ref.shape[1]
    copies = Copies(send_sems, recv_sems)
    greet([{'model': plane_peer(model_id, a, b)} for a, b in STEPS])
    mine = pl.ds(pl.multiple_of(model_id * width, width), width)
    for a, b in STEPS:
        peer = plane_peer(model_id, a, b)
        copies.start((a, b), cols_ref.at[pl.ds(pl.multiple_of(peer * rows, rows), rows), :], out_ref.at[:, mine], {'model': peer})
    out_ref[:, mine] = cols_ref[pl.ds(pl.multiple_of(model_id * rows, rows), rows), :]
    for a, b in STEPS:
        peer = plane_peer(model_id, -a, -b)
        copies.wait((a, b), out_ref.at[:, pl.ds(pl.multiple_of(peer * width, width), width)], {'model': peer})
    copies.finish()


def swap(cols, collective_id):
    rows, width = cols.shape[0] // PLANE, cols.shape[1]
    return pl.pallas_call(
        swap_kernel,
        out_shape=jax.ShapeDtypeStruct((rows, PLANE * width), cols.dtype),
        in_specs=[pl.BlockSpec(memory_space=pltpu.VMEM)],
        out_specs=pl.BlockSpec(memory_space=pltpu.VMEM),
        scratch_shapes=[pltpu.SemaphoreType.DMA((15,)), pltpu.SemaphoreType.DMA((15,))],
        compiler_params=pltpu.CompilerParams(collective_id=collective_id, has_side_effects=True),
    )(cols)


def split_factor(left_cols, right_mat):
    return matmul_tn(left_cols, right_mat)


def solution(mesh):
    data_ways = mesh.shape['data']
    model_ways = mesh.shape['model']

    def shard_body(x_tokens, dy_tokens, w_col, w_row, a_old_col, s_old_col, a_old_row, s_old_row, a_inv_col, s_inv_col, a_inv_row, s_inv_row):
        model_id = lax.axis_index('model')
        data_id = lax.axis_index('data')
        width = x_tokens.shape[1]
        block = width // model_ways
        piece = block // data_ways
        inv_rows = 1.0 / (x_tokens.shape[0] * data_ways)

        def own_cols(mat):
            return lax.dynamic_slice_in_dim(mat, model_id * block, block, axis=1)

        def new_factor(local_rows, old_mat):
            total = lax.psum_scatter(local_rows, 'data', scatter_dimension=0, tiled=True)
            old_rows = lax.dynamic_slice_in_dim(old_mat, model_id * block + data_id * piece, piece, axis=0)
            mixed = FACTOR_DECAY * old_rows + (1.0 - FACTOR_DECAY) * inv_rows * total
            return lax.all_gather(mixed, ('model', 'data'), axis=0, tiled=True)

        z_one = matmul(x_tokens, w_col[0]).astype(jnp.bfloat16)
        h_one = activate(z_one)
        h_one_rows = swap(h_one, 0)
        w_two = gather_shared(w_row[0], 1)
        w_three_t = gather_shared(w_col[1].T, 2)
        z_two_rows = matmul(h_one_rows, w_two).astype(jnp.bfloat16)
        h_two = gather_rows(activate(z_two_rows), 3)
        z_three = matmul(h_two, w_col[1]).astype(jnp.bfloat16)
        h_three = activate(z_three)
        g_three = back_gate(matmul_nt(dy_tokens, w_row[1]).astype(jnp.bfloat16), z_three)
        dh_two_rows = matmul(swap(g_three, 4), w_three_t).astype(jnp.bfloat16)
        g_two = gather_rows(back_gate(dh_two_rows, z_two_rows), 5)
        g_one = back_gate(matmul_nt(g_two, w_row[0]).astype(jnp.bfloat16), z_one)

        a_new_col = jnp.stack([
            new_factor(split_factor(own_cols(x_tokens), x_tokens), a_old_col[0]),
            new_factor(split_factor(own_cols(h_two), h_two), a_old_col[1]),
        ])
        s_new_row = jnp.stack([
            new_factor(split_factor(own_cols(g_two), g_two), s_old_row[0]),
            new_factor(split_factor(own_cols(dy_tokens), dy_tokens), s_old_row[1]),
        ])
        small = lax.psum(jnp.stack([matmul_tn(mat, mat) for mat in (g_one, g_three, h_one, h_three)]), 'data')
        s_new_col = blend_factor(s_old_col, small[0], small[1], inv_rows)
        a_new_row = blend_factor(a_old_row, small[2], small[3], inv_rows)

        grads = [matmul_tn(x_tokens, g_one), matmul_tn(h_one, g_two), matmul_tn(h_two, g_three), matmul_tn(h_three, dy_tokens)]
        grads = [lax.psum(grad, 'data') * inv_rows for grad in grads]
        u_col = jnp.stack([precondition(a_inv_col[0], grads[0], s_inv_col[0]), precondition(a_inv_col[1], grads[2], s_inv_col[1])])
        u_row = jnp.stack([precondition(a_inv_row[0], grads[1], s_inv_row[0]), precondition(a_inv_row[1], grads[3], s_inv_row[1])])
        return (u_col, u_row, a_new_col, s_new_col, a_new_row, s_new_row)

    batch_split = P('data', None)
    col_split = P(None, None, 'model')
    row_split = P(None, 'model', None)
    replicated = P()
    return jax.shard_map(
        shard_body,
        mesh=mesh,
        in_specs=(batch_split, batch_split, col_split, row_split, replicated, row_split, row_split, replicated, replicated, row_split, row_split, replicated),
        out_specs=(col_split, row_split, replicated, row_split, row_split, replicated),
        check_vma=False,
    )
```

```python
import functools
import math
import jax
import jax.numpy as jnp
from jax import lax
from jax.experimental import pallas as pl
from jax.experimental.pallas import tpu as pltpu
from jax.sharding import PartitionSpec as P

FACTOR_DECAY = 0.8
GELU_SCALE = math.sqrt(2.0 / math.pi)
GELU_CUBIC = 0.044715
EXACT = lax.Precision.HIGHEST
MESH = pl.DeviceIdType.MESH
SIDE = 4
PLANE = 16
DATA_WAYS = 8
WIDTH = 2048
BLOCK = 128
PIECE = 16
TRI = 9
PARTS = 3
PART_COLS = TRI * BLOCK // PARTS
GRAD_COLS = WIDTH + BLOCK
NT_DIMS = (((1,), (1,)), ((), ()))


def gelu_value(pre_act):
    tanh_arg = GELU_SCALE * (pre_act + GELU_CUBIC * pre_act * pre_act * pre_act)
    return 0.5 * pre_act * (1.0 + jnp.tanh(tanh_arg))


def gelu_slope(pre_act):
    tanh_arg = GELU_SCALE * (pre_act + GELU_CUBIC * pre_act * pre_act * pre_act)
    tanh_val = jnp.tanh(tanh_arg)
    return 0.5 * (1.0 + tanh_val) + 0.5 * pre_act * (1.0 - tanh_val * tanh_val) * GELU_SCALE * (1.0 + 3.0 * GELU_CUBIC * pre_act * pre_act)


def activate(pre_act):
    return gelu_value(pre_act.astype(jnp.float32)).astype(jnp.bfloat16)


def back_gate(grad_act, pre_act):
    return (grad_act.astype(jnp.float32) * gelu_slope(pre_act.astype(jnp.float32))).astype(jnp.bfloat16)


def matmul(left_mat, right_mat):
    return jnp.dot(left_mat, right_mat, preferred_element_type=jnp.float32)


def matmul_nt(left_mat, right_mat):
    return lax.dot_general(left_mat, right_mat, NT_DIMS, preferred_element_type=jnp.float32)


def exact_dot(left_mat, right_mat):
    return jnp.dot(left_mat, right_mat, precision=EXACT, preferred_element_type=jnp.float32)


def span_of(index, size):
    return pl.ds(pl.multiple_of(index * size, size), size)


class Place:
    def __init__(self):
        self.model, self.data = lax.axis_index('model'), lax.axis_index('data')
        self.core = lax.rem(self.data, 2)
        here = {'x': lax.div(self.data, 2), 'y': lax.rem(self.model, SIDE), 'z': lax.div(self.model, SIDE)}
        self.along = {dim: [at] + [lax.rem(at + step, SIDE) for step in range(1, SIDE)] for dim, at in here.items()}
        self.planes = [[z * SIDE + y for y in self.along['y']] for z in self.along['z']]
        self.lines = [x * 2 + self.core for x in self.along['x']]
        self.mate = (self.model, self.data + 1 - 2 * self.core)

    def at(self, dim, step):
        return self.along[dim][step % SIDE]

    def peer(self, z_step, y_step):
        return self.planes[z_step % SIDE][y_step % SIDE]

    def device(self, dim, step):
        if dim == 'x':
            return (self.model, self.lines[step % SIDE])
        return (self.peer(step, 0) if dim == 'z' else self.peer(0, step), self.data)


class Copies:
    def __init__(self, send_sems, recv_sems):
        self.send_sems, self.recv_sems = send_sems, recv_sems
        self.names, self.batches = {}, {}

    def start(self, batch, name, src, dst, device):
        num = self.names.setdefault((batch, name), len(self.names))
        out = self.batches.setdefault(batch, len(self.batches))
        pltpu.make_async_remote_copy(src_ref=src, dst_ref=dst, send_sem=self.send_sems.at[out], recv_sem=self.recv_sems.at[num], device_id=device, device_id_type=MESH).start()

    def wait(self, batch, name, ref):
        num = self.names.setdefault((batch, name), len(self.names))
        pltpu.make_async_copy(ref, ref, self.recv_sems.at[num]).wait()

    def left(self, batch, ref):
        pltpu.make_async_copy(ref, ref, self.send_sems.at[self.batches[batch]]).wait()


def greet(devices):
    barrier = pltpu.get_barrier_semaphore()
    for device in devices:
        pl.semaphore_signal(barrier, inc=1, device_id=device, device_id_type=MESH)
    pl.semaphore_wait(barrier, len(devices))


def plane_gather(copies, batch, place, region, own, on_piece):
    def steps(order, first, second):
        return (second, first) if order == 0 else (first, second)

    def send(order, name, k, part, first, second, src=None):
        ref = region(place.peer(*steps(order, *k)), order, *part)
        copies.start(batch, (order,) + name, ref if src is None else src, ref, (place.peer(*steps(order, first, second)), place.data))

    def recv(order, name, k, part):
        copies.wait(batch, (order,) + name, region(place.peer(*steps(order, *k)), order, *part))

    whole, low, high = (0, 2), (0, 1), (1, 2)

    def spread(order, k, src=None):
        for step in (1, -1):
            send(order, ('b', k, -step), (k, 0), whole, 0, step, src)

    def pass_on(order, k):
        for step, part in ((-1, low), (1, high)):
            recv(order, ('b', k, step), (k, step), whole)
            send(order, ('b', k, 2 * step), (k, step), part, 0, -step)
            on_piece(order, *steps(order, k, step))

    for order in (0, 1):
        for step in (1, -1):
            send(order, ('a', -step), (0, 0), whole, step, 0, own(order))
    for order in (0, 1):
        spread(order, 0, own(order))
    yield
    for order in (0, 1):
        for step, part in ((-1, low), (1, high)):
            recv(order, ('a', step), (step, 0), whole)
            send(order, ('a', 2 * step), (step, 0), part, -step, 0)
            spread(order, step)
            on_piece(order, *steps(order, step, 0))
        yield
    for order in (0, 1):
        pass_on(order, 0)
        yield
    for order in (0, 1):
        recv(order, ('a', -2), (2, 0), low)
        recv(order, ('a', 2), (2, 0), high)
        spread(order, 2)
        on_piece(order, *steps(order, 2, 0))
        yield
    for k in (-1, 1, 2):
        for order in (0, 1):
            pass_on(order, k)
            yield
    for k in (0, -1, 1, 2):
        for order in (0, 1):
            recv(order, ('b', k, -2), (k, 2), low)
            recv(order, ('b', k, 2), (k, 2), high)
            on_piece(order, *steps(order, k, 2))
        yield


STEPS = [(a, b) for a in range(SIDE) for b in range(SIDE) if (a, b) != (0, 0)]


def line_reduce(copies, batch, place, src, near, far, store):
    core = place.core
    copies.start((batch, 'near'), 0, src.at[:, 1 - core], near, place.mate)
    yield
    copies.wait((batch, 'near'), 0, near)
    for step in (2, 1, 3):
        there = place.at('x', step)
        near[there] = near[there] + src[there, core]
        copies.start((batch, 'far'), step, near.at[there], far.at[step - 1], place.device('x', step))
    here = place.at('x', 0)
    near[here] = near[here] + src[here, core]
    yield
    for step in (1, 3, 2):
        copies.wait((batch, 'far'), step, far.at[step - 1])
    store(near[here] + far[0] + far[1] + far[2])
    copies.left((batch, 'near'), near)
    copies.left((batch, 'far'), far)
    yield


def line_gather(copies, batch, place, out):
    core = place.core
    mine = out.at[place.at('x', 0), core]
    for step in (2, 1, 3):
        copies.start((batch, 'all'), step, mine, mine, place.device('x', step))
    copies.start((batch, 'hand'), 0, mine, mine, place.mate)
    yield
    for step in (1, 3, 2):
        theirs = out.at[place.at('x', -step), core]
        copies.wait((batch, 'all'), step, theirs)
        copies.start((batch, 'hand'), 0, theirs, theirs, place.mate)
    yield
    copies.wait((batch, 'hand'), 0, out.at[:, 0])
    copies.left((batch, 'all'), out.at[0:3, 0])
    copies.left((batch, 'hand'), out.at[:, 0])
    yield


BALANCED = (('x', 'y', 'z'), ('y', 'z', 'x'), ('z', 'x', 'y'))
X_LAST = (('y', 'z', 'x'), ('z', 'y', 'x'), ('y', 'z', 'x'))


def cube_gather(copies, batch, place, view, order):
    first, second, third = order
    core = place.core

    def at(which, places):
        return view(which, places['z'], places['y'], places['x'])

    def single(step):
        return at(core, {first: place.at(first, step), second: place.at(second, 0), third: place.at(third, 0)})

    def group(a, b, span=(0, SIDE)):
        return at(core, {first: pl.ds(*span), second: place.at(second, a), third: place.at(third, b)})

    low, high = (0, 2), (2, 2)

    def hand(a, b):
        ref = group(a, b)
        copies.start((batch, 'mate'), 0, ref, ref, place.mate)

    def spread(a):
        ref = group(a, 0)
        for step in (1, -1):
            copies.start((batch, 'three'), (a, -step), ref, ref, place.device(third, step))
        hand(a, 0)

    def pass_on(a):
        for step, span in ((-1, low), (1, high)):
            copies.wait((batch, 'three'), (a, step), group(a, step))
            half = group(a, step, span)
            copies.start((batch, 'three'), (a, 2 * step), half, half, place.device(third, -step))
            hand(a, step)

    for step in (2, 1, -1):
        copies.start((batch, 'one'), -step % SIDE, single(0), single(0), place.device(first, step))
    yield
    for step in (1, 3, 2):
        copies.wait((batch, 'one'), step, single(step))
    for step in (1, -1):
        copies.start((batch, 'two'), -step, group(0, 0), group(0, 0), place.device(second, step))
    spread(0)
    yield
    for step, span in ((-1, low), (1, high)):
        copies.wait((batch, 'two'), step, group(step, 0))
        half = group(step, 0, span)
        copies.start((batch, 'two'), 2 * step, half, half, place.device(second, -step))
        spread(step)
    yield
    pass_on(0)
    yield
    for step, span in ((-1, low), (1, high)):
        copies.wait((batch, 'two'), 2 * step, group(2, 0, span))
    spread(2)
    yield
    for a in (-1, 1, 2):
        pass_on(a)
        yield
    for a in (0, -1, 1, 2):
        for step, span in ((-1, low), (1, high)):
            copies.wait((batch, 'three'), (a, 2 * step), group(a, 2, span))
        hand(a, 2)
        yield
    whole = pl.ds(0, SIDE)
    copies.wait((batch, 'mate'), 0, view(0, whole, whole, whole))
    copies.left((batch, 'mate'), view(0, whole, whole, whole))
    copies.left((batch, 'one'), view(0, 0, 0, pl.ds(0, 3)))
    copies.left((batch, 'two'), view(0, 0, pl.ds(0, 3), whole))
    copies.left((batch, 'three'), view(0, pl.ds(0, 3), whole, whole))
    yield


def interleave(*gens):
    gens = list(gens)
    while gens:
        for gen in list(gens):
            try:
                next(gen)
            except StopIteration:
                gens.remove(gen)
        yield


def pump(gen, count=1):
    for _ in range(count):
        next(gen, None)


def drain(gen):
    for _ in gen:
        pass


def step_kernel(scale, x_hbm, dy_hbm, w_col, w_row, a_old, s_old, fact, grads, x_buf, dy_buf, w_two, h_two, w_three, z_one, h_one, h_three,
                g_three, g_one, t_three, rows_buf, z_two, left, w_three_t, gram_src, gram_near, gram_far, old_buf, piece_buf, grad_src, grad_near,
                grad_far, load_sems, old_sems, send_sems, recv_sems):
    place = Place()
    model_id, data_id, core = place.model, place.data, place.core
    spot, y_pos, z_pos = place.at('x', 0), place.at('y', 0), place.at('z', 0)
    copies = Copies(send_sems, recv_sems)
    my_rows = span_of(model_id, BLOCK)
    my_cols = span_of(model_id, BLOCK)
    olds = [a_old.at[0], s_old.at[1], a_old.at[1], s_old.at[0]]
    chunk = 256
    n_chunks = WIDTH // chunk

    def load(src, dst, base, i):
        rows = span_of(i, chunk)
        return pltpu.make_async_copy(src.at[rows, :], dst.at[rows, :], load_sems.at[base + i])

    def load_x(i):
        return load(x_hbm, x_buf, 0, i)

    def load_dy(i):
        return load(dy_hbm, dy_buf, n_chunks, i)

    def load_old(mat, j):
        rows = pl.ds(pl.multiple_of(model_id * BLOCK + data_id * PIECE, PIECE), PIECE)
        cols = span_of(lax.rem(model_id + j, PLANE), BLOCK)
        return pltpu.make_async_copy(olds[mat].at[rows, cols], old_buf.at[mat, :, pl.ds(j * BLOCK, BLOCK)], old_sems.at[mat * TRI + j])

    for i in range(n_chunks):
        load_x(i).start()
    for i in range(n_chunks):
        load_dy(i).start()
    for mat in range(4):
        for j in range(TRI):
            load_old(mat, j).start()

    greet([(place.peer(a, b), data_id) for a, b in STEPS] + [place.mate] + [place.device('x', step) for step in (1, 2, 3)])

    half = BLOCK // 2

    def w_two_rows(which, owner, order, lo, hi):
        start = owner * BLOCK + which * half + order * (half // 2) + lo * (half // 4)
        return w_two.at[pl.ds(pl.multiple_of(start, half // 4), (hi - lo) * (half // 4)), :]

    def own_w_two(order):
        start = core * half + order * (half // 2)
        return w_row.at[0, pl.ds(pl.multiple_of(start, half // 2), half // 2), :]

    def hand(order, a, b):
        ref = w_two_rows(core, place.peer(a, b), order, 0, 2)
        copies.start('w2mate', 0, ref, ref, place.mate)

    w_two_gen = plane_gather(copies, 'w2', place, functools.partial(w_two_rows, core), own_w_two, hand)
    pump(w_two_gen)
    w_two[my_rows, :] = w_row[0]

    def z_one_step(i, carry):
        rows = span_of(i, chunk)
        load_x(i).wait()
        pre_act = matmul(x_buf[rows, :], w_col[0]).astype(jnp.bfloat16)
        z_one[rows, :] = pre_act
        h_one[rows, :] = activate(pre_act)
        return carry

    lax.fori_loop(0, n_chunks // 2, z_one_step, 0)
    pump(w_two_gen, 2)
    lax.fori_loop(n_chunks // 2, n_chunks, z_one_step, 0)

    def send_block(batch, cols_ref, a, b):
        peer = place.peer(a, b)
        copies.start(batch, 0, cols_ref.at[span_of(peer, BLOCK), :], rows_buf.at[:, my_cols], (peer, data_id))

    def wait_blocks(batch):
        others = rows_buf.at[:, 0:WIDTH - BLOCK]
        copies.wait(batch, 0, others)
        copies.left(batch, others)

    for a, b in STEPS:
        send_block('h1', h_one, a, b)
    rows_buf[:, my_cols] = h_one[my_rows, :]
    pump(w_two_gen, 2)

    w_three_t[...] = w_col[1].T

    def t_three_step(i, carry):
        rows = span_of(i, chunk)
        load_dy(i).wait()
        t_three[rows, :] = matmul_nt(dy_buf[rows, :], w_row[1]).astype(jnp.bfloat16)
        return carry

    lax.fori_loop(0, n_chunks // 2, t_three_step, 0)
    pump(w_two_gen)
    lax.fori_loop(n_chunks // 2, n_chunks, t_three_step, 0)
    pump(w_two_gen)

    def turn(dst, src, cols):
        for i in range(4):
            dst[:, i * 512:(i + 1) * 512] = src[i * 512:(i + 1) * 512, cols].T

    def gram_product(src, lhs, right, slot):
        def gram_step(j, carry):
            cols = span_of(lax.rem(model_id + j, PLANE), BLOCK)
            block = matmul(lhs[...], right[:, cols])
            src[:, :, slot * PIECE:(slot + 1) * PIECE, span_of(j, BLOCK)] = block.reshape(SIDE, 2, PIECE, BLOCK)
            return carry
        lax.fori_loop(0, TRI, gram_step, 0)

    def grad_product(lhs, right, same, slot):
        def grad_step(i, carry):
            cols = span_of(i, chunk)
            block = matmul(lhs[...], right[:, cols])
            grad_src[:, :, slot * PIECE:(slot + 1) * PIECE, cols] = block.reshape(SIDE, 2, PIECE, chunk)
            return carry
        lax.fori_loop(0, n_chunks, grad_step, 0)
        block = matmul(lhs[...], same[...])
        grad_src[:, :, slot * PIECE:(slot + 1) * PIECE, WIDTH:GRAD_COLS] = block.reshape(SIDE, 2, PIECE, BLOCK)

    turn(left.at[0], x_buf, my_cols)
    gram_product(gram_src.at[0], left.at[0], x_buf, 0)
    pump(w_two_gen, 2)
    turn(left.at[1], dy_buf, my_cols)
    gram_product(gram_src.at[0], left.at[1], dy_buf, 1)
    pump(w_two_gen, 2)

    def store_factors(pair, total):
        for num in range(2):
            mat = 2 * pair + num
            for j in range(TRI):
                load_old(mat, j).wait()
            mixed = FACTOR_DECAY * old_buf[mat] + scale * total[num * PIECE:(num + 1) * PIECE]
            for part in range(PARTS):
                piece_buf[pair, part, num] = mixed[:, part * PART_COLS:(part + 1) * PART_COLS]
        moves = [pltpu.make_async_copy(piece_buf.at[pair, part], fact.at[core, z_pos, y_pos, spot, part, pl.ds(2 * pair, 2)], old_sems.at[4 * TRI + part]) for part in range(PARTS)]
        for move in moves:
            move.start()
        for move in moves:
            move.wait()

    def factor_thread(pair, orders):
        yield from line_reduce(copies, ('gram', pair), place, gram_src.at[pair], gram_near.at[pair], gram_far.at[pair], functools.partial(store_factors, pair))
        def view(part, which, z, y, x):
            return fact.at[which, z, y, x, part, pl.ds(2 * pair, 2)]
        yield from interleave(*[cube_gather(copies, ('fact', pair, part), place, functools.partial(view, part), orders[part]) for part in range(PARTS)])

    def w_three_view(part, which, z, y, x):
        return w_three.at[z, y, x, which, :, pl.ds(part * 1024, 1024)]

    w_three[z_pos, y_pos, spot, core] = w_three_t[pl.ds(pl.multiple_of(data_id * PIECE, PIECE), PIECE), :]
    w_three_gen = interleave(*[cube_gather(copies, ('w3', part), place, functools.partial(w_three_view, part), X_LAST[part]) for part in range(2)])
    first_pair = factor_thread(0, X_LAST)
    pump(first_pair)
    pump(w_three_gen)
    pump(w_two_gen, 2)
    pump(first_pair)
    pump(w_three_gen)
    drain(w_two_gen)
    others = w_two.at[0:WIDTH - BLOCK, :]
    copies.wait('w2mate', 0, others.at[0:(WIDTH - BLOCK) // 2, :])
    copies.left('w2mate', others.at[0:(WIDTH - BLOCK) // 2, :])
    copies.left('w2', others.at[0:(WIDTH - BLOCK) // 2, :])
    wait_blocks('h1')

    def z_two_step(i, carry):
        cols = span_of(i, chunk)
        pre_act = matmul(rows_buf[...], w_two[:, cols]).astype(jnp.bfloat16)
        z_two[:, cols] = pre_act
        h_two[my_rows, cols] = activate(pre_act)
        return carry

    lax.fori_loop(0, n_chunks, z_two_step, 0)

    def token_rows(buf):
        def region(owner, order, lo, hi):
            start = owner * BLOCK + order * (BLOCK // 2) + lo * (BLOCK // 4)
            return buf.at[pl.ds(pl.multiple_of(start, BLOCK // 4), (hi - lo) * (BLOCK // 4)), :]
        return region, lambda order: region(model_id, order, 0, 2)

    def forward_block(a, b):
        rows = span_of(place.peer(a, b), BLOCK)
        pre_act = matmul(h_two[rows, :], w_col[1]).astype(jnp.bfloat16)
        h_three[rows, :] = activate(pre_act)
        g_three[rows, :] = back_gate(t_three[rows, :], pre_act)
        if (a, b) != (0, 0):
            send_block('g3', g_three, a, b)

    def backward_block(a, b):
        rows = span_of(place.peer(a, b), BLOCK)
        grad = matmul_nt(w_two[rows, :], w_row[0]).astype(jnp.bfloat16)
        g_one[rows, :] = back_gate(grad, z_one[rows, :])

    def gather_tokens(tag, buf, block_step, fill):
        seen = {}

        def on_piece(order, first, second):
            where = (first % SIDE, second % SIDE)
            seen[where] = seen.get(where, 0) + 1

        region, own = token_rows(buf)
        done = {(0, 0)}
        gen = plane_gather(copies, tag, place, region, own, on_piece)
        next(gen)
        block_step(0, 0)
        for num, _ in enumerate(gen):
            for where in sorted(seen):
                if seen[where] == 2 and where not in done:
                    done.add(where)
                    block_step(*where)
            fill(num)
        copies.left(tag, buf.at[0:WIDTH - BLOCK, :])

    def fill_forward(num):
        pump(first_pair)
        pump(w_three_gen)

    gather_tokens('h2', h_two, forward_block, fill_forward)
    drain(w_three_gen)
    wait_blocks('g3')
    rows_buf[:, my_cols] = g_three[my_rows, :]

    def g_two_step(i, carry):
        cols = span_of(i, chunk)
        weights = w_three[:, :, :, :, :, cols].reshape(WIDTH, chunk)
        grad = matmul(rows_buf[...], weights).astype(jnp.bfloat16)
        w_two[my_rows, cols] = back_gate(grad, z_two[:, cols])
        return carry

    lax.fori_loop(0, n_chunks, g_two_step, 0)

    def store_grads(batch, total):
        grads[batch, spot, core] = total

    def grad_thread(batch):
        yield from line_reduce(copies, ('grad', batch), place, grad_src, grad_near, grad_far, functools.partial(store_grads, batch))
        yield from line_gather(copies, ('grad', batch), place, grads.at[batch])

    def third_grad():
        turn(left.at[0], g_three, slice(0, BLOCK))
        grad_product(left.at[0], h_two, g_three, 0)

    def fourth_grad():
        turn(left.at[1], h_three, slice(0, BLOCK))
        grad_product(left.at[1], dy_buf, h_three, 1)

    def third_gram():
        turn(left.at[0], h_two, my_cols)
        gram_product(gram_src.at[1], left.at[0], h_two, 0)

    late = grad_thread(0)
    work = {0: third_grad, 1: fourth_grad, 2: lambda: pump(late), 3: third_gram, 5: lambda: pump(late), 7: lambda: pump(late), 9: lambda: pump(late), 11: lambda: pump(late), 13: lambda: pump(late)}

    def fill_backward(num):
        work.get(num, lambda: None)()
        pump(first_pair)

    gather_tokens('g2', w_two, backward_block, fill_backward)
    drain(late)
    turn(left.at[0], w_two, my_cols)
    gram_product(gram_src.at[1], left.at[0], w_two, 1)
    second_pair = factor_thread(1, BALANCED)
    pump(second_pair)
    turn(left.at[1], g_one, slice(0, BLOCK))
    grad_product(left.at[1], x_buf, g_one, 0)
    pump(second_pair)
    turn(left.at[0], h_one, slice(0, BLOCK))
    grad_product(left.at[0], w_two, h_one, 1)
    late = grad_thread(1)
    pump(late)
    pump(second_pair)
    pump(late)
    drain(first_pair)
    drain(interleave(late, second_pair))


def step_call(x_tokens, dy_tokens, w_col, w_row, a_old, s_old, scale):
    f32, bf16 = jnp.float32, jnp.bfloat16
    tall, wide = (WIDTH, BLOCK), (BLOCK, WIDTH)
    rows = 2 * PIECE
    vmem = pl.BlockSpec(memory_space=pltpu.VMEM)
    hbm = pl.BlockSpec(memory_space=pl.ANY)
    scratch = [pltpu.VMEM((WIDTH, WIDTH), bf16)] * 4 + [pltpu.VMEM((SIDE, SIDE, SIDE, 2, PIECE, WIDTH), bf16)]
    scratch += [pltpu.VMEM(tall, bf16)] * 6 + [pltpu.VMEM(wide, bf16)] * 2 + [pltpu.VMEM((2,) + wide, bf16), pltpu.VMEM(wide, bf16)]
    scratch += [pltpu.VMEM((2, SIDE, 2, rows, TRI * BLOCK), f32), pltpu.VMEM((2, SIDE, rows, TRI * BLOCK), f32), pltpu.VMEM((2, 3, rows, TRI * BLOCK), f32)]
    scratch += [pltpu.VMEM((4, PIECE, TRI * BLOCK), f32), pltpu.VMEM((2, PARTS, 2, PIECE, PART_COLS), f32)]
    scratch += [pltpu.VMEM((SIDE, 2, rows, GRAD_COLS), f32), pltpu.VMEM((SIDE, rows, GRAD_COLS), f32), pltpu.VMEM((3, rows, GRAD_COLS), f32)]
    scratch += [pltpu.SemaphoreType.DMA((16,)), pltpu.SemaphoreType.DMA((4 * TRI + PARTS,)), pltpu.SemaphoreType.DMA((N_BATCHES,)), pltpu.SemaphoreType.DMA((N_COPIES,))]
    return pl.pallas_call(
        functools.partial(step_kernel, scale),
        out_shape=[jax.ShapeDtypeStruct((2, SIDE, SIDE, SIDE, PARTS, 4, PIECE, PART_COLS), f32), jax.ShapeDtypeStruct((2, SIDE, 2, rows, GRAD_COLS), f32)],
        in_specs=[hbm, hbm, vmem, vmem, hbm, hbm],
        out_specs=[hbm, vmem],
        scratch_shapes=scratch,
        compiler_params=pltpu.CompilerParams(collective_id=0, has_side_effects=True, vmem_limit_bytes=67043328),
        name='step',
    )(x_tokens, dy_tokens, w_col, w_row, a_old, s_old)


N_BATCHES = 64
N_COPIES = 420


def finish_kernel(first_mat, second_mat, direct_ref, *refs):
    turned, out_ref = refs[:TRI - 2], refs[TRI - 2]
    row_block = pl.program_id(1)
    for j in range(TRI):
        cols = span_of(lax.rem(row_block + j, PLANE), BLOCK)
        part, start = j // PARTS, j % PARTS * BLOCK
        for spot in range(SIDE):
            for core in range(2):
                rows = (2 * spot + core) * PIECE
                out_ref[0, rows:rows + PIECE, cols] = direct_ref[core, 0, 0, spot, part, 0, :, start:start + BLOCK]
    for j in range(1, TRI - 1):
        cols = span_of(lax.rem(row_block + PLANE - j, PLANE), BLOCK)
        block = jnp.concatenate([turned[j - 1][core, 0, 0, spot, 0, 0] for spot in range(SIDE) for core in range(2)], axis=0)
        out_ref[0, :, cols] = block.T


def finish_call(fact, first_mat, second_mat):
    def place(index):
        return lax.div(index, SIDE), lax.rem(index, SIDE)

    def mat_of(i):
        return first_mat + i * (second_mat - first_mat)

    def direct_map(i, n):
        return (0, *place(n), 0, 0, mat_of(i), 0, 0)

    def turned_map(j, i, n):
        return (0, *place(lax.rem(n + PLANE - j, PLANE)), 0, j // PARTS, mat_of(i), 0, j % PARTS)

    return pl.pallas_call(
        functools.partial(finish_kernel, first_mat, second_mat),
        grid=(2, PLANE),
        out_shape=jax.ShapeDtypeStruct((2, WIDTH, WIDTH), jnp.float32),
        in_specs=[pl.BlockSpec((2, 1, 1, SIDE, PARTS, 1, PIECE, PART_COLS), direct_map)] + [pl.BlockSpec((2, 1, 1, SIDE, 1, 1, PIECE, BLOCK), functools.partial(turned_map, j)) for j in range(1, TRI - 1)],
        out_specs=pl.BlockSpec((1, BLOCK, WIDTH), lambda i, n: (i, n, 0)),
        name='finish',
    )(*[fact] * (TRI - 1))


def solution(mesh):
    def shard_body(x_tokens, dy_tokens, w_col, w_row, a_old_col, s_old_col, a_old_row, s_old_row, a_inv_col, s_inv_col, a_inv_row, s_inv_row):
        inv_rows = 1.0 / (x_tokens.shape[0] * DATA_WAYS)
        scale = (1.0 - FACTOR_DECAY) * inv_rows
        fact, grads = step_call(x_tokens, dy_tokens, w_col, w_row, a_old_col, s_old_row, scale)
        a_new_col = finish_call(fact, 0, 2)
        s_new_row = finish_call(fact, 3, 1)
        sums = grads.reshape(2, DATA_WAYS, 2, PIECE, GRAD_COLS).transpose(0, 2, 1, 3, 4).reshape(4, BLOCK, GRAD_COLS)
        third, fourth, first, second = [sums[num, :, :WIDTH] * inv_rows for num in range(4)]
        u_col = jnp.stack([exact_dot(exact_dot(a_inv_col[num], grad.T), s_inv_col[num]) for num, grad in ((0, first), (1, third))])
        u_row = jnp.stack([exact_dot(exact_dot(a_inv_row[num], grad), s_inv_row[num]) for num, grad in ((0, second), (1, fourth))])
        s_new_col = FACTOR_DECAY * s_old_col + scale * jnp.stack([sums[2, :, WIDTH:], sums[0, :, WIDTH:]])
        a_new_row = FACTOR_DECAY * a_old_row + scale * jnp.stack([sums[3, :, WIDTH:], sums[1, :, WIDTH:]])
        return (u_col, u_row, a_new_col, s_new_col, a_new_row, s_new_row)

    batch_split = P('data', None)
    col_split = P(None, None, 'model')
    row_split = P(None, 'model', None)
    replicated = P()
    return jax.shard_map(
        shard_body,
        mesh=mesh,
        in_specs=(batch_split, batch_split, col_split, row_split, replicated, row_split, row_split, replicated, replicated, row_split, row_split, replicated),
        out_specs=(col_split, row_split, replicated, row_split, row_split, replicated),
        check_vma=False,
    )
```

```python
import contextlib
import functools
import math
import jax
import jax.numpy as jnp
from jax import lax
from jax.experimental import pallas as pl
from jax.experimental.pallas import tpu as pltpu
from jax.sharding import PartitionSpec as P

FACTOR_DECAY = 0.8
GELU_SCALE = math.sqrt(2.0 / math.pi)
GELU_CUBIC = 0.044715
EXACT = lax.Precision.HIGHEST
MESH = pl.DeviceIdType.MESH
SIDE = 4
PLANE = 16
DATA_WAYS = 8
WIDTH = 2048
BLOCK = 128
PIECE = 16
TRI = 9
SCOPED = False
FACTOR_COLS = TRI * BLOCK
GRAD_COLS = WIDTH + BLOCK
NT_DIMS = (((1,), (1,)), ((), ()))


def gelu_value(pre_act):
    tanh_arg = GELU_SCALE * (pre_act + GELU_CUBIC * pre_act * pre_act * pre_act)
    return 0.5 * pre_act * (1.0 + jnp.tanh(tanh_arg))


def gelu_slope(pre_act):
    tanh_arg = GELU_SCALE * (pre_act + GELU_CUBIC * pre_act * pre_act * pre_act)
    tanh_val = jnp.tanh(tanh_arg)
    return 0.5 * (1.0 + tanh_val) + 0.5 * pre_act * (1.0 - tanh_val * tanh_val) * GELU_SCALE * (1.0 + 3.0 * GELU_CUBIC * pre_act * pre_act)


def activate(pre_act):
    return gelu_value(pre_act.astype(jnp.float32)).astype(jnp.bfloat16)


def back_gate(grad_act, pre_act):
    return (grad_act.astype(jnp.float32) * gelu_slope(pre_act.astype(jnp.float32))).astype(jnp.bfloat16)


def matmul(left_mat, right_mat):
    return jnp.dot(left_mat, right_mat, preferred_element_type=jnp.float32)


def matmul_nt(left_mat, right_mat):
    return lax.dot_general(left_mat, right_mat, NT_DIMS, preferred_element_type=jnp.float32)


def exact_dot(left_mat, right_mat):
    return jnp.dot(left_mat, right_mat, precision=EXACT, preferred_element_type=jnp.float32)


def scope(name):
    return jax.named_scope(name) if SCOPED else contextlib.nullcontext()


def span_of(index, size):
    return pl.ds(pl.multiple_of(index * size, size), size)


class Place:
    def __init__(self):
        self.model, self.data = lax.axis_index('model'), lax.axis_index('data')
        self.core = lax.rem(self.data, 2)
        here = {'x': lax.div(self.data, 2), 'y': lax.rem(self.model, SIDE), 'z': lax.div(self.model, SIDE)}
        self.along = {dim: [at] + [lax.rem(at + step, SIDE) for step in range(1, SIDE)] for dim, at in here.items()}
        self.planes = [[z * SIDE + y for y in self.along['y']] for z in self.along['z']]
        self.lines = [x * 2 + self.core for x in self.along['x']]
        self.mate = (self.model, self.data + 1 - 2 * self.core)

    def at(self, dim, step):
        return self.along[dim][step % SIDE]

    def peer(self, z_step, y_step):
        return self.planes[z_step % SIDE][y_step % SIDE]

    def device(self, dim, step):
        if dim == 'x':
            return (self.model, self.lines[step % SIDE])
        return (self.peer(step, 0) if dim == 'z' else self.peer(0, step), self.data)


class Copies:
    def __init__(self, send_sems, recv_sems):
        self.send_sems, self.recv_sems = send_sems, recv_sems
        self.names, self.batches = {}, {}

    def start(self, batch, name, src, dst, device):
        num = self.names.setdefault((batch, name), len(self.names))
        out = self.batches.setdefault(batch, len(self.batches))
        pltpu.make_async_remote_copy(src_ref=src, dst_ref=dst, send_sem=self.send_sems.at[out], recv_sem=self.recv_sems.at[num], device_id=device, device_id_type=MESH).start()

    def wait(self, batch, name, ref):
        num = self.names.setdefault((batch, name), len(self.names))
        pltpu.make_async_copy(ref, ref, self.recv_sems.at[num]).wait()

    def left(self, batch, ref):
        pltpu.make_async_copy(ref, ref, self.send_sems.at[self.batches[batch]]).wait()


def call_out(devices):
    for device in devices:
        pl.semaphore_signal(pltpu.get_barrier_semaphore(), inc=1, device_id=device, device_id_type=MESH)


def all_here(devices):
    pl.semaphore_wait(pltpu.get_barrier_semaphore(), len(devices))


def plane_gather(copies, batch, place, region, on_piece):
    def steps(order, first, second):
        return (second, first) if order == 0 else (first, second)

    def rows(order, k, part):
        z_step, y_step = steps(order, *k)
        return region(place.at('z', z_step), place.at('y', y_step), order, *part)

    def send(order, name, k, part, first, second):
        ref = rows(order, k, part)
        copies.start(batch, (order,) + name, ref, ref, (place.peer(*steps(order, first, second)), place.data))

    def recv(order, name, k, part):
        copies.wait(batch, (order,) + name, rows(order, k, part))

    whole, low, high = (0, 2), (0, 1), (1, 2)

    def spread(order, k):
        for step in (1, -1):
            send(order, ('b', k, -step), (k, 0), whole, 0, step)

    def pass_on(order, k):
        for step, part in ((-1, low), (1, high)):
            recv(order, ('b', k, step), (k, step), whole)
            send(order, ('b', k, 2 * step), (k, step), part, 0, -step)
            on_piece(order, *steps(order, k, step))

    for order in (0, 1):
        for step in (1, -1):
            send(order, ('a', -step), (0, 0), whole, step, 0)
    for order in (0, 1):
        spread(order, 0)
    yield
    for order in (0, 1):
        for step, part in ((-1, low), (1, high)):
            recv(order, ('a', step), (step, 0), whole)
            send(order, ('a', 2 * step), (step, 0), part, -step, 0)
            on_piece(order, *steps(order, step, 0))
    yield
    for step in (-1, 1):
        for order in (0, 1):
            spread(order, step)
    yield
    for order in (0, 1):
        pass_on(order, 0)
        yield
    for order in (0, 1):
        recv(order, ('a', -2), (2, 0), low)
        recv(order, ('a', 2), (2, 0), high)
        spread(order, 2)
        on_piece(order, *steps(order, 2, 0))
        yield
    for k in (-1, 1, 2):
        for order in (0, 1):
            pass_on(order, k)
            yield
    for k in (0, -1, 1, 2):
        for order in (0, 1):
            recv(order, ('b', k, -2), (k, 2), low)
            recv(order, ('b', k, 2), (k, 2), high)
            on_piece(order, *steps(order, k, 2))
        yield


STEPS = [(a, b) for a in range(SIDE) for b in range(SIDE) if (a, b) != (0, 0)]


def line_reduce(copies, batch, place, src, near, far, store):
    core = place.core
    half = near.shape[1] // 2
    low, high = pl.ds(0, half), pl.ds(half, half)
    here, right, across, left = [place.at('x', step) for step in range(SIDE)]
    copies.start((batch, 'near'), 0, src.at[:, 1 - core], near, place.mate)
    yield
    copies.wait((batch, 'near'), 0, near)
    near[across] = near[across] + src[across, core]
    copies.start((batch, 'half'), 1, near.at[across, low], far.at[0, low], place.device('x', 1))
    copies.start((batch, 'half'), -1, near.at[across, high], far.at[0, high], place.device('x', -1))
    for there in (right, left, here):
        near[there] = near[there] + src[there, core]
    yield
    copies.wait((batch, 'half'), 1, far.at[0, low])
    near[right, low] = near[right, low] + far[0, low]
    copies.start((batch, 'full'), 1, near.at[right], far.at[1], place.device('x', 1))
    copies.wait((batch, 'half'), -1, far.at[0, high])
    near[left, high] = near[left, high] + far[0, high]
    copies.start((batch, 'full'), -1, near.at[left], far.at[2], place.device('x', -1))
    yield
    copies.wait((batch, 'full'), 1, far.at[1])
    copies.wait((batch, 'full'), -1, far.at[2])
    store(near[here] + far[1] + far[2])
    copies.left((batch, 'near'), near)
    copies.left((batch, 'half'), far.at[0])
    copies.left((batch, 'full'), far.at[pl.ds(1, 2)])
    yield


def line_gather(copies, batch, place, out):
    core = place.core
    half = out.shape[2] // 2
    here, right, across, left = [out.at[place.at('x', step), core] for step in range(SIDE)]

    def hand(ref):
        copies.start((batch, 'hand'), 0, ref, ref, place.mate)

    for step in (1, -1):
        copies.start((batch, 'all'), step, here, here, place.device('x', step))
    hand(here)
    yield
    for step, ref, span in ((1, left, pl.ds(0, half)), (-1, right, pl.ds(half, half))):
        copies.wait((batch, 'all'), step, ref)
        copies.start((batch, 'all'), 2 * step, ref.at[span], ref.at[span], place.device('x', step))
        hand(ref)
    yield
    for step, span in ((1, pl.ds(0, half)), (-1, pl.ds(half, half))):
        copies.wait((batch, 'all'), 2 * step, across.at[span])
    hand(across)
    yield
    copies.wait((batch, 'hand'), 0, out.at[:, 0])
    copies.left((batch, 'all'), out.at[0:3, 0])
    copies.left((batch, 'hand'), out.at[:, 0])
    yield


BALANCED = (('x', 'y', 'z'), ('y', 'z', 'x'), ('z', 'x', 'y'))
X_LAST = (('y', 'z', 'x'), ('z', 'y', 'x'))


def cube_gather(copies, batch, place, view, order):
    first, second, third = order
    core = place.core

    def at(which, places):
        return view(which, places['z'], places['y'], places['x'])

    def single(step):
        return at(core, {first: place.at(first, step), second: place.at(second, 0), third: place.at(third, 0)})

    def group(a, b, span=(0, SIDE)):
        return at(core, {first: pl.ds(*span), second: place.at(second, a), third: place.at(third, b)})

    low, high = (0, 2), (2, 2)

    def hand(a, b):
        ref = group(a, b)
        copies.start((batch, 'mate'), 0, ref, ref, place.mate)

    def spread(a):
        ref = group(a, 0)
        for step in (1, -1):
            copies.start((batch, 'three'), (a, -step), ref, ref, place.device(third, step))
        hand(a, 0)

    def pass_on(a):
        for step, span in ((-1, low), (1, high)):
            copies.wait((batch, 'three'), (a, step), group(a, step))
            half = group(a, step, span)
            copies.start((batch, 'three'), (a, 2 * step), half, half, place.device(third, -step))
            hand(a, step)

    for step in (2, 1, -1):
        copies.start((batch, 'one'), -step % SIDE, single(0), single(0), place.device(first, step))
    yield
    for step in (1, 3, 2):
        copies.wait((batch, 'one'), step, single(step))
    for step in (1, -1):
        copies.start((batch, 'two'), -step, group(0, 0), group(0, 0), place.device(second, step))
    spread(0)
    yield
    for step, span in ((-1, low), (1, high)):
        copies.wait((batch, 'two'), step, group(step, 0))
        half = group(step, 0, span)
        copies.start((batch, 'two'), 2 * step, half, half, place.device(second, -step))
        spread(step)
    yield
    pass_on(0)
    yield
    for step, span in ((-1, low), (1, high)):
        copies.wait((batch, 'two'), 2 * step, group(2, 0, span))
    spread(2)
    yield
    for a in (-1, 1, 2):
        pass_on(a)
        yield
    for a in (0, -1, 1, 2):
        for step, span in ((-1, low), (1, high)):
            copies.wait((batch, 'three'), (a, 2 * step), group(a, 2, span))
        hand(a, 2)
        yield
    whole = pl.ds(0, SIDE)
    copies.wait((batch, 'mate'), 0, view(0, whole, whole, whole))
    copies.left((batch, 'mate'), view(0, whole, whole, whole))
    copies.left((batch, 'one'), view(0, 0, 0, pl.ds(0, 3)))
    copies.left((batch, 'two'), view(0, 0, pl.ds(0, 3), whole))
    copies.left((batch, 'three'), view(0, pl.ds(0, 3), whole, whole))
    yield


def interleave(*gens):
    gens = list(gens)
    while gens:
        for gen in list(gens):
            try:
                next(gen)
            except StopIteration:
                gens.remove(gen)
        yield


def pump(gen, count=1, name='pump'):
    for _ in range(count):
        with scope(name):
            next(gen, None)


def drain(gen, name='drain'):
    with scope(name):
        for _ in gen:
            pass


def step_kernel(scale, x_hbm, dy_hbm, w_col, w_row, a_old, s_old, a_inv, s_inv, fact, grads, x_buf, dy_buf, h_two, w_two, w_three, z_one, h_one, h_three,
                g_three, t_three, rows_buf, z_two, left, w_three_t, gram_src, gram_near, gram_far, old_buf, piece_buf, grad_src, grad_near,
                grad_far, grad_sum, grad_out, big_buf, load_sems, old_sems, big_sems, send_sems, recv_sems):
    place = Place()
    model_id, data_id, core = place.model, place.data, place.core
    spot, y_pos, z_pos = place.at('x', 0), place.at('y', 0), place.at('z', 0)
    copies = Copies(send_sems, recv_sems)
    my_rows = span_of(model_id, BLOCK)
    my_cols = span_of(model_id, BLOCK)
    my_part = pl.ds(pl.multiple_of(data_id * PIECE, PIECE), PIECE)
    g_one = t_three
    olds = [a_old.at[0], s_old.at[1], a_old.at[1], s_old.at[0]]
    chunk = 256
    n_chunks = WIDTH // chunk
    met = [(place.peer(a, b), data_id) for a, b in STEPS] + [place.mate] + [place.device('x', step) for step in (1, 2, 3)]

    def load(src, dst, base, i):
        rows = span_of(i, chunk)
        return pltpu.make_async_copy(src.at[rows, :], dst.at[rows, :], load_sems.at[base + i])

    def load_x(i):
        return load(x_hbm, x_buf, 0, i)

    def load_dy(i):
        return load(dy_hbm, dy_buf, n_chunks, i)

    def load_old(mat, j):
        rows = pl.ds(pl.multiple_of(model_id * BLOCK + data_id * PIECE, PIECE), PIECE)
        cols = span_of(lax.rem(model_id + j, PLANE), BLOCK)
        return pltpu.make_async_copy(olds[mat].at[rows, cols], old_buf.at[mat, :, pl.ds(j * BLOCK, BLOCK)], old_sems.at[mat])

    def cols_of(buf, cols):
        return buf[:, cols] if len(buf.shape) == 2 else buf[:, :, :, :, :, cols].reshape(WIDTH, cols.size)

    def rows_of(buf, z_step, y_step):
        return buf[place.at('z', z_step), place.at('y', y_step)].reshape(BLOCK, WIDTH)

    call_out(met)
    for i in range(n_chunks):
        load_x(i).start()
    for i in range(n_chunks):
        load_dy(i).start()
    for mat in range(4):
        for j in range(TRI):
            load_old(mat, j).start()

    def z_one_step(i, carry):
        rows = span_of(i, chunk)
        load_x(i).wait()
        pre_act = matmul(x_buf[rows, :], w_col[0]).astype(jnp.bfloat16)
        z_one[rows, :] = pre_act
        h_one[rows, :] = activate(pre_act)
        return carry

    with scope('z1a'):
        w_two[z_pos, y_pos] = w_row[0].reshape(SIDE, 2, PIECE, WIDTH)
        w_three_t[...] = w_col[1].T
        w_three[z_pos, y_pos, spot, core] = w_three_t[my_part, :]
        lax.fori_loop(0, n_chunks // 2, z_one_step, 0)
    with scope('greet'):
        all_here(met)

    def weight_thread(batch, buf, orders, cuts):
        def view(part, which, z, y, x):
            return buf.at[z, y, x, which, :, pl.ds(cuts[part], cuts[part + 1] - cuts[part])]
        return interleave(*[cube_gather(copies, (batch, part), place, functools.partial(view, part), orders[part]) for part in range(len(cuts) - 1)])

    def half_rows(z, y, order, lo, hi):
        return w_two.at[z, y, 2 * core + order, pl.ds(lo, hi - lo)]

    def hand_rows(order, z_step, y_step):
        ref = half_rows(place.at('z', z_step), place.at('y', y_step), order, 0, 2)
        copies.start('w2mate', 0, ref, ref, place.mate)

    w_two_gen = plane_gather(copies, 'w2', place, half_rows, hand_rows)
    w_three_gen = weight_thread('w3', w_three, X_LAST, (0, WIDTH // 2, WIDTH))
    pump(w_three_gen, 1, 'w3')
    pump(w_two_gen, 1, 'w2')
    with scope('z1b'):
        lax.fori_loop(n_chunks // 2, n_chunks, z_one_step, 0)

    def send_block(batch, cols_ref, a, b):
        peer = place.peer(a, b)
        copies.start(batch, 0, cols_ref.at[span_of(peer, BLOCK), :], rows_buf.at[:, my_cols], (peer, data_id))

    def wait_blocks(batch):
        others = rows_buf.at[:, 0:WIDTH - BLOCK]
        copies.wait(batch, 0, others)
        copies.left(batch, others)

    def t_three_step(i, carry):
        rows = span_of(i, chunk)
        t_three[rows, :] = matmul_nt(dy_buf[rows, :], w_row[1]).astype(jnp.bfloat16)
        return carry

    def turn(dst, src, cols):
        for i in range(4):
            rows = slice(i * 512, (i + 1) * 512)
            dst[:, rows] = (src[rows, cols] if len(src.shape) == 2 else src[i, :, :, :, :, cols].reshape(512, BLOCK)).T

    def gram_product(mat, lhs, right):
        def gram_step(j, carry):
            block = matmul(lhs[...], cols_of(right, span_of(lax.rem(model_id + j, PLANE), BLOCK)))
            gram_src[mat, :, :, :, span_of(j, BLOCK)] = block.reshape(SIDE, 2, PIECE, BLOCK)
            return carry
        lax.fori_loop(0, TRI, gram_step, 0)

    def grad_product(lhs, right, same, slot):
        def grad_step(i, carry):
            cols = span_of(i, chunk)
            block = matmul(lhs[...], cols_of(right, cols))
            grad_src[:, :, slot * PIECE:(slot + 1) * PIECE, cols] = block.reshape(SIDE, 2, PIECE, chunk)
            return carry
        lax.fori_loop(0, n_chunks, grad_step, 0)
        block = matmul(lhs[...], same[...])
        grad_src[:, :, slot * PIECE:(slot + 1) * PIECE, WIDTH:GRAD_COLS] = block.reshape(SIDE, 2, PIECE, BLOCK)

    def store_factor(mat, total):
        pltpu.make_async_copy(old_buf.at[mat], old_buf.at[mat], old_sems.at[mat]).wait()
        mixed = FACTOR_DECAY * old_buf[mat] + scale * total
        piece_buf[mat] = mixed

    def sum_thread(mat):
        return line_reduce(copies, ('gram', mat), place, gram_src.at[mat], gram_near.at[mat], gram_far.at[mat], functools.partial(store_factor, mat))

    def factor_thread(first, count, orders, cuts):
        mats = pl.ds(first, count)

        def view(part, which, z, y, x):
            return fact.at[z, y, x, which, mats, :, pl.ds(cuts[part], cuts[part + 1] - cuts[part])]

        move = pltpu.make_async_copy(piece_buf.at[mats], fact.at[z_pos, y_pos, spot, core, mats], old_sems.at[4])
        move.start()
        move.wait()
        yield from interleave(*[cube_gather(copies, ('fact', first, part), place, functools.partial(view, part), orders[part]) for part in range(len(orders))])

    first_sum, second_sum = sum_thread(0), sum_thread(1)
    first_pair = factor_thread(0, 2, X_LAST, (0, 640, FACTOR_COLS))
    with scope('gramA1'):
        turn(left.at[0], x_buf, my_cols)
        gram_product(0, left.at[0], x_buf)
    pump(first_sum)
    pump(w_two_gen, 2, 'w2')
    pump(w_three_gen, 1, 'w3')
    with scope('gramS4'):
        for i in range(n_chunks):
            load_dy(i).wait()
        turn(left.at[1], dy_buf, my_cols)
        gram_product(1, left.at[1], dy_buf)
    pump(second_sum)
    pump(w_two_gen, 2, 'w2')
    pump(first_sum, 1, 'sum')
    for a, b in STEPS:
        send_block('h1', h_one, a, b)
    rows_buf[:, my_cols] = h_one[my_rows, :]
    with scope('t3a'):
        lax.fori_loop(0, n_chunks // 4, t_three_step, 0)
    pump(w_two_gen, 2, 'w2')
    pump(second_sum, 1, 'sum')
    with scope('t3b'):
        lax.fori_loop(n_chunks // 4, n_chunks // 2, t_three_step, 0)
    pump(first_sum, 1, 'sum')
    with scope('t3c'):
        lax.fori_loop(n_chunks // 2, 3 * n_chunks // 4, t_three_step, 0)
    pump(w_two_gen, 2, 'w2')
    pump(second_sum, 1, 'sum')
    with scope('t3d'):
        lax.fori_loop(3 * n_chunks // 4, n_chunks, t_three_step, 0)
    pump(w_two_gen, 2, 'w2')
    pump(first_sum, 1, 'sum')
    pump(second_sum, 1, 'sum')
    pump(first_pair, 1, 'pair')
    pump(w_two_gen, 2, 'w2')
    pump(w_three_gen, 1, 'w3')
    pump(w_two_gen, 1, 'w2')
    pump(w_three_gen, 1, 'w3')
    drain(w_two_gen, 'w2_rest')
    pump(w_three_gen, 1, 'w3')
    with scope('wait_w2mate'):
        rows = x_buf.at[0:(WIDTH - BLOCK) // 2, :]
        copies.wait('w2mate', 0, rows)
        copies.left('w2mate', rows)
        copies.left('w2', rows)
    with scope('wait_h1'):
        wait_blocks('h1')

    def z_two_step(i, carry):
        cols = span_of(i, chunk)
        pre_act = matmul(rows_buf[...], cols_of(w_two, cols)).astype(jnp.bfloat16)
        z_two[:, cols] = pre_act
        h_two[z_pos, y_pos, :, :, :, cols] = activate(pre_act).reshape(SIDE, 2, PIECE, chunk)
        return carry

    with scope('z2'):
        lax.fori_loop(0, n_chunks, z_two_step, 0)

    def forward_block(a, b):
        rows = span_of(place.peer(a, b), BLOCK)
        pre_act = matmul(rows_of(h_two, a, b), w_col[1]).astype(jnp.bfloat16)
        h_three[rows, :] = activate(pre_act)
        g_three[rows, :] = back_gate(t_three[rows, :], pre_act)
        if (a, b) != (0, 0):
            send_block('g3', g_three, a, b)

    def backward_block(a, b):
        rows = span_of(place.peer(a, b), BLOCK)
        grad = matmul_nt(rows_of(w_two, a, b), w_row[0]).astype(jnp.bfloat16)
        g_one[rows, :] = back_gate(grad, z_one[rows, :])

    def gather_tokens(tag, buf, block_step, fill):
        seen = {}

        def on_piece(order, first, second):
            where = (first % SIDE, second % SIDE)
            seen[where] = seen.get(where, 0) + 1

        def region(z, y, order, lo, hi):
            return buf.at[z, y, pl.ds(2 * order + lo, hi - lo)]

        done = {(0, 0)}
        gen = plane_gather(copies, tag, place, region, on_piece)
        pump(gen, 1, tag + '_step')
        with scope(tag + '_blocks'):
            block_step(0, 0)
        for num in range(GATHER_STEPS):
            pump(gen, 1, tag + '_step#n=' + str(num))
            ready = [where for where in sorted(seen) if seen[where] == 2 and where not in done]
            with scope(tag + '_blocks'):
                for where in ready:
                    block_step(*where)
            done.update(ready)
            for job in fill.get(num, ()):
                job()
        copies.left(tag, x_buf.at[0:WIDTH - BLOCK, :])

    def step_of(gen, name, count=1):
        return functools.partial(pump, gen, count, name)

    pump(w_three_gen, 1, 'w3')
    gather_tokens('h2', h_two, forward_block, {
        0: [step_of(w_three_gen, 'w3')],
        2: [step_of(w_three_gen, 'w3'), step_of(first_pair, 'pair')],
        8: [step_of(first_pair, 'pair')],
        10: [step_of(w_three_gen, 'w3', 2)],
        12: [step_of(first_pair, 'pair', 2), step_of(w_three_gen, 'w3')],
        13: [step_of(w_three_gen, 'w3')],
        15: [step_of(first_pair, 'pair')],
    })
    with scope('dW4'):
        turn(left.at[1], h_three, slice(0, BLOCK))
        grad_product(left.at[1], dy_buf, h_three, 1)
    drain(w_three_gen, 'w3_rest')
    pump(first_pair, 1, 'pair')
    with scope('wait_g3'):
        wait_blocks('g3')
        rows_buf[:, my_cols] = g_three[my_rows, :]

    def g_two_step(i, carry):
        cols = span_of(i, chunk)
        grad = matmul(rows_buf[...], cols_of(w_three, cols)).astype(jnp.bfloat16)
        w_two[z_pos, y_pos, :, :, :, cols] = back_gate(grad, z_two[:, cols]).reshape(SIDE, 2, PIECE, chunk)
        return carry

    with scope('g2'):
        lax.fori_loop(0, n_chunks, g_two_step, 0)

    def split(value):
        high = value.astype(jnp.bfloat16)
        rest = value - high.astype(jnp.float32)
        middle = rest.astype(jnp.bfloat16)
        return high, middle, (rest - middle.astype(jnp.float32)).astype(jnp.bfloat16)

    def grad_thread(batch):
        sum_ref, out_ref = grad_sum.at[batch], grad_out.at[batch]

        def keep_sum(total):
            sum_ref[core] = total

        yield from line_reduce(copies, ('grad', batch), place, grad_src, grad_near.at[batch], grad_far.at[batch], keep_sum)
        copies.start(('pair', batch), 0, sum_ref.at[core], sum_ref.at[core], place.mate)
        layers = [(a_inv, 1), (s_inv, 1)] if batch == 0 else [(a_inv, 0), (s_inv, 0)]
        rows = 2 * PIECE

        def load_big(inverse, num, i):
            slot = lax.rem(i, 2)
            return pltpu.make_async_copy(inverse.at[num, span_of(i, chunk), span_of(core, WIDTH // 2)], big_buf.at[slot], big_sems.at[slot])

        yield
        for slot, (inverse, num) in enumerate(layers):
            mine = slice(slot * PIECE, (slot + 1) * PIECE)
            out = slice(slot * rows, (slot + 1) * rows)
            load = functools.partial(load_big, inverse, num)

            def big_step(i, carry):
                load(i).wait()
                lhs = jnp.concatenate(split(sum_ref[:, mine, span_of(i, chunk)].reshape(rows, chunk)), axis=0)
                high, middle, low = split(big_buf[lax.rem(i, 2)])
                by_high, by_middle, by_low = matmul(lhs, high), matmul(lhs[:2 * rows], middle), matmul(lhs[:rows], low)
                small = by_high[2 * rows:] + by_middle[rows:] + by_low
                out_ref[out, :WIDTH // 2] += by_high[:rows] + (by_high[rows:2 * rows] + by_middle[:rows] + small)

                @pl.when(i + 2 < n_chunks)
                def _():
                    load(i + 2).start()
                return carry

            load(0).start()
            load(1).start()
            if slot == 0:
                copies.wait(('pair', batch), 0, sum_ref.at[1 - core])
                copies.left(('pair', batch), sum_ref.at[0])
            out_ref[out, :] = jnp.concatenate([jnp.zeros((rows, WIDTH // 2), jnp.float32), sum_ref[:, mine, WIDTH:].reshape(rows, BLOCK)], axis=1)
            with scope('X'):
                lax.fori_loop(0, n_chunks // 2, big_step, 0)
            yield
            with scope('X'):
                lax.fori_loop(n_chunks // 2, n_chunks, big_step, 0)
            if slot == 0:
                yield
        move = pltpu.make_async_copy(out_ref, grads.at[batch, spot, core], old_sems.at[5])
        move.start()
        move.wait()
        yield from line_gather(copies, ('grad', batch), place, grads.at[batch])

    def third_grad():
        with scope('dW3'):
            turn(left.at[0], g_three, slice(0, BLOCK))
            grad_product(left.at[0], h_two, g_three, 0)

    third_sum = sum_thread(2)

    def third_gram():
        with scope('gramA3'):
            turn(left.at[0], h_two, my_cols)
            gram_product(2, left.at[0], h_two)

    late = grad_thread(0)
    cuts = (0, 384, 640, FACTOR_COLS)
    third_factor = factor_thread(2, 1, BALANCED, cuts)
    gather_tokens('g2', w_two, backward_block, {
        0: [third_grad, step_of(late, 'late')],
        1: [third_gram, step_of(third_sum, 'sum'), step_of(late, 'late')],
        2: [step_of(first_pair, 'pair')],
        4: [step_of(third_sum, 'sum')],
        7: [step_of(first_pair, 'pair')],
        8: [step_of(third_sum, 'sum')],
        9: [step_of(first_pair, 'pair')],
        10: [step_of(late, 'late')],
        12: [step_of(first_pair, 'pair')],
        13: [step_of(third_sum, 'sum'), step_of(third_factor, 'a3')],
        14: [step_of(first_pair, 'pair')],
        15: [step_of(late, 'late'), step_of(third_factor, 'a3')],
    })
    with scope('dW2'):
        turn(left.at[0], h_one, slice(0, BLOCK))
        grad_product(left.at[0], w_two, h_one, 1)
    pump(late, 1, 'late')
    with scope('dW1'):
        turn(left.at[1], g_one, slice(0, BLOCK))
        grad_product(left.at[1], x_buf, g_one, 0)
    last = grad_thread(1)
    pump(last, 1, 'last')
    pump(third_factor, 1, 'a3')
    with scope('gramS2'):
        turn(left.at[0], w_two, my_cols)
        gram_product(3, left.at[0], w_two)
    last_sum = sum_thread(3)
    pump(last_sum, 1, 'sum')
    pump(third_factor, 1, 'a3')
    for _ in range(2):
        pump(last, 1, 'last')
        pump(late, 1, 'late')
        pump(last_sum, 1, 'sum')
        pump(third_factor, 1, 'a3')
    pump(last, 2, 'last')
    drain(last_sum, 'sum')
    last_factor = factor_thread(3, 1, BALANCED, cuts)
    pump(last_factor, 1, 's2')
    pump(late, 1, 'late')
    pump(third_factor, 1, 'a3')
    pump(last_factor, 1, 's2')
    pump(late, 1, 'late')
    pump(third_factor, 1, 'a3')
    pump(last, 1, 'last')
    pump(last_factor, 1, 's2')
    pump(third_factor, 1, 'a3')
    pump(last, 1, 'last')
    pump(last_factor, 1, 's2')
    pump(late, 1, 'late')
    pump(third_factor, 1, 'a3')
    pump(last, 1, 'last')
    pump(last_factor, 1, 's2')
    pump(third_factor, 1, 'a3')
    pump(last, 1, 'last')
    pump(late, 1, 'late')
    pump(last_factor, 2, 's2')
    pump(third_factor, 1, 'a3')
    pump(last, 1, 'last')
    pump(last_factor, 1, 's2')
    pump(late, 1, 'late')
    pump(last, 1, 'last')
    pump(last_factor, 2, 's2')
    drain(third_factor, 'a3_rest')
    drain(first_pair, 'pair_rest')
    drain(late, 'late_rest')
    drain(last, 'last_rest')
    drain(last_factor, 's2_rest')
    assert len(copies.batches) <= N_BATCHES and len(copies.names) <= N_COPIES, (len(copies.batches), len(copies.names))


GATHER_STEPS = 17
N_BATCHES = 70
N_COPIES = 405


def step_call(x_tokens, dy_tokens, w_col, w_row, a_old, s_old, a_inv, s_inv, scale):
    f32, bf16 = jnp.float32, jnp.bfloat16
    tall, wide = (WIDTH, BLOCK), (BLOCK, WIDTH)
    cube = (SIDE, SIDE, SIDE, 2)
    rows = 2 * PIECE
    vmem = pl.BlockSpec(memory_space=pltpu.VMEM)
    hbm = pl.BlockSpec(memory_space=pl.ANY)
    scratch = [pltpu.VMEM((WIDTH, WIDTH), bf16)] * 2 + [pltpu.VMEM(cube + (PIECE, WIDTH), bf16)] * 3
    scratch += [pltpu.VMEM(tall, bf16)] * 5 + [pltpu.VMEM(wide, bf16)] * 2 + [pltpu.VMEM((2,) + wide, bf16), pltpu.VMEM(wide, bf16)]
    scratch += [pltpu.VMEM((4, SIDE, 2, PIECE, TRI * BLOCK), f32), pltpu.VMEM((4, SIDE, PIECE, TRI * BLOCK), f32), pltpu.VMEM((4, 3, PIECE, TRI * BLOCK), f32)]
    scratch += [pltpu.VMEM((4, PIECE, TRI * BLOCK), f32), pltpu.VMEM((4, PIECE, FACTOR_COLS), f32)]
    scratch += [pltpu.VMEM((SIDE, 2, rows, GRAD_COLS), f32), pltpu.VMEM((2, SIDE, rows, GRAD_COLS), f32), pltpu.VMEM((2, 3, rows, GRAD_COLS), f32)]
    scratch += [pltpu.VMEM((2, 2, rows, GRAD_COLS), f32), pltpu.VMEM((2, 2 * rows, WIDTH // 2 + BLOCK), f32), pltpu.VMEM((2, 256, WIDTH // 2), f32)]
    scratch += [pltpu.SemaphoreType.DMA((num,)) for num in (16, 6, 2, N_BATCHES, N_COPIES)]
    return pl.pallas_call(
        functools.partial(step_kernel, scale),
        out_shape=[jax.ShapeDtypeStruct(cube + (4, PIECE, FACTOR_COLS), f32), jax.ShapeDtypeStruct((2, SIDE, 2, 2 * rows, WIDTH // 2 + BLOCK), f32)],
        in_specs=[hbm, hbm, vmem, vmem] + [hbm] * 4,
        out_specs=[hbm, hbm],
        scratch_shapes=scratch,
        compiler_params=pltpu.CompilerParams(collective_id=0, has_side_effects=True, vmem_limit_bytes=67043328),
        name='step',
    )(x_tokens, dy_tokens, w_col, w_row, a_old, s_old, a_inv, s_inv)


def finish_kernel(scale, inv_rows, fact, grads, s_old_col, a_old_row, s_inv_col, a_inv_row, a_new, s_new, u_col, u_row, s_new_col, a_new_row, buf, turned, sums, load_sems, out_sems, turn_sems):
    outs = [(a_new, 0), (s_new, 1), (a_new, 1), (s_new, 0)]

    def load(mat, row):
        z, y = lax.div(row, SIDE), lax.rem(row, SIDE)
        return pltpu.make_async_copy(fact.at[z, y, :, :, mat], buf.at[mat, row], load_sems.at[mat * PLANE + row])

    def turn_done(slot):
        return pltpu.make_async_copy(turned.at[slot], turned.at[slot], turn_sems.at[slot])

    def start_load(mat):
        def body(row, carry):
            load(mat, row).start()
            return carry
        lax.fori_loop(0, PLANE, body, 0)

    load_sums = pltpu.make_async_copy(grads, sums, out_sems.at[4])
    load_sums.start()
    for mat in range(4):
        start_load(mat)
    half = WIDTH // 2
    load_sums.wait()
    layers = [(0, 0, 1), (0, 1, 1), (1, 0, 0), (1, 1, 0)]
    for batch, slot, num in layers:
        block = scale * sums[batch, :, 0, slot * 2 * PIECE:(slot + 1) * 2 * PIECE, half:].reshape(BLOCK, BLOCK)
        if slot == 0:
            s_new_col[num] = FACTOR_DECAY * s_old_col[num] + block
        else:
            a_new_row[num] = FACTOR_DECAY * a_old_row[num] + block

    def small_product(layer, row):
        batch, slot, num = layers[layer]
        core, cols = lax.div(row, PLANE // 2), span_of(lax.rem(row, PLANE // 2), BLOCK)
        product = sums[batch, :, core, slot * 2 * PIECE:(slot + 1) * 2 * PIECE, cols].reshape(BLOCK, BLOCK)
        if slot == 0:
            u_col[num, span_of(row, BLOCK), :] = exact_dot(product.T, s_inv_col[num]) * inv_rows
        else:
            u_row[num, :, span_of(row, BLOCK)] = exact_dot(a_inv_row[num], product) * inv_rows

    for mat, (out, num) in enumerate(outs):
        def row_step(row, carry):
            load(mat, row).wait()
            slot = lax.rem(row, 2)
            small_product(mat, row)
            for j in range(TRI):
                cols = span_of(lax.rem(row + j, PLANE), BLOCK)
                pltpu.make_async_copy(buf.at[mat, row, :, :, :, pl.ds(j * BLOCK, BLOCK)], out.at[num, row, :, :, :, cols], out_sems.at[mat]).start()
            if mat > 0:
                turn_done(slot).wait()
            else:
                @pl.when(row >= 2)
                def _():
                    turn_done(slot).wait()
            for j in range(1, TRI - 1):
                other = lax.rem(row + j, PLANE)
                block = buf[mat, row, :, :, :, j * BLOCK:(j + 1) * BLOCK].reshape(BLOCK, BLOCK).T
                turned[slot, j - 1] = block.reshape(SIDE, 2, PIECE, BLOCK)
                pltpu.make_async_copy(turned.at[slot, j - 1], out.at[num, other, :, :, :, span_of(row, BLOCK)], turn_sems.at[slot]).start()
            return carry

        lax.fori_loop(0, PLANE, row_step, 0)
    for slot in range(2):
        turn_done(slot).wait()
    for mat in range(4):
        pltpu.make_async_copy(buf.at[mat], buf.at[mat], out_sems.at[mat]).wait()


def finish_call(fact, grads, s_old_col, a_old_row, s_inv_col, a_inv_row, scale, inv_rows):
    f32 = jnp.float32
    shapes = [(2, PLANE, SIDE, 2, PIECE, WIDTH)] * 2 + [(2, WIDTH, BLOCK), (2, BLOCK, WIDTH)] + [(2, BLOCK, BLOCK)] * 2
    hbm, vmem = pl.BlockSpec(memory_space=pl.ANY), pl.BlockSpec(memory_space=pltpu.VMEM)
    return pl.pallas_call(
        functools.partial(finish_kernel, scale, inv_rows),
        out_shape=[jax.ShapeDtypeStruct(shape, f32) for shape in shapes],
        in_specs=[hbm] * 2 + [vmem] * 4,
        out_specs=[hbm] * 2 + [vmem] * 4,
        scratch_shapes=[pltpu.VMEM((4, PLANE, SIDE, 2, PIECE, FACTOR_COLS), f32), pltpu.VMEM((2, TRI - 2, SIDE, 2, PIECE, BLOCK), f32), pltpu.VMEM(grads.shape, f32)] + [pltpu.SemaphoreType.DMA((num,)) for num in (4 * PLANE, 5, 2)],
        compiler_params=pltpu.CompilerParams(vmem_limit_bytes=67043328),
        name='finish',
    )(fact, grads, s_old_col, a_old_row, s_inv_col, a_inv_row)


def solution(mesh):
    def shard_body(x_tokens, dy_tokens, w_col, w_row, a_old_col, s_old_col, a_old_row, s_old_row, a_inv_col, s_inv_col, a_inv_row, s_inv_row):
        inv_rows = 1.0 / (x_tokens.shape[0] * DATA_WAYS)
        scale = (1.0 - FACTOR_DECAY) * inv_rows
        fact, grads = step_call(x_tokens, dy_tokens, w_col, w_row, a_old_col, s_old_row, a_inv_col, s_inv_row, scale)
        a_new_col, s_new_row, u_col, u_row, s_new_col, a_new_row = finish_call(fact, grads, s_old_col, a_old_row, s_inv_col, a_inv_row, scale, inv_rows)
        return (u_col, u_row, a_new_col.reshape(2, WIDTH, WIDTH), s_new_col, a_new_row, s_new_row.reshape(2, WIDTH, WIDTH))

    batch_split = P('data', None)
    col_split = P(None, None, 'model')
    row_split = P(None, 'model', None)
    replicated = P()
    return jax.shard_map(
        shard_body,
        mesh=mesh,
        in_specs=(batch_split, batch_split, col_split, row_split, replicated, row_split, row_split, replicated, replicated, row_split, row_split, replicated),
        out_specs=(col_split, row_split, replicated, row_split, row_split, replicated),
        check_vma=False,
    )
```

```python
import contextlib
import functools
import math
import jax
import jax.numpy as jnp
from jax import lax
from jax.experimental import pallas as pl
from jax.experimental.pallas import tpu as pltpu
from jax.sharding import PartitionSpec as P

FACTOR_DECAY = 0.8
GELU_SCALE = math.sqrt(2.0 / math.pi)
GELU_CUBIC = 0.044715
EXACT = lax.Precision.HIGHEST
MESH = pl.DeviceIdType.MESH
SIDE = 4
PLANE = 16
DATA_WAYS = 8
WIDTH = 2048
BLOCK = 128
PIECE = 16
TRI = 9
ONLY = 0
CORES = 2
BOTH_WAYS = (1, -1)
ORDERS = (0, 1)
HALF = WIDTH // 2
SCOPED = False
FACTOR_COLS = TRI * BLOCK
GRAD_COLS = WIDTH + BLOCK
NT_DIMS = (((1,), (1,)), ((), ()))


def gelu_value(pre_act):
    tanh_arg = GELU_SCALE * (pre_act + GELU_CUBIC * pre_act * pre_act * pre_act)
    return 0.5 * pre_act * (1.0 + jnp.tanh(tanh_arg))


def gelu_slope(pre_act):
    tanh_arg = GELU_SCALE * (pre_act + GELU_CUBIC * pre_act * pre_act * pre_act)
    tanh_val = jnp.tanh(tanh_arg)
    return 0.5 * (1.0 + tanh_val) + 0.5 * pre_act * (1.0 - tanh_val * tanh_val) * GELU_SCALE * (1.0 + 3.0 * GELU_CUBIC * pre_act * pre_act)


def activate(pre_act):
    return gelu_value(pre_act.astype(jnp.float32)).astype(jnp.bfloat16)


def back_gate(grad_act, pre_act):
    return (grad_act.astype(jnp.float32) * gelu_slope(pre_act.astype(jnp.float32))).astype(jnp.bfloat16)


def matmul(left_mat, right_mat):
    return jnp.dot(left_mat, right_mat, preferred_element_type=jnp.float32)


def matmul_nt(left_mat, right_mat):
    return lax.dot_general(left_mat, right_mat, NT_DIMS, preferred_element_type=jnp.float32)


def exact_dot(left_mat, right_mat):
    return jnp.dot(left_mat, right_mat, precision=EXACT, preferred_element_type=jnp.float32)


def scope(name):
    return jax.named_scope(name) if SCOPED else contextlib.nullcontext()


def span_of(index, size):
    return pl.ds(pl.multiple_of(index * size, size), size)


class Place:
    def __init__(self):
        self.model, self.data = lax.axis_index('model'), lax.axis_index('data')
        self.core = lax.rem(self.data, 2)
        here = {'x': lax.div(self.data, 2), 'y': lax.rem(self.model, SIDE), 'z': lax.div(self.model, SIDE)}
        self.along = {dim: [at] + [lax.rem(at + step, SIDE) for step in range(1, SIDE)] for dim, at in here.items()}
        self.planes = [[z * SIDE + y for y in self.along['y']] for z in self.along['z']]
        self.lines = [x * 2 + self.core for x in self.along['x']]
        self.mate = (self.model, self.data + 1 - 2 * self.core)

    def at(self, dim, step):
        return self.along[dim][step % SIDE]

    def peer(self, z_step, y_step):
        return self.planes[z_step % SIDE][y_step % SIDE]

    def device(self, dim, step):
        if dim == 'x':
            return (self.model, self.lines[step % SIDE])
        return (self.peer(step, 0) if dim == 'z' else self.peer(0, step), self.data)


class Copies:
    def __init__(self, send_sems, recv_sems):
        self.send_sems, self.recv_sems = send_sems, recv_sems
        self.names, self.batches = {}, {}

    def start(self, batch, name, src, dst, device):
        num = self.names.setdefault((batch, name), len(self.names))
        out = self.batches.setdefault(batch, len(self.batches))
        pltpu.make_async_remote_copy(src_ref=src, dst_ref=dst, send_sem=self.send_sems.at[out], recv_sem=self.recv_sems.at[num], device_id=device, device_id_type=MESH).start()

    def wait(self, batch, name, ref):
        num = self.names.setdefault((batch, name), len(self.names))
        pltpu.make_async_copy(ref, ref, self.recv_sems.at[num]).wait()

    def left(self, batch, ref):
        pltpu.make_async_copy(ref, ref, self.send_sems.at[self.batches[batch]]).wait()


def call_out(devices):
    for device in devices:
        pl.semaphore_signal(pltpu.get_barrier_semaphore(), inc=1, device_id=device, device_id_type=MESH)


def all_here(devices):
    pl.semaphore_wait(pltpu.get_barrier_semaphore(), len(devices))


def plane_gather(copies, batch, place, region, like, on_piece):
    def steps(order, first, second):
        return (second, first) if order == 0 else (first, second)

    def send(order, name, k, part, first, second):
        z_step, y_step = steps(order, *k)
        ref = region(place.at('z', z_step), place.at('y', y_step), order, *part)
        copies.start(batch, name, ref, ref, (place.peer(*steps(order, first, second)), place.data))

    whole, low, high = (0, 2), (0, 1), (1, 2)

    def spread(order, k):
        for step in BOTH_WAYS:
            send(order, ('b', order, k), (k, 0), whole, 0, step)

    def pass_on(order, k):
        copies.wait(batch, ('b', order, k), like(4))
        for step, part in ((-1, low), (1, high)) if k != 2 else ((1, whole),):
            send(order, ('end', k), (k, step), part, 0, -step)
        for step in BOTH_WAYS:
            on_piece(order, *steps(order, k, step))

    for order in ORDERS:
        for step in BOTH_WAYS:
            send(order, 'a', (0, 0), whole, step, 0)
    for order in ORDERS:
        spread(order, 0)
    yield
    copies.wait(batch, 'a', like(8))
    for order in ORDERS:
        for step, part in ((-1, low), (1, high)):
            send(order, ('across', order), (step, 0), part, -step, 0)
            on_piece(order, *steps(order, step, 0))
    yield
    for step in BOTH_WAYS:
        for order in ORDERS:
            spread(order, step)
    yield
    for order in ORDERS:
        pass_on(order, 0)
        yield
    for order in ORDERS:
        copies.wait(batch, ('across', order), like(2))
        spread(order, 2)
        on_piece(order, *steps(order, 2, 0))
        yield
    for k in (-1, 1, 2):
        for order in ORDERS:
            pass_on(order, k)
            yield
    for k in (0, -1, 1, 2):
        copies.wait(batch, ('end', k), like(4))
        for order in ORDERS:
            on_piece(order, *steps(order, k, 2))
        yield


STEPS = [(a, b) for a in range(SIDE) for b in range(SIDE) if (a, b) != (0, 0)]


def line_reduce(copies, batch, place, src, near, far, store):
    core = place.core
    half = near.shape[1] // 2
    low, high = pl.ds(0, half), pl.ds(half, half)
    here, right, across, left = [place.at('x', step) for step in range(SIDE)]
    copies.start((batch, 'near'), ONLY, src.at[:, 1 - core], near, place.mate)
    yield
    copies.wait((batch, 'near'), ONLY, near)
    near[across] = near[across] + src[across, core]
    copies.start((batch, 'half'), 1, near.at[across, low], far.at[0, low], place.device('x', 1))
    copies.start((batch, 'half'), -1, near.at[across, high], far.at[0, high], place.device('x', -1))
    for there in (right, left, here):
        near[there] = near[there] + src[there, core]
    yield
    copies.wait((batch, 'half'), 1, far.at[0, low])
    near[right, low] = near[right, low] + far[0, low]
    copies.start((batch, 'full'), 1, near.at[right], far.at[1], place.device('x', 1))
    copies.wait((batch, 'half'), -1, far.at[0, high])
    near[left, high] = near[left, high] + far[0, high]
    copies.start((batch, 'full'), -1, near.at[left], far.at[2], place.device('x', -1))
    yield
    copies.wait((batch, 'full'), 1, far.at[1])
    copies.wait((batch, 'full'), -1, far.at[2])
    store(near[here] + far[1] + far[2])
    copies.left((batch, 'near'), near)
    copies.left((batch, 'half'), far.at[0])
    copies.left((batch, 'full'), far.at[pl.ds(1, 2)])
    yield


def line_gather(copies, batch, place, out):
    core = place.core
    half = out.shape[2] // 2
    here, right, across, left = [out.at[place.at('x', step), core] for step in range(SIDE)]

    def hand(ref):
        copies.start((batch, 'hand'), ONLY, ref, ref, place.mate)

    for step in BOTH_WAYS:
        copies.start((batch, 'all'), step, here, here, place.device('x', step))
    hand(here)
    yield
    for step, ref, span in ((1, left, pl.ds(0, half)), (-1, right, pl.ds(half, half))):
        copies.wait((batch, 'all'), step, ref)
        copies.start((batch, 'all'), 2 * step, ref.at[span], ref.at[span], place.device('x', step))
        hand(ref)
    yield
    for step, span in ((1, pl.ds(0, half)), (-1, pl.ds(half, half))):
        copies.wait((batch, 'all'), 2 * step, across.at[span])
    hand(across)
    yield
    copies.wait((batch, 'hand'), ONLY, out.at[:, 0])
    copies.left((batch, 'all'), out.at[0:3, 0])
    copies.left((batch, 'hand'), out.at[:, 0])
    yield


BALANCED = (('x', 'y', 'z'), ('y', 'z', 'x'), ('z', 'x', 'y'))
X_LAST = (('y', 'z', 'x'), ('z', 'y', 'x'))


def cube_gather(copies, batch, place, view, cuts, orders):
    core = place.core
    parts = [(order, pl.ds(start, end - start)) for order, start, end in zip(orders, cuts[:-1], cuts[1:])]
    every, low, high = (0, SIDE), (0, 2), (2, 2)

    def like(z, y, x):
        return view(0, *[pl.ds(0, num) if num > 1 else 0 for num in (z, y, x)], pl.ds(0, cuts[-1]))

    def at(order, cols, places):
        where = dict(zip(order, places))
        return view(core, where['z'], where['y'], where['x'], cols)

    def single(order, cols, step):
        return at(order, cols, (place.at(order[0], step), place.at(order[1], 0), place.at(order[2], 0)))

    def group(order, cols, a, b, span=every):
        return at(order, cols, (pl.ds(*span), place.at(order[1], a), place.at(order[2], b)))

    def hand(order, cols, a, b):
        ref = group(order, cols, a, b)
        copies.start((batch, 'mate'), ONLY, ref, ref, place.mate)

    def spread(order, cols, a):
        ref = group(order, cols, a, 0)
        for step in BOTH_WAYS:
            copies.start((batch, 'three'), a, ref, ref, place.device(order[2], step))
        hand(order, cols, a, 0)

    def pass_on(a):
        copies.wait((batch, 'three'), a, like(1, 2, SIDE))
        for order, cols in parts:
            for step, span in ((-1, low), (1, high)):
                half = group(order, cols, a, step, span)
                copies.start((batch, 'three'), ('end', a), half, half, place.device(order[2], -step))
                hand(order, cols, a, step)

    for order, cols in parts:
        for step in (2, 1, -1):
            copies.start((batch, 'one'), ONLY, single(order, cols, 0), single(order, cols, 0), place.device(order[0], step))
    yield
    copies.wait((batch, 'one'), ONLY, like(1, 1, 3))
    for order, cols in parts:
        for step in BOTH_WAYS:
            copies.start((batch, 'two'), ONLY, group(order, cols, 0, 0), group(order, cols, 0, 0), place.device(order[1], step))
    for order, cols in parts:
        spread(order, cols, 0)
    yield
    copies.wait((batch, 'two'), ONLY, like(1, 2, SIDE))
    for order, cols in parts:
        for step, span in ((-1, low), (1, high)):
            half = group(order, cols, step, 0, span)
            copies.start((batch, 'two'), 'end', half, half, place.device(order[1], -step))
    for order, cols in parts:
        for step in BOTH_WAYS:
            spread(order, cols, step)
    yield
    pass_on(0)
    yield
    copies.wait((batch, 'two'), 'end', like(1, 1, SIDE))
    for order, cols in parts:
        spread(order, cols, 2)
    yield
    for a in (-1, 1, 2):
        pass_on(a)
        yield
    for a in (0, -1, 1, 2):
        copies.wait((batch, 'three'), ('end', a), like(1, 1, SIDE))
        for order, cols in parts:
            hand(order, cols, a, 2)
        yield
    copies.wait((batch, 'mate'), ONLY, like(SIDE, SIDE, SIDE))
    copies.left((batch, 'mate'), like(SIDE, SIDE, SIDE))
    copies.left((batch, 'one'), like(1, 1, 3))
    copies.left((batch, 'two'), like(1, 3, SIDE))
    copies.left((batch, 'three'), like(3, SIDE, SIDE))
    yield


def pump(gen, name):
    with scope(name):
        next(gen, None)


def drain(gen, name):
    with scope(name):
        for _ in gen:
            pass


def step_kernel(scale, x_hbm, dy_hbm, w_col_hbm, w_row_hbm, a_old, s_old, a_inv, s_inv, fact, grads, w_col, w_row, x_buf, dy_buf, h_two, w_two, w_three, z_one, h_one, h_three,
                g_three, t_three, rows_buf, z_two, left, w_three_t, gram_src, gram_near, gram_far, old_buf, piece_buf, grad_src, grad_near,
                grad_far, grad_sum, grad_out, big_buf, load_sems, old_sems, big_sems, send_sems, recv_sems):
    place = Place()
    model_id, data_id, core = place.model, place.data, place.core
    spot, y_pos, z_pos = place.at('x', 0), place.at('y', 0), place.at('z', 0)
    copies = Copies(send_sems, recv_sems)
    my_rows = span_of(model_id, BLOCK)
    my_cols = span_of(model_id, BLOCK)
    my_part = pl.ds(pl.multiple_of(data_id * PIECE, PIECE), PIECE)
    g_one = t_three
    olds = [a_old.at[0], s_old.at[1], a_old.at[1], s_old.at[0]]
    chunk = 256
    n_chunks = WIDTH // chunk
    met = [(place.peer(a, b), data_id) for a, b in STEPS] + [place.mate] + [place.device('x', step) for step in (1, 2, 3)]

    def load(src, dst, base, i):
        rows = span_of(i, chunk)
        return pltpu.make_async_copy(src.at[rows, :], dst.at[rows, :], load_sems.at[base + i])

    def load_x(i):
        return load(x_hbm, x_buf, 0, i)

    def load_dy(i):
        return load(dy_hbm, dy_buf, n_chunks, i)

    def load_old(mat, j):
        rows = pl.ds(pl.multiple_of(model_id * BLOCK + data_id * PIECE, PIECE), PIECE)
        cols = span_of(lax.rem(model_id + j, PLANE), BLOCK)
        return pltpu.make_async_copy(olds[mat].at[rows, cols], old_buf.at[mat, :, pl.ds(j * BLOCK, BLOCK)], old_sems.at[mat])

    def cols_of(buf, cols):
        return buf[:, cols] if len(buf.shape) == 2 else buf[:, :, :, :, :, cols].reshape(WIDTH, cols.size)

    def rows_of(buf, z_step, y_step):
        return buf[place.at('z', z_step), place.at('y', y_step)].reshape(BLOCK, WIDTH)

    call_out(met)
    own_w_two = pltpu.make_async_copy(w_row_hbm.at[0, my_part, :], w_two.at[z_pos, y_pos, spot, core], old_sems.at[4])
    own_w_two.start()
    load_w = [pltpu.make_async_copy(w_col_hbm, w_col, big_sems.at[0]), pltpu.make_async_copy(w_row_hbm, w_row, big_sems.at[1])]
    for move in load_w:
        move.start()
    for i in range(n_chunks):
        load_x(i).start()

    def z_one_step(i, carry):
        rows = span_of(i, chunk)
        load_x(i).wait()
        pre_act = matmul(x_buf[rows, :], w_col[0]).astype(jnp.bfloat16)
        z_one[rows, :] = pre_act
        h_one[rows, :] = activate(pre_act)
        return carry

    own_w_two.wait()
    with scope('greet'):
        all_here(met)

    def z_one_first():
        with scope('z1a'):
            for move in load_w:
                move.wait()
            w_three_t[...] = w_col[1].T
            w_three[z_pos, y_pos, spot, core] = w_three_t[my_part, :]
            lax.fori_loop(0, n_chunks // 2, z_one_step, 0)
        for i in range(n_chunks):
            load_dy(i).start()
        for mat in range(4):
            for j in range(TRI):
                load_old(mat, j).start()

    def weight_thread(batch, buf, cuts, orders):
        def view(which, z, y, x, cols):
            return buf.at[z, y, x, which, :, cols]
        return cube_gather(copies, batch, place, view, cuts, orders)

    def z_one_rest():
        with scope('z1b'):
            lax.fori_loop(n_chunks // 2, n_chunks, z_one_step, 0)

    def send_block(batch, cols_ref, a, b):
        peer = place.peer(a, b)
        copies.start(batch, ONLY, cols_ref.at[span_of(peer, BLOCK), :], rows_buf.at[:, my_cols], (peer, data_id))

    def wait_blocks(batch):
        others = rows_buf.at[:, 0:WIDTH - BLOCK]
        copies.wait(batch, ONLY, others)
        copies.left(batch, others)

    loaded = []

    def wait_dy():
        if not loaded:
            for i in range(n_chunks):
                load_dy(i).wait()
            loaded.append(True)

    def t_three_step(i, carry):
        rows = span_of(i, chunk)
        t_three[rows, :] = matmul_nt(dy_buf[rows, :], w_row[1]).astype(jnp.bfloat16)
        return carry

    def t_three_part(num):
        wait_dy()
        with scope('t3'):
            lax.fori_loop(num * n_chunks // 4, (num + 1) * n_chunks // 4, t_three_step, 0)

    def turn(dst, src, cols):
        for i in range(4):
            rows = slice(i * 512, (i + 1) * 512)
            dst[:, rows] = (src[rows, cols] if len(src.shape) == 2 else src[i, :, :, :, :, cols].reshape(512, BLOCK)).T

    def gram_product(mat, lhs, right):
        def block_cols(j):
            return cols_of(right, span_of(lax.rem(model_id + j, PLANE), BLOCK))

        def gram_step(i, carry):
            block = matmul(lhs[...], jnp.concatenate([block_cols(2 * i), block_cols(2 * i + 1)], axis=1))
            gram_src[mat, :, :, :, span_of(i, chunk)] = block.reshape(SIDE, CORES, PIECE, chunk)
            return carry
        lax.fori_loop(0, TRI // 2, gram_step, 0)
        block = matmul(lhs[...], block_cols(TRI - 1))
        gram_src[mat, :, :, :, (TRI - 1) * BLOCK:] = block.reshape(SIDE, CORES, PIECE, BLOCK)

    def grad_product(lhs, right, same, slot):
        def grad_step(i, carry):
            cols = span_of(i, chunk)
            block = matmul(lhs[...], cols_of(right, cols))
            grad_src[slot, :, :, :, cols] = block.reshape(SIDE, CORES, PIECE, chunk)
            return carry
        lax.fori_loop(0, n_chunks, grad_step, 0)
        block = matmul(lhs[...], same[...])
        grad_src[slot, :, :, :, WIDTH:GRAD_COLS] = block.reshape(SIDE, CORES, PIECE, BLOCK)

    def store_factor(mat, total):
        pltpu.make_async_copy(old_buf.at[mat], old_buf.at[mat], old_sems.at[mat]).wait()
        mixed = FACTOR_DECAY * old_buf[mat] + scale * total
        piece_buf[mat] = mixed

    def sum_thread(mat):
        return line_reduce(copies, ('gram', mat), place, gram_src.at[mat], gram_near.at[mat], gram_far.at[mat], functools.partial(store_factor, mat))

    def factor_thread(first, count, cuts, orders):
        mats = pl.ds(first, count)

        def view(which, z, y, x, cols):
            return fact.at[z, y, x, which, mats, :, cols]

        move = pltpu.make_async_copy(piece_buf.at[mats], fact.at[z_pos, y_pos, spot, core, mats], old_sems.at[4])
        move.start()
        move.wait()
        yield from cube_gather(copies, ('fact', first), place, view, cuts, orders)

    def gram_job(mat, slot, right):
        if mat == 1:
            wait_dy()
        with scope('gram'):
            turn(left.at[slot], right, my_cols)
            gram_product(mat, left.at[slot], right)

    def grad_job(layer, slot, lhs, right):
        with scope('dW'):
            turn(left.at[slot], lhs, slice(0, BLOCK))
            grad_product(left.at[slot], right, lhs, layer % 2)
        if layer == 0:
            load_big(0, 0).start()
            load_big(0, 1).start()

    def swap_first():
        for a, b in STEPS:
            send_block('h1', h_one, a, b)
        rows_buf[:, my_cols] = h_one[my_rows, :]

    def z_two_step(i, carry):
        cols = span_of(i, chunk)
        pre_act = matmul(rows_buf[...], cols_of(w_two, cols)).astype(jnp.bfloat16)
        z_two[:, cols] = pre_act
        h_two[z_pos, y_pos, :, :, :, cols] = activate(pre_act).reshape(SIDE, CORES, PIECE, chunk)
        return carry

    def second_forward():
        drain(threads['w2'], 'w2_rest')
        with scope('wait_h1'):
            wait_blocks('h1')
        with scope('z2'):
            lax.fori_loop(0, n_chunks, z_two_step, 0)

    def forward_block(a, b):
        rows = span_of(place.peer(a, b), BLOCK)
        pre_act = matmul(rows_of(h_two, a, b), w_col[1]).astype(jnp.bfloat16)
        h_three[rows, :] = activate(pre_act)
        g_three[rows, :] = back_gate(t_three[rows, :], pre_act)
        if (a, b) != (0, 0):
            send_block('g3', g_three, a, b)

    def backward_block(a, b):
        rows = span_of(place.peer(a, b), BLOCK)
        grad = matmul_nt(rows_of(w_two, a, b), w_row[0]).astype(jnp.bfloat16)
        g_one[rows, :] = back_gate(grad, z_one[rows, :])

    def gather_tokens(tag, buf, block_step):
        seen = {}

        def on_piece(order, first, second):
            where = (first % SIDE, second % SIDE)
            seen[where] = seen.get(where, 0) + 1

        def region(z, y, order, lo, hi):
            return buf.at[z, y, pl.ds(2 * order + lo, hi - lo)]

        def like(quarters):
            return x_buf.at[0:quarters * BLOCK // 4, :]

        done = {(0, 0)}
        gen = plane_gather(copies, tag, place, region, like, on_piece)
        next(gen)
        with scope(tag + '_blocks'):
            block_step(0, 0)
        yield
        for _ in gen:
            ready = [where for where in sorted(seen) if seen[where] == 2 and where not in done]
            with scope(tag + '_blocks'):
                for where in ready:
                    block_step(*where)
            done.update(ready)
            yield
        copies.left(tag, x_buf.at[0:WIDTH - BLOCK, :])

    def split(value):
        high = value.astype(jnp.bfloat16)
        rest = value - high.astype(jnp.float32)
        middle = rest.astype(jnp.bfloat16)
        return high, middle, (rest - middle.astype(jnp.float32)).astype(jnp.bfloat16)

    inverses = [s_inv.at[1], a_inv.at[1], s_inv.at[0], a_inv.at[0]]
    big_rows = 2 * PIECE

    def load_big(layer, i):
        slot = lax.rem(i, 2)
        return pltpu.make_async_copy(inverses[layer].at[span_of(i, chunk), span_of(core, HALF)], big_buf.at[slot], big_sems.at[slot])

    def grad_thread(layer):
        sum_ref, out_ref, tag = grad_sum.at[layer], grad_out.at[layer], ('grad', layer)

        def keep_sum(total):
            sum_ref[core] = total

        def big_step(i, carry):
            load_big(layer, i).wait()
            lhs = jnp.concatenate(split(sum_ref[:, :, span_of(i, chunk)].reshape(big_rows, chunk)), axis=0)
            high, middle, low = split(big_buf[lax.rem(i, 2)])
            by_high, by_middle, by_low = matmul(lhs, high), matmul(lhs[:2 * big_rows], middle), matmul(lhs[:big_rows], low)
            small = by_high[2 * big_rows:] + by_middle[big_rows:] + by_low
            out_ref[:, :HALF] += by_high[:big_rows] + (by_high[big_rows:2 * big_rows] + by_middle[:big_rows] + small)

            @pl.when(i + 2 < n_chunks)
            def _():
                load_big(layer, i + 2).start()
            if layer < 3:
                @pl.when(i + 2 >= n_chunks)
                def _():
                    load_big(layer + 1, i + 2 - n_chunks).start()
            return carry

        yield from line_reduce(copies, tag, place, grad_src.at[layer % 2], grad_near.at[layer], grad_far.at[layer], keep_sum)
        copies.start(tag + ('pair',), ONLY, sum_ref.at[core], sum_ref.at[core], place.mate)
        yield
        copies.wait(tag + ('pair',), ONLY, sum_ref.at[1 - core])
        copies.left(tag + ('pair',), sum_ref.at[0])
        out_ref[...] = jnp.concatenate([jnp.zeros((big_rows, HALF), jnp.float32), sum_ref[:, :, WIDTH:].reshape(big_rows, BLOCK)], axis=1)
        with scope('X'):
            lax.fori_loop(0, n_chunks // 2, big_step, 0)
        yield
        with scope('X'):
            lax.fori_loop(n_chunks // 2, n_chunks, big_step, 0)
        move = pltpu.make_async_copy(out_ref, grads.at[layer, spot, core], old_sems.at[5])
        move.start()
        move.wait()
        yield from line_gather(copies, tag, place, grads.at[layer])

    def g_two_step(i, carry):
        cols = span_of(i, chunk)
        grad = matmul(rows_buf[...], cols_of(w_three, cols)).astype(jnp.bfloat16)
        w_two[z_pos, y_pos, :, :, :, cols] = back_gate(grad, z_two[:, cols]).reshape(SIDE, CORES, PIECE, chunk)
        return carry

    def second_backward():
        drain(threads['w3'], 'w3_rest')
        with scope('wait_g3'):
            wait_blocks('g3')
            rows_buf[:, my_cols] = g_three[my_rows, :]
        with scope('g2'):
            lax.fori_loop(0, n_chunks, g_two_step, 0)

    threads = dict(
        w2=weight_thread('w2', w_two, W_TWO_CUTS, BALANCED),
        w3=weight_thread('w3', w_three, W_THREE_CUTS, MOSTLY_X),
        h2=gather_tokens('h2', h_two, forward_block),
        g2=gather_tokens('g2', w_two, backward_block),
        pair=factor_thread(0, 2, PAIR_CUTS, MOSTLY_X),
        fa3=factor_thread(2, 1, LATE_CUTS, BALANCED),
        fs2=factor_thread(3, 1, LATE_CUTS, BALANCED),
        sum0=sum_thread(0), sum1=sum_thread(1), sum2=sum_thread(2), sum3=sum_thread(3),
        grad4=grad_thread(0), grad3=grad_thread(1), grad2=grad_thread(2), grad1=grad_thread(3),
    )
    steps = {name: functools.partial(pump, thread, name) for name, thread in threads.items()}
    steps.update(
        z0=z_one_first, z1=z_one_rest, swap=swap_first, z2=second_forward, back=second_backward,
        A1=functools.partial(gram_job, 0, 0, x_buf), S4=functools.partial(gram_job, 1, 1, dy_buf),
        A3=functools.partial(gram_job, 2, 0, h_two), S2=functools.partial(gram_job, 3, 0, w_two),
        dW4=functools.partial(grad_job, 0, 1, h_three, dy_buf), dW3=functools.partial(grad_job, 1, 0, g_three, h_two),
        dW2=functools.partial(grad_job, 2, 0, h_one, w_two), dW1=functools.partial(grad_job, 3, 1, g_one, x_buf),
        t0=functools.partial(t_three_part, 0), t1=functools.partial(t_three_part, 1),
        t2=functools.partial(t_three_part, 2), t3=functools.partial(t_three_part, 3),
    )
    for step in plan(**steps):
        step()
    for name, thread in threads.items():
        drain(thread, name)
    assert len(copies.batches) == N_BATCHES and len(copies.names) == N_COPIES, (len(copies.batches), len(copies.names))


W_TWO_CUTS = (0, 384, 1536, 2048)
W_THREE_CUTS = (0, 1152, 1920, 2048)
PAIR_CUTS = (0, 384, 1024, 1152)
LATE_CUTS = (0, 512, 640, 1152)
MOSTLY_X = (('y', 'z', 'x'), ('z', 'y', 'x'), ('x', 'y', 'z'))


def plan(w2, w3, h2, g2, pair, fa3, fs2, sum0, sum1, sum2, sum3, grad4, grad3, grad2, grad1, z0, z1, swap, z2, back, A1, S4, A3, S2, dW4, dW3, dW2, dW1, t0, t1, t2, t3):
    return (
        w2, z0, w2, t3, w3, t2, w2, z1, w2, A1, w2, t0, swap, S4, sum1, sum0, w2, sum0, w2, w2, w2, t1, sum1, w3, w2, w2, sum0, w2, sum1, w3, w2, z2,
        h2, sum0, sum1, w3, pair, h2, h2, w3, pair, h2, w3, h2, h2, h2, h2, w3, w3, h2, h2, w3, h2, pair, h2, w3, w3, h2, w3, h2, h2, h2, w3, h2,
        pair, pair, A3, sum2, dW3, pair, back, g2, g2, dW4, grad3, grad4, g2, g2, sum2, grad3, g2, g2, grad4, pair, sum2, g2, grad4, grad3, g2, sum2,
        g2, grad4, fa3, grad4, g2, grad4, grad3, g2, g2, pair, grad3, grad4, g2, g2, grad3, g2, pair, fa3, g2, pair, grad3, g2, S2, fa3, sum3, dW2,
        sum3, grad4, grad2, fa3, sum3, pair, grad2, fa3, dW1, sum3, fa3, grad1, fs2, grad2, grad1, fs2, grad2, grad2, grad1, grad3, pair, grad2, fa3,
        fs2, fa3, fs2, grad1, grad1, pair, grad2, grad1, fs2, grad1, grad4, fa3, fa3, grad3, fs2, fa3, fs2, grad4, grad2, fs2, grad1, fs2, fs2, fa3,
        fs2, grad2, grad3, fs2, grad1, fs2, grad2, fa3, grad1,
    )


N_BATCHES = 60
N_COPIES = 156


def step_call(x_tokens, dy_tokens, w_col, w_row, a_old, s_old, a_inv, s_inv, scale):
    f32, bf16 = jnp.float32, jnp.bfloat16
    tall, wide = (WIDTH, BLOCK), (BLOCK, WIDTH)
    cube = (SIDE, SIDE, SIDE, 2)
    rows = 2 * PIECE
    hbm = pl.BlockSpec(memory_space=pl.ANY)
    scratch = [pltpu.VMEM((2,) + tall, bf16), pltpu.VMEM((2,) + wide, bf16)] + [pltpu.VMEM((WIDTH, WIDTH), bf16)] * 2 + [pltpu.VMEM(cube + (PIECE, WIDTH), bf16)] * 3
    scratch += [pltpu.VMEM(tall, bf16)] * 5 + [pltpu.VMEM(wide, bf16)] * 2 + [pltpu.VMEM((2,) + wide, bf16), pltpu.VMEM(wide, bf16)]
    scratch += [pltpu.VMEM((4, SIDE, CORES, PIECE, TRI * BLOCK), f32), pltpu.VMEM((4, SIDE, PIECE, TRI * BLOCK), f32), pltpu.VMEM((4, 3, PIECE, TRI * BLOCK), f32)]
    scratch += [pltpu.VMEM((4, PIECE, TRI * BLOCK), f32), pltpu.VMEM((4, PIECE, FACTOR_COLS), f32)]
    scratch += [pltpu.VMEM((2, SIDE, CORES, PIECE, GRAD_COLS), f32), pltpu.VMEM((4, SIDE, PIECE, GRAD_COLS), f32), pltpu.VMEM((4, 3, PIECE, GRAD_COLS), f32)]
    scratch += [pltpu.VMEM((4, 2, PIECE, GRAD_COLS), f32), pltpu.VMEM((4, rows, HALF + BLOCK), f32), pltpu.VMEM((2, 256, HALF), f32)]
    scratch += [pltpu.SemaphoreType.DMA((num,)) for num in (16, 6, 2, N_BATCHES, N_COPIES)]
    return pl.pallas_call(
        functools.partial(step_kernel, scale),
        out_shape=[jax.ShapeDtypeStruct(cube + (4, PIECE, FACTOR_COLS), f32), jax.ShapeDtypeStruct((4, SIDE, 2, rows, HALF + BLOCK), f32)],
        in_specs=[hbm] * 8,
        out_specs=[hbm, hbm],
        scratch_shapes=scratch,
        compiler_params=pltpu.CompilerParams(collective_id=0, has_side_effects=True, vmem_limit_bytes=67043328),
        name='step',
    )(x_tokens, dy_tokens, w_col, w_row, a_old, s_old, a_inv, s_inv)


def finish_kernel(scale, inv_rows, fact, grads, s_old_col, a_old_row, s_inv_col, a_inv_row, a_new, s_new, u_col, u_row, s_new_col, a_new_row, buf, turned, sums, u_col_buf, u_row_buf, load_sems, out_sems, turn_sems, small_sems):
    outs = [(a_new, 0), (s_new, 1), (a_new, 1), (s_new, 0)]

    def load(mat, row):
        z, y = lax.div(row, SIDE), lax.rem(row, SIDE)
        return pltpu.make_async_copy(fact.at[z, y, :, :, mat], buf.at[mat, row], load_sems.at[mat * PLANE + row])

    def turn_done(slot):
        return pltpu.make_async_copy(turned.at[slot], turned.at[slot], turn_sems.at[slot])

    def start_load(mat):
        def body(row, carry):
            load(mat, row).start()
            return carry
        lax.fori_loop(0, PLANE, body, 0)

    load_sums = pltpu.make_async_copy(grads, sums, out_sems.at[4])
    load_sums.start()
    for mat in range(4):
        start_load(mat)
    half = HALF

    def new_blocks():
        load_sums.wait()
        for layer in range(4):
            block, num = scale * sums[layer, :, 0, :, half:].reshape(BLOCK, BLOCK), 1 - layer // 2
            if layer % 2 == 1:
                s_new_col[num] = FACTOR_DECAY * s_old_col[num] + block
            else:
                a_new_row[num] = FACTOR_DECAY * a_old_row[num] + block

    def move_small(batch):
        moves = [(u_col_buf, u_col), (u_row_buf, u_row)]
        return [pltpu.make_async_copy(src.at[1 - batch], dst.at[1 - batch], small_sems.at[2 * batch + num]) for num, (src, dst) in enumerate(moves)]

    chunk = 2 * BLOCK

    def small_product(layer, i):
        num = 1 - layer // 2
        core, cols, out = lax.div(i, SIDE), span_of(lax.rem(i, SIDE), chunk), span_of(i, chunk)
        product = sums[layer, :, core, :, cols].reshape(BLOCK, chunk)
        if layer % 2 == 1:
            u_col_buf[num, out, :] = exact_dot(product.T, s_inv_col[num]) * inv_rows
        else:
            u_row_buf[num, :, out] = exact_dot(a_inv_row[num], product) * inv_rows

    for mat, (out, num) in enumerate(outs):
        def row_step(row, carry):
            load(mat, row).wait()
            slot = lax.rem(row, 2)
            if mat in (1, 2):
                @pl.when(row < PLANE // 2)
                def _():
                    small_product(2 * mat - 2, row)

                @pl.when(row >= PLANE // 2)
                def _():
                    small_product(2 * mat - 1, row - PLANE // 2)
            for j in range(TRI):
                cols = span_of(lax.rem(row + j, PLANE), BLOCK)
                pltpu.make_async_copy(buf.at[mat, row, :, :, :, pl.ds(j * BLOCK, BLOCK)], out.at[num, row, :, :, :, cols], out_sems.at[mat]).start()
            if mat > 0:
                turn_done(slot).wait()
            else:
                @pl.when(row >= 2)
                def _():
                    turn_done(slot).wait()
            for j in range(1, TRI - 1):
                other = lax.rem(row + j, PLANE)
                block = buf[mat, row, :, :, :, j * BLOCK:(j + 1) * BLOCK].reshape(BLOCK, BLOCK).T
                turned[slot, j - 1] = block.reshape(SIDE, CORES, PIECE, BLOCK)
                pltpu.make_async_copy(turned.at[slot, j - 1], out.at[num, other, :, :, :, span_of(row, BLOCK)], turn_sems.at[slot]).start()
            return carry

        if mat == 1:
            new_blocks()
        lax.fori_loop(0, PLANE, row_step, 0)
        if mat in (1, 2):
            for move in move_small(mat - 1):
                move.start()
    for batch in range(2):
        for move in move_small(batch):
            move.wait()
    for slot in range(2):
        turn_done(slot).wait()
    for mat in range(4):
        pltpu.make_async_copy(buf.at[mat], buf.at[mat], out_sems.at[mat]).wait()


def finish_call(fact, grads, s_old_col, a_old_row, s_inv_col, a_inv_row, scale, inv_rows):
    f32 = jnp.float32
    shapes = [(2, PLANE, SIDE, CORES, PIECE, WIDTH)] * 2 + [(2, WIDTH, BLOCK), (2, BLOCK, WIDTH)] + [(2, BLOCK, BLOCK)] * 2
    hbm, vmem = pl.BlockSpec(memory_space=pl.ANY), pl.BlockSpec(memory_space=pltpu.VMEM)
    return pl.pallas_call(
        functools.partial(finish_kernel, scale, inv_rows),
        out_shape=[jax.ShapeDtypeStruct(shape, f32) for shape in shapes],
        in_specs=[hbm] * 2 + [vmem] * 4,
        out_specs=[hbm] * 4 + [vmem] * 2,
        scratch_shapes=[pltpu.VMEM((4, PLANE, SIDE, CORES, PIECE, FACTOR_COLS), f32), pltpu.VMEM((2, TRI - 2, SIDE, CORES, PIECE, BLOCK), f32), pltpu.VMEM(grads.shape, f32), pltpu.VMEM((2, WIDTH, BLOCK), f32), pltpu.VMEM((2, BLOCK, WIDTH), f32)] + [pltpu.SemaphoreType.DMA((num,)) for num in (4 * PLANE, 5, 2, 4)],
        compiler_params=pltpu.CompilerParams(vmem_limit_bytes=67043328),
        name='finish',
    )(fact, grads, s_old_col, a_old_row, s_inv_col, a_inv_row)


def solution(mesh):
    def shard_body(x_tokens, dy_tokens, w_col, w_row, a_old_col, s_old_col, a_old_row, s_old_row, a_inv_col, s_inv_col, a_inv_row, s_inv_row):
        inv_rows = 1.0 / (x_tokens.shape[0] * DATA_WAYS)
        scale = (1.0 - FACTOR_DECAY) * inv_rows
        fact, grads = step_call(x_tokens, dy_tokens, w_col, w_row, a_old_col, s_old_row, a_inv_col, s_inv_row, scale)
        a_new_col, s_new_row, u_col, u_row, s_new_col, a_new_row = finish_call(fact, grads, s_old_col, a_old_row, s_inv_col, a_inv_row, scale, inv_rows)
        return (u_col, u_row, a_new_col.reshape(2, WIDTH, WIDTH), s_new_col, a_new_row, s_new_row.reshape(2, WIDTH, WIDTH))

    batch_split = P('data', None)
    col_split = P(None, None, 'model')
    row_split = P(None, 'model', None)
    replicated = P()
    return jax.shard_map(
        shard_body,
        mesh=mesh,
        in_specs=(batch_split, batch_split, col_split, row_split, replicated, row_split, row_split, replicated, replicated, row_split, row_split, replicated),
        out_specs=(col_split, row_split, replicated, row_split, row_split, replicated),
        check_vma=False,
    )
```

```python
import contextlib
import functools
import math
import jax
import jax.numpy as jnp
from jax import lax
from jax.experimental import pallas as pl
from jax.experimental.pallas import tpu as pltpu
from jax.sharding import PartitionSpec as P

FACTOR_DECAY = 0.8
GELU_SCALE = math.sqrt(2.0 / math.pi)
GELU_CUBIC = 0.044715
EXACT = lax.Precision.HIGHEST
MESH = pl.DeviceIdType.MESH
SIDE = 4
PLANE = 16
DATA_WAYS = 8
WIDTH = 2048
BLOCK = 128
PIECE = 16
TRI = 9
ONLY = 0
CORES = 2
BOTH_WAYS = (1, -1)
ORDERS = (0, 1)
HALF = WIDTH // 2
SCOPED = False
FACTOR_COLS = TRI * BLOCK
GRAD_COLS = WIDTH + BLOCK
NT_DIMS = (((1,), (1,)), ((), ()))


def gelu_value(pre_act):
    tanh_arg = GELU_SCALE * (pre_act + GELU_CUBIC * pre_act * pre_act * pre_act)
    return 0.5 * pre_act * (1.0 + jnp.tanh(tanh_arg))


def gelu_slope(pre_act):
    tanh_arg = GELU_SCALE * (pre_act + GELU_CUBIC * pre_act * pre_act * pre_act)
    tanh_val = jnp.tanh(tanh_arg)
    return 0.5 * (1.0 + tanh_val) + 0.5 * pre_act * (1.0 - tanh_val * tanh_val) * GELU_SCALE * (1.0 + 3.0 * GELU_CUBIC * pre_act * pre_act)


def activate(pre_act):
    return gelu_value(pre_act.astype(jnp.float32)).astype(jnp.bfloat16)


def back_gate(grad_act, pre_act):
    return (grad_act.astype(jnp.float32) * gelu_slope(pre_act.astype(jnp.float32))).astype(jnp.bfloat16)


def matmul(left_mat, right_mat):
    return jnp.dot(left_mat, right_mat, preferred_element_type=jnp.float32)


def matmul_nt(left_mat, right_mat):
    return lax.dot_general(left_mat, right_mat, NT_DIMS, preferred_element_type=jnp.float32)


def exact_dot(left_mat, right_mat):
    return jnp.dot(left_mat, right_mat, precision=EXACT, preferred_element_type=jnp.float32)


def scope(name):
    return jax.named_scope(name) if SCOPED else contextlib.nullcontext()


def span_of(index, size):
    return pl.ds(pl.multiple_of(index * size, size), size)


class Place:
    def __init__(self):
        self.model, self.data = lax.axis_index('model'), lax.axis_index('data')
        self.core = lax.rem(self.data, 2)
        here = {'x': lax.div(self.data, 2), 'y': lax.rem(self.model, SIDE), 'z': lax.div(self.model, SIDE)}
        self.along = {dim: [at] + [lax.rem(at + step, SIDE) for step in range(1, SIDE)] for dim, at in here.items()}
        self.planes = [[z * SIDE + y for y in self.along['y']] for z in self.along['z']]
        self.lines = [x * 2 + self.core for x in self.along['x']]
        self.mate = (self.model, self.data + 1 - 2 * self.core)

    def at(self, dim, step):
        return self.along[dim][step % SIDE]

    def peer(self, z_step, y_step):
        return self.planes[z_step % SIDE][y_step % SIDE]

    def device(self, dim, step):
        if dim == 'x':
            return (self.model, self.lines[step % SIDE])
        return (self.peer(step, 0) if dim == 'z' else self.peer(0, step), self.data)


class Copies:
    def __init__(self, send_sems, recv_sems):
        self.send_sems, self.recv_sems = send_sems, recv_sems
        self.names, self.batches = {}, {}

    def start(self, batch, name, src, dst, device):
        num = self.names.setdefault((batch, name), len(self.names))
        out = self.batches.setdefault(batch, len(self.batches))
        pltpu.make_async_remote_copy(src_ref=src, dst_ref=dst, send_sem=self.send_sems.at[out], recv_sem=self.recv_sems.at[num], device_id=device, device_id_type=MESH).start()

    def wait(self, batch, name, ref):
        num = self.names.setdefault((batch, name), len(self.names))
        pltpu.make_async_copy(ref, ref, self.recv_sems.at[num]).wait()

    def left(self, batch, ref):
        pltpu.make_async_copy(ref, ref, self.send_sems.at[self.batches[batch]]).wait()


def call_out(devices):
    for device in devices:
        pl.semaphore_signal(pltpu.get_barrier_semaphore(), inc=1, device_id=device, device_id_type=MESH)


def all_here(devices):
    pl.semaphore_wait(pltpu.get_barrier_semaphore(), len(devices))


def plane_gather(copies, batch, place, region, like, on_piece):
    def steps(order, first, second):
        return (second, first) if order == 0 else (first, second)

    def send(order, name, k, part, first, second):
        z_step, y_step = steps(order, *k)
        ref = region(place.at('z', z_step), place.at('y', y_step), order, *part)
        copies.start(batch, name, ref, ref, (place.peer(*steps(order, first, second)), place.data))

    whole, low, high = (0, 2), (0, 1), (1, 2)

    def spread(order, k):
        for step in BOTH_WAYS:
            send(order, ('b', order, k), (k, 0), whole, 0, step)

    def pass_on(order, k):
        copies.wait(batch, ('b', order, k), like(4))
        for step, part in ((-1, low), (1, high)) if k != 2 else ((1, whole),):
            send(order, ('end', k), (k, step), part, 0, -step)
        for step in BOTH_WAYS:
            on_piece(order, *steps(order, k, step))

    for order in ORDERS:
        for step in BOTH_WAYS:
            send(order, 'a', (0, 0), whole, step, 0)
    for order in ORDERS:
        spread(order, 0)
    yield
    copies.wait(batch, 'a', like(8))
    for order in ORDERS:
        for step, part in ((-1, low), (1, high)):
            send(order, ('across', order), (step, 0), part, -step, 0)
            on_piece(order, *steps(order, step, 0))
    yield
    for step in BOTH_WAYS:
        for order in ORDERS:
            spread(order, step)
    yield
    for order in ORDERS:
        pass_on(order, 0)
        yield
    for order in ORDERS:
        copies.wait(batch, ('across', order), like(2))
        spread(order, 2)
        on_piece(order, *steps(order, 2, 0))
        yield
    for k in (-1, 1, 2):
        for order in ORDERS:
            pass_on(order, k)
            yield
    for k in (0, -1, 1, 2):
        copies.wait(batch, ('end', k), like(4))
        for order in ORDERS:
            on_piece(order, *steps(order, k, 2))
        yield


STEPS = [(a, b) for a in range(SIDE) for b in range(SIDE) if (a, b) != (0, 0)]


def line_reduce(copies, batch, place, src, near, far, store):
    core = place.core
    half = near.shape[1] // 2
    low, high = pl.ds(0, half), pl.ds(half, half)
    here, right, across, left = [place.at('x', step) for step in range(SIDE)]
    copies.start((batch, 'near'), ONLY, src.at[:, 1 - core], near, place.mate)
    yield
    copies.wait((batch, 'near'), ONLY, near)
    near[across] = near[across] + src[across, core]
    copies.start((batch, 'half'), 1, near.at[across, low], far.at[0, low], place.device('x', 1))
    copies.start((batch, 'half'), -1, near.at[across, high], far.at[0, high], place.device('x', -1))
    for there in (right, left, here):
        near[there] = near[there] + src[there, core]
    yield
    copies.wait((batch, 'half'), 1, far.at[0, low])
    near[right, low] = near[right, low] + far[0, low]
    copies.start((batch, 'full'), 1, near.at[right], far.at[1], place.device('x', 1))
    copies.wait((batch, 'half'), -1, far.at[0, high])
    near[left, high] = near[left, high] + far[0, high]
    copies.start((batch, 'full'), -1, near.at[left], far.at[2], place.device('x', -1))
    yield
    copies.wait((batch, 'full'), 1, far.at[1])
    copies.wait((batch, 'full'), -1, far.at[2])
    store(near[here] + far[1] + far[2])
    copies.left((batch, 'near'), near)
    copies.left((batch, 'half'), far.at[0])
    copies.left((batch, 'full'), far.at[pl.ds(1, 2)])
    yield


def line_gather(copies, batch, place, out):
    core = place.core
    half = out.shape[2] // 2
    here, right, across, left = [out.at[place.at('x', step), core] for step in range(SIDE)]

    def hand(ref):
        copies.start((batch, 'hand'), ONLY, ref, ref, place.mate)

    for step in BOTH_WAYS:
        copies.start((batch, 'all'), step, here, here, place.device('x', step))
    hand(here)
    yield
    for step, ref, span in ((1, left, pl.ds(0, half)), (-1, right, pl.ds(half, half))):
        copies.wait((batch, 'all'), step, ref)
        copies.start((batch, 'all'), 2 * step, ref.at[span], ref.at[span], place.device('x', step))
        hand(ref)
    yield
    for step, span in ((1, pl.ds(0, half)), (-1, pl.ds(half, half))):
        copies.wait((batch, 'all'), 2 * step, across.at[span])
    hand(across)
    yield
    copies.wait((batch, 'hand'), ONLY, out.at[:, 0])
    copies.left((batch, 'all'), out.at[0:3, 0])
    copies.left((batch, 'hand'), out.at[:, 0])
    yield


BALANCED = (('x', 'y', 'z'), ('y', 'z', 'x'), ('z', 'x', 'y'))
X_LAST = (('y', 'z', 'x'), ('z', 'y', 'x'))


def cube_gather(copies, batch, place, view, cuts, orders, one_way, owners=SIDE):
    core = place.core
    parts = [(order, pl.ds(start, end - start)) for order, start, end in zip(orders, cuts[:-1], cuts[1:])]
    every, low, high = (0, owners), (0, owners // 2), (owners // 2, owners // 2)

    def like(z, y, x):
        return view(0, *[pl.ds(0, num) if num > 1 else 0 for num in (z, y, x)], pl.ds(cuts[0], cuts[-1] - cuts[0]))

    def at(order, cols, places):
        where = dict(zip(order, places))
        return view(core, where['z'], where['y'], where['x'], cols)

    def single(order, cols):
        return at(order, cols, [place.at(dim, 0) for dim in order])

    def group(order, cols, a, b, span=every):
        return at(order, cols, (pl.ds(*span), place.at(order[1], a), place.at(order[2], b)))

    def hand(order, cols, a, b):
        ref = group(order, cols, a, b)
        copies.start((batch, 'mate'), ONLY, ref, ref, place.mate)

    def spread(order, cols, a):
        ref = group(order, cols, a, 0)
        for step in BOTH_WAYS:
            copies.start((batch, 'three'), a, ref, ref, place.device(order[2], step))
        hand(order, cols, a, 0)

    def ways(single_way, dim):
        return ((1, every),) if single_way and dim != 'x' else ((-1, low), (1, high))

    def pass_on(a):
        copies.wait((batch, 'three'), a, like(1, CORES, owners))
        for order, cols in parts:
            for step, span in ways(a in one_way, order[2]):
                half = group(order, cols, a, step, span)
                copies.start((batch, 'three'), ('end', a), half, half, place.device(order[2], -step))
            for step in BOTH_WAYS:
                hand(order, cols, a, step)

    def first_sends():
        for order, cols in parts:
            for step in (2, 1, -1):
                copies.start((batch, 'one'), ONLY, single(order, cols), single(order, cols), place.device(order[0], step))

    if owners == SIDE:
        first_sends()
        yield
        copies.wait((batch, 'one'), ONLY, like(1, 1, 3))
    else:
        pl.when(place.at('z', 0) < owners)(first_sends)
        yield
        pl.when(place.at('z', 0) < owners)(lambda: copies.wait((batch, 'one'), ONLY, like(1, 1, 1)))
        pl.when(place.at('z', 0) >= owners)(lambda: copies.wait((batch, 'one'), ONLY, like(1, 1, owners)))
    for order, cols in parts:
        for step in BOTH_WAYS:
            copies.start((batch, 'two'), ONLY, group(order, cols, 0, 0), group(order, cols, 0, 0), place.device(order[1], step))
    for order, cols in parts:
        spread(order, cols, 0)
    yield
    copies.wait((batch, 'two'), ONLY, like(1, CORES, owners))
    for order, cols in parts:
        for step, span in ways(len(one_way) > 2, order[1]):
            half = group(order, cols, step, 0, span)
            copies.start((batch, 'two'), 'end', half, half, place.device(order[1], -step))
    for order, cols in parts:
        for step in BOTH_WAYS:
            spread(order, cols, step)
    yield
    pass_on(0)
    yield
    copies.wait((batch, 'two'), 'end', like(1, 1, owners))
    for order, cols in parts:
        spread(order, cols, 2)
    yield
    for a in (-1, 1, 2):
        pass_on(a)
        yield
    for a in (0, -1, 1, 2):
        copies.wait((batch, 'three'), ('end', a), like(1, 1, owners))
        for order, cols in parts:
            hand(order, cols, a, 2)
        yield
    whole = like(SIDE, SIDE, owners)
    copies.wait((batch, 'mate'), ONLY, whole)
    copies.left((batch, 'mate'), whole)
    if owners == SIDE:
        copies.left((batch, 'one'), like(1, 1, 3))
    else:
        pl.when(place.at('z', 0) < owners)(lambda: copies.left((batch, 'one'), like(1, 1, 3)))
    copies.left((batch, 'two'), like(1, 3, owners))
    copies.left((batch, 'three'), like(3, SIDE, owners))
    yield


def pump(gen, name):
    with scope(name):
        next(gen, None)


def drain(gen, name):
    with scope(name):
        for _ in gen:
            pass


def step_kernel(scale, x_hbm, dy_hbm, w_col_hbm, w_row_hbm, a_old, s_old, a_inv, s_inv, fact, grads, w_col, w_row, x_buf, dy_buf, h_two, w_two, w_three, z_one, h_one, h_three,
                g_three, t_three, rows_buf, z_two, left, w_three_t, gram_src, gram_near, gram_far, old_buf, piece_buf, grad_src, grad_near,
                grad_far, grad_sum, grad_out, big_buf, load_sems, old_sems, big_sems, send_sems, recv_sems):
    place = Place()
    model_id, data_id, core = place.model, place.data, place.core
    spot, y_pos, z_pos = place.at('x', 0), place.at('y', 0), place.at('z', 0)
    copies = Copies(send_sems, recv_sems)
    my_rows = span_of(model_id, BLOCK)
    my_cols = span_of(model_id, BLOCK)
    my_part = pl.ds(pl.multiple_of(data_id * PIECE, PIECE), PIECE)
    g_one = t_three
    olds = [a_old.at[0], s_old.at[1], a_old.at[1], s_old.at[0]]
    chunk = 256
    n_chunks = WIDTH // chunk
    half_way = n_chunks // CORES
    met = [(place.peer(a, b), data_id) for a, b in STEPS] + [place.mate] + [place.device('x', step) for step in (1, 2, 3)]

    def load(src, dst, base, i):
        rows = span_of(i, chunk)
        return pltpu.make_async_copy(src.at[rows, :], dst.at[rows, :], load_sems.at[base + i])

    def load_x(i):
        return load(x_hbm, x_buf, 0, i)

    def load_dy(i):
        return load(dy_hbm, dy_buf, n_chunks, i)

    def load_old(mat, j):
        rows = pl.ds(pl.multiple_of(model_id * BLOCK + data_id * PIECE, PIECE), PIECE)
        cols = span_of(lax.rem(model_id + j, PLANE), BLOCK)
        return pltpu.make_async_copy(olds[mat].at[rows, cols], old_buf.at[mat, :, pl.ds(j * BLOCK, BLOCK)], old_sems.at[mat])

    def cols_of(buf, cols):
        return buf[:, cols] if len(buf.shape) == 2 else buf[:, :, :, :, :, cols].reshape(WIDTH, cols.size)

    def rows_of(buf, z_step, y_step):
        return buf[place.at('z', z_step), place.at('y', y_step)].reshape(BLOCK, WIDTH)

    call_out(met)
    own_w_two = pltpu.make_async_copy(w_row_hbm.at[0, my_part, :], w_two.at[z_pos, y_pos, spot, core], old_sems.at[4])
    own_w_two.start()
    load_w = [pltpu.make_async_copy(w_col_hbm, w_col, big_sems.at[0]), pltpu.make_async_copy(w_row_hbm, w_row, big_sems.at[1])]
    for move in load_w:
        move.start()
    for i in range(n_chunks):
        load_x(i).start()

    def z_one_step(i, carry):
        rows = span_of(i, chunk)
        load_x(i).wait()
        pre_act = matmul(x_buf[rows, :], w_col[0]).astype(jnp.bfloat16)
        z_one[rows, :] = pre_act
        h_one[rows, :] = activate(pre_act)
        return carry

    own_w_two.wait()
    with scope('greet'):
        all_here(met)

    def z_one_first():
        with scope('z1a'):
            for move in load_w:
                move.wait()
            w_three_t[...] = w_col[1].T
            w_three[z_pos, y_pos, spot, core] = w_three_t[my_part, :]
            lax.fori_loop(0, half_way, z_one_step, 0)
        for i in range(n_chunks):
            load_dy(i).start()
        for mat in range(4):
            for j in range(TRI):
                load_old(mat, j).start()

    def weight_thread(batch, buf, cuts, orders, one_way):
        def view(which, z, y, x, cols):
            return buf.at[z, y, x, which, :, cols]
        return cube_gather(copies, batch, place, view, cuts, orders, one_way)

    def z_one_rest():
        with scope('z1b'):
            lax.fori_loop(half_way, n_chunks, z_one_step, 0)

    def send_block(batch, cols_ref, a, b):
        peer = place.peer(a, b)
        copies.start(batch, ONLY, cols_ref.at[span_of(peer, BLOCK), :], rows_buf.at[:, my_cols], (peer, data_id))

    def wait_blocks(batch):
        others = rows_buf.at[:, 0:WIDTH - BLOCK]
        copies.wait(batch, ONLY, others)
        copies.left(batch, others)

    loaded = []

    def wait_dy():
        if not loaded:
            for i in range(n_chunks):
                load_dy(i).wait()
            loaded.append(True)

    def t_three_step(i, carry):
        rows = span_of(i, chunk)
        t_three[rows, :] = matmul_nt(dy_buf[rows, :], w_row[1]).astype(jnp.bfloat16)
        return carry

    def t_three_thread():
        wait_dy()
        for i in range(0, n_chunks, CORES):
            with scope('t3'):
                lax.fori_loop(i, i + CORES, t_three_step, 0)
            yield

    def turn(dst, src, cols):
        for i in range(4):
            rows = slice(i * 512, (i + 1) * 512)
            dst[:, rows] = (src[rows, cols] if len(src.shape) == 2 else src[i, :, :, :, :, cols].reshape(512, BLOCK)).T

    def gram_product(mat, lhs, right):
        def block_cols(j):
            return cols_of(right, span_of(lax.rem(model_id + j, PLANE), BLOCK))

        def gram_step(i, carry):
            block = matmul(lhs[...], jnp.concatenate([block_cols(2 * i), block_cols(2 * i + 1)], axis=1))
            gram_src[mat, :, :, :, span_of(i, chunk)] = block.reshape(SIDE, CORES, PIECE, chunk)
            return carry
        lax.fori_loop(0, TRI // 2, gram_step, 0)
        block = matmul(lhs[...], block_cols(TRI - 1))
        gram_src[mat, :, :, :, (TRI - 1) * BLOCK:] = block.reshape(SIDE, CORES, PIECE, BLOCK)

    def grad_product(lhs, right, same, slot):
        def grad_step(i, carry):
            cols = span_of(i, chunk)
            block = matmul(lhs[...], cols_of(right, cols))
            grad_src[slot, :, :, :, cols] = block.reshape(SIDE, CORES, PIECE, chunk)
            return carry
        lax.fori_loop(0, n_chunks, grad_step, 0)
        block = matmul(lhs[...], same[...])
        grad_src[slot, :, :, :, WIDTH:GRAD_COLS] = block.reshape(SIDE, CORES, PIECE, BLOCK)

    def store_factor(mat, total):
        pltpu.make_async_copy(old_buf.at[mat], old_buf.at[mat], old_sems.at[mat]).wait()
        mixed = FACTOR_DECAY * old_buf[mat] + scale * total
        piece_buf[mat] = mixed

    def sum_thread(mat):
        return line_reduce(copies, ('gram', mat), place, gram_src.at[mat], gram_near.at[mat], gram_far.at[mat], functools.partial(store_factor, mat))

    def factor_thread(first, count, cuts, orders, one_way, rest_order):
        mats = pl.ds(first, count)

        def view(which, z, y, x, cols):
            return fact.at[z, y, x, which, mats, :, cols]

        move = pltpu.make_async_copy(piece_buf.at[mats], fact.at[z_pos, y_pos, spot, core, mats], old_sems.at[4])
        move.start()
        move.wait()
        main = cube_gather(copies, ('fact', first), place, view, cuts, orders, one_way)
        rest = cube_gather(copies, ('rest', first), place, view, (TRI * BLOCK - BLOCK, FACTOR_COLS), (rest_order,), (), CORES)
        for _ in main:
            next(rest)
            yield


    def gram_job(mat, slot, right):
        if mat == 1:
            wait_dy()
        with scope('gram'):
            turn(left.at[slot], right, my_cols)
            gram_product(mat, left.at[slot], right)

    def grad_job(layer, slot, lhs, right):
        with scope('dW'):
            turn(left.at[slot], lhs, slice(0, BLOCK))
            grad_product(left.at[slot], right, lhs, layer % 2)
        if layer == 0:
            load_big(0, 0).start()
            load_big(0, 1).start()

    near_by = [(a, b) for a in range(SIDE) for b in range(SIDE) if 2 not in (a, b)]
    far_off = [where for where in [(0, 0)] + STEPS if where not in near_by]

    def picked(buf, places, cols):
        if len(buf.shape) == 2:
            parts = [buf[span_of(place.peer(a, b), BLOCK), cols] for a, b in places]
        else:
            parts = [buf[place.at('z', a), place.at('y', b), :, :, :, cols] for a, b in places]
        return [part.reshape(BLOCK, part.shape[-1]) for part in parts]

    def turn_picked(slot, buf, places, cols):
        for num, part in enumerate(picked(buf, places, cols)):
            left[slot, :, num * BLOCK:(num + 1) * BLOCK] = part.T

    def put(dst, cols, product, places):
        value = product.reshape(SIDE, CORES, PIECE, product.shape[-1])
        dst[:, :, :, cols] = value if places is near_by else dst[:, :, :, cols] + value

    def late_grad(layer, slot, lhs, right, places):
        def late_step(i, carry):
            cols = span_of(i, chunk)
            put(dst, cols, matmul(left[slot, :, :depth], jnp.concatenate(picked(right, places, cols), axis=0)), places)
            return carry

        dst, depth, block = grad_src.at[layer % 2], len(places) * BLOCK, slice(0, BLOCK)
        with scope('dW'):
            turn_picked(slot, lhs, places, block)
            lax.fori_loop(0, n_chunks, late_step, 0)
            put(dst, slice(WIDTH, GRAD_COLS), matmul(left[slot, :, :depth], jnp.concatenate(picked(lhs, places, block), axis=0)), places)

    def late_gram(mat, slot, right, places):
        def block_cols(j):
            return jnp.concatenate(picked(right, places, span_of(lax.rem(model_id + j, PLANE), BLOCK)), axis=0)

        def late_step(i, carry):
            put(dst, span_of(i, chunk), matmul(left[slot, :, :depth], jnp.concatenate([block_cols(2 * i), block_cols(2 * i + 1)], axis=1)), places)
            return carry

        dst, depth = gram_src.at[mat], len(places) * BLOCK
        with scope('gram'):
            turn_picked(slot, right, places, my_cols)
            lax.fori_loop(0, TRI // 2, late_step, 0)
            put(dst, slice((TRI - 1) * BLOCK, FACTOR_COLS), matmul(left[slot, :, :depth], block_cols(TRI - 1)), places)

    def swap_first():
        for a, b in STEPS:
            send_block('h1', h_one, a, b)
        rows_buf[:, my_cols] = h_one[my_rows, :]

    def z_two_step(i, carry):
        cols = span_of(i, chunk)
        pre_act = matmul(rows_buf[...], cols_of(w_two, cols)).astype(jnp.bfloat16)
        z_two[:, cols] = pre_act
        h_two[z_pos, y_pos, :, :, :, cols] = activate(pre_act).reshape(SIDE, CORES, PIECE, chunk)
        return carry

    def second_forward():
        drain(threads['w2'], 'w2_rest')
        with scope('wait_h1'):
            wait_blocks('h1')
        with scope('z2'):
            lax.fori_loop(0, n_chunks, z_two_step, 0)

    def forward_block(a, b):
        rows = span_of(place.peer(a, b), BLOCK)
        pre_act = matmul(rows_of(h_two, a, b), w_col[1]).astype(jnp.bfloat16)
        h_three[rows, :] = activate(pre_act)
        g_three[rows, :] = back_gate(t_three[rows, :], pre_act)
        if (a, b) != (0, 0):
            send_block('g3', g_three, a, b)

    def backward_block(a, b):
        rows = span_of(place.peer(a, b), BLOCK)
        grad = matmul_nt(rows_of(w_two, a, b), w_row[0]).astype(jnp.bfloat16)
        g_one[rows, :] = back_gate(grad, z_one[rows, :])

    def gather_tokens(tag, buf, block_step):
        seen = {}

        def on_piece(order, first, second):
            where = (first % SIDE, second % SIDE)
            seen[where] = seen.get(where, 0) + 1

        def region(z, y, order, lo, hi):
            return buf.at[z, y, pl.ds(2 * order + lo, hi - lo)]

        def like(quarters):
            return x_buf.at[0:quarters * BLOCK // 4, :]

        done = {(0, 0)}
        gen = plane_gather(copies, tag, place, region, like, on_piece)
        next(gen)
        with scope(tag + '_blocks'):
            block_step(0, 0)
        yield
        for _ in gen:
            ready = [where for where in sorted(seen) if seen[where] == 2 and where not in done]
            with scope(tag + '_blocks'):
                for where in ready:
                    block_step(*where)
            done.update(ready)
            yield
        copies.left(tag, x_buf.at[0:WIDTH - BLOCK, :])

    def split(value):
        high = value.astype(jnp.bfloat16)
        rest = value - high.astype(jnp.float32)
        middle = rest.astype(jnp.bfloat16)
        return high, middle, (rest - middle.astype(jnp.float32)).astype(jnp.bfloat16)

    inverses = [s_inv.at[1], a_inv.at[1], s_inv.at[0], a_inv.at[0]]
    big_rows = 2 * PIECE

    def load_big(layer, i):
        slot = lax.rem(i, CORES)
        return pltpu.make_async_copy(inverses[layer].at[span_of(i, chunk), span_of(core, HALF)], big_buf.at[slot], big_sems.at[slot])

    def grad_thread(layer):
        sum_ref, out_ref, tag = grad_sum.at[layer], grad_out.at[layer], ('grad', layer)

        def keep_sum(total):
            sum_ref[core] = total

        def big_step(i, carry):
            load_big(layer, i).wait()
            lhs = jnp.concatenate(split(sum_ref[:, :, span_of(i, chunk)].reshape(big_rows, chunk)), axis=0)
            high, middle, low = split(big_buf[lax.rem(i, CORES)])
            by_high, by_middle, by_low = matmul(lhs, high), matmul(lhs[:2 * big_rows], middle), matmul(lhs[:big_rows], low)
            small = by_high[2 * big_rows:] + by_middle[big_rows:] + by_low
            out_ref[:, :HALF] += by_high[:big_rows] + (by_high[big_rows:2 * big_rows] + by_middle[:big_rows] + small)

            @pl.when(i + 2 < n_chunks)
            def _():
                load_big(layer, i + 2).start()
            if layer < 3:
                @pl.when(i + 2 >= n_chunks)
                def _():
                    load_big(layer + 1, i + 2 - n_chunks).start()
            return carry

        yield from line_reduce(copies, tag, place, grad_src.at[layer % 2], grad_near.at[layer], grad_far.at[layer], keep_sum)
        copies.start(tag + ('pair',), ONLY, sum_ref.at[core], sum_ref.at[core], place.mate)
        yield
        copies.wait(tag + ('pair',), ONLY, sum_ref.at[1 - core])
        copies.left(tag + ('pair',), sum_ref.at[0])
        out_ref[...] = jnp.concatenate([jnp.zeros((big_rows, HALF), jnp.float32), sum_ref[:, :, WIDTH:].reshape(big_rows, BLOCK)], axis=1)
        with scope('X'):
            lax.fori_loop(0, half_way, big_step, 0)
        yield
        with scope('X'):
            lax.fori_loop(half_way, n_chunks, big_step, 0)
        move = pltpu.make_async_copy(out_ref, grads.at[layer, spot, core], old_sems.at[5])
        move.start()
        move.wait()
        yield from line_gather(copies, tag, place, grads.at[layer])

    def g_two_step(i, carry):
        cols = span_of(i, chunk)
        grad = matmul(rows_buf[...], cols_of(w_three, cols)).astype(jnp.bfloat16)
        w_two[z_pos, y_pos, :, :, :, cols] = back_gate(grad, z_two[:, cols]).reshape(SIDE, CORES, PIECE, chunk)
        return carry

    def second_backward():
        drain(threads['w3'], 'w3_rest')
        with scope('wait_g3'):
            wait_blocks('g3')
            rows_buf[:, my_cols] = g_three[my_rows, :]
        with scope('g2'):
            lax.fori_loop(0, n_chunks, g_two_step, 0)

    threads = dict(
        w2=weight_thread('w2', w_two, W_TWO_CUTS, BALANCED, W_TWO_WAYS),
        w3=weight_thread('w3', w_three, W_THREE_CUTS, MOSTLY_X, W_THREE_WAYS),
        h2=gather_tokens('h2', h_two, forward_block),
        g2=gather_tokens('g2', w_two, backward_block),
        pair=factor_thread(0, 2, PAIR_CUTS, MOSTLY_X, PAIR_WAYS, ('z', 'y', 'x')),
        fa3=factor_thread(2, 1, LATE_CUTS, BALANCED, LATE_WAYS, ('z', 'x', 'y')),
        fs2=factor_thread(3, 1, LATE_CUTS, BALANCED, LATE_WAYS, ('z', 'x', 'y')),
        sum0=sum_thread(0), sum1=sum_thread(1), sum2=sum_thread(2), sum3=sum_thread(3),
        t3=t_three_thread(),
        grad4=grad_thread(0), grad3=grad_thread(1), grad2=grad_thread(2), grad1=grad_thread(3),
    )
    steps = {name: functools.partial(pump, thread, name) for name, thread in threads.items()}
    steps.update(
        z0=z_one_first, z1=z_one_rest, swap=swap_first, z2=second_forward, back=second_backward,
        A1=functools.partial(gram_job, 0, 0, x_buf), S4=functools.partial(gram_job, 1, 1, dy_buf),
        A3=functools.partial(gram_job, 2, 0, h_two),
        S2a=functools.partial(late_gram, 3, 0, w_two, near_by), S2b=functools.partial(late_gram, 3, 0, w_two, far_off),
        dW4=functools.partial(grad_job, 0, 1, h_three, dy_buf), dW3=functools.partial(grad_job, 1, 0, g_three, h_two),
        dW2a=functools.partial(late_grad, 2, 0, h_one, w_two, near_by), dW2b=functools.partial(late_grad, 2, 0, h_one, w_two, far_off),
        dW1a=functools.partial(late_grad, 3, 1, g_one, x_buf, near_by), dW1b=functools.partial(late_grad, 3, 1, g_one, x_buf, far_off),
    )
    for step in plan(**steps):
        step()
    for name, thread in threads.items():
        drain(thread, name)
    assert len(copies.batches) == N_BATCHES and len(copies.names) == N_COPIES, (len(copies.batches), len(copies.names))


W_TWO_CUTS = (0, 640, 1408, 2048)
W_THREE_CUTS = (0, 896, 1920, 2048)
PAIR_CUTS = (0, 384, 896, 1024)
LATE_CUTS = (0, 512, 640, 1024)
W_TWO_WAYS = (-1, 1, 2)
W_THREE_WAYS = (-1, 0)
PAIR_WAYS = (0, 1)
LATE_WAYS = ()
MOSTLY_X = (('y', 'z', 'x'), ('z', 'y', 'x'), ('x', 'y', 'z'))


def plan(w2, w3, h2, g2, pair, fa3, fs2, sum0, sum1, sum2, sum3, grad4, grad3, grad2, grad1, z0, z1, swap, z2, back, A1, S4, A3, S2a, S2b, dW4, dW3, dW2a, dW2b, dW1a, dW1b, t3):
    return (
        w2, w2, z0, w3, w2, z1, w2, A1, sum0, w2, S4, sum1, swap, sum0, sum1, w2, t3, t3, t3, w2, sum0, sum1, w2, w3, t3, w2, sum0, w2, w2, sum1, w2,
        pair, w2, w3, z2, h2, pair, h2, w3, h2, w3, h2, pair, h2, h2, h2, h2, w3, h2, h2, h2, h2, h2, h2, pair, w3, h2, w3, h2, w3, w3, pair, h2, w3,
        w3, pair, pair, A3, w3, back, g2, dW3, sum2, g2, dW4, grad4, grad3, grad4, g2, sum2, grad4, grad3, sum2, grad4, grad4, g2, g2, grad3, grad4,
        g2, g2, sum2, fa3, g2, g2, grad3, g2, grad4, g2, grad3, dW1a, g2, pair, grad3, g2, grad3, g2, pair, g2, S2a, grad4, dW2a, fa3, g2, grad3, g2,
        S2b, sum3, dW2b, grad2, sum3, fa3, grad2, dW1b, sum3, grad1, grad3, fa3, grad1, grad2, fa3, pair, sum3, fs2, fa3, grad2, grad2, pair, grad1,
        fa3, grad2, fs2, fa3, pair, grad2, grad1, grad1, fa3, fa3, fs2, grad1, fs2, grad1, fs2, pair, fs2, fa3, fs2, grad2, grad1, grad4, fs2, grad3,
        fs2, fs2, grad4, fs2, grad2, fa3, grad1, fs2, grad1, fa3, grad2, fs2,
    )


N_BATCHES = 72
N_COPIES = 192


def step_call(x_tokens, dy_tokens, w_col, w_row, a_old, s_old, a_inv, s_inv, scale):
    f32, bf16 = jnp.float32, jnp.bfloat16
    tall, wide = (WIDTH, BLOCK), (BLOCK, WIDTH)
    cube = (SIDE, SIDE, SIDE, 2)
    rows = 2 * PIECE
    hbm = pl.BlockSpec(memory_space=pl.ANY)
    scratch = [pltpu.VMEM((2,) + tall, bf16), pltpu.VMEM((2,) + wide, bf16)] + [pltpu.VMEM((WIDTH, WIDTH), bf16)] * 2 + [pltpu.VMEM(cube + (PIECE, WIDTH), bf16)] * 3
    scratch += [pltpu.VMEM(tall, bf16)] * 5 + [pltpu.VMEM(wide, bf16)] * 2 + [pltpu.VMEM((2,) + wide, bf16), pltpu.VMEM(wide, bf16)]
    scratch += [pltpu.VMEM((SIDE, SIDE, CORES, PIECE, TRI * BLOCK), f32), pltpu.VMEM((SIDE, SIDE, PIECE, TRI * BLOCK), f32), pltpu.VMEM((4, 3, PIECE, TRI * BLOCK), f32)]
    scratch += [pltpu.VMEM((4, PIECE, TRI * BLOCK), f32), pltpu.VMEM((4, PIECE, FACTOR_COLS), f32)]
    scratch += [pltpu.VMEM((2, SIDE, CORES, PIECE, GRAD_COLS), f32), pltpu.VMEM((SIDE, SIDE, PIECE, GRAD_COLS), f32), pltpu.VMEM((4, 3, PIECE, GRAD_COLS), f32)]
    scratch += [pltpu.VMEM((4, 2, PIECE, GRAD_COLS), f32), pltpu.VMEM((4, rows, HALF + BLOCK), f32), pltpu.VMEM((2, 256, HALF), f32)]
    scratch += [pltpu.SemaphoreType.DMA((num,)) for num in (16, 6, 2, N_BATCHES, N_COPIES)]
    return pl.pallas_call(
        functools.partial(step_kernel, scale),
        out_shape=[jax.ShapeDtypeStruct(cube + (4, PIECE, FACTOR_COLS), f32), jax.ShapeDtypeStruct((4, SIDE, 2, rows, HALF + BLOCK), f32)],
        in_specs=[hbm] * 8,
        out_specs=[hbm, hbm],
        scratch_shapes=scratch,
        compiler_params=pltpu.CompilerParams(collective_id=0, has_side_effects=True, vmem_limit_bytes=67043328),
        name='step',
    )(x_tokens, dy_tokens, w_col, w_row, a_old, s_old, a_inv, s_inv)


def finish_kernel(scale, inv_rows, fact, grads, s_old_col, a_old_row, s_inv_col, a_inv_row, a_new, s_new, u_col, u_row, s_new_col, a_new_row, buf, turned, sums, u_col_buf, u_row_buf, load_sems, out_sems, turn_sems, far_sems, far_out_sems, small_sems):
    mid = PLANE // CORES
    outs = [(a_new, 0), (s_new, 1), (a_new, 1), (s_new, 0)]

    def load(mat, row):
        z, y = lax.div(row, SIDE), lax.rem(row, SIDE)
        return pltpu.make_async_copy(fact.at[z, y, :, :, mat], buf.at[mat, row], load_sems.at[mat * PLANE + row])

    def turn_done(slot):
        ref = turned.at[slot, pl.ds(0, TRI - 2)]
        return pltpu.make_async_copy(ref, ref, turn_sems.at[slot])

    def far_done(row):
        slot = lax.rem(row, CORES)
        ref = turned.at[slot, TRI - 2]
        return pltpu.make_async_copy(ref, ref, far_sems.at[slot])

    def start_load(mat):
        def body(row, carry):
            load(mat, row).start()
            return carry
        lax.fori_loop(0, PLANE, body, 0)

    load_sums = pltpu.make_async_copy(grads, sums, out_sems.at[4])
    load_sums.start()
    for mat in range(SIDE):
        start_load(mat)
    half = HALF

    def new_blocks():
        load_sums.wait()
        for layer in range(SIDE):
            block, num = scale * sums[layer, :, 0, :, half:].reshape(BLOCK, BLOCK), 1 - layer // 2
            if layer % 2 == 1:
                s_new_col[num] = FACTOR_DECAY * s_old_col[num] + block
            else:
                a_new_row[num] = FACTOR_DECAY * a_old_row[num] + block

    def move_small(batch):
        moves = [(u_col_buf, u_col), (u_row_buf, u_row)]
        return [pltpu.make_async_copy(src.at[1 - batch], dst.at[1 - batch], small_sems.at[2 * batch + num]) for num, (src, dst) in enumerate(moves)]

    chunk = 2 * BLOCK

    def small_product(layer, i):
        num = 1 - layer // 2
        core, cols, out = lax.div(i, SIDE), span_of(lax.rem(i, SIDE), chunk), span_of(i, chunk)
        product = sums[layer, :, core, :, cols].reshape(BLOCK, chunk)
        if layer % 2 == 1:
            u_col_buf[num, out, :] = exact_dot(product.T, s_inv_col[num]) * inv_rows
        else:
            u_row_buf[num, :, out] = exact_dot(a_inv_row[num], product) * inv_rows

    for mat, (out, num) in enumerate(outs):
        def row_step(row, carry):
            load(mat, row).wait()
            slot = lax.rem(row, CORES)
            if mat in (1, 2):
                @pl.when(row < mid)
                def _():
                    small_product(2 * mat - 2, row)

                @pl.when(row >= mid)
                def _():
                    small_product(2 * mat - 1, row - mid)
            far = TRI - 1
            def place_block(j, sem):
                cols = span_of(lax.rem(row + j, PLANE), BLOCK)
                pltpu.make_async_copy(buf.at[mat, row, :, :, :, pl.ds(j * BLOCK, BLOCK)], out.at[num, row, :, :, :, cols], sem).start()

            def place_turned(j, sem):
                block = buf[mat, row, :, :, :, j * BLOCK:(j + 1) * BLOCK].reshape(BLOCK, BLOCK).T
                turned[slot, j - 1] = block.reshape(SIDE, CORES, PIECE, BLOCK)
                pltpu.make_async_copy(turned.at[slot, j - 1], out.at[num, lax.rem(row + j, PLANE), :, :, :, span_of(row, BLOCK)], sem).start()

            for j in range(far):
                place_block(j, out_sems.at[mat])
            if mat > 0:
                turn_done(slot).wait()
            else:
                @pl.when(row >= 2)
                def _():
                    turn_done(slot).wait()
            for j in range(1, far):
                place_turned(j, turn_sems.at[slot])

            @pl.when(row < mid)
            def _():
                if mat > 0:
                    far_done(row).wait()
                else:
                    @pl.when(row >= 2)
                    def _():
                        far_done(row).wait()
                place_block(far, far_out_sems.at[mat])
                place_turned(far, far_sems.at[slot])
            return carry

        if mat == 1:
            new_blocks()
        lax.fori_loop(0, PLANE, row_step, 0)
        if mat in (1, 2):
            for move in move_small(mat - 1):
                move.start()
    for batch in range(CORES):
        for move in move_small(batch):
            move.wait()
    for slot in range(CORES):
        turn_done(slot).wait()
        far_done(slot).wait()
    for mat in range(SIDE):
        near, far = buf.at[mat, :, :, :, :, pl.ds(0, mid * BLOCK)], buf.at[mat, pl.ds(0, mid), :, :, :, pl.ds(0, BLOCK)]
        pltpu.make_async_copy(near, near, out_sems.at[mat]).wait()
        pltpu.make_async_copy(far, far, far_out_sems.at[mat]).wait()


def finish_call(fact, grads, s_old_col, a_old_row, s_inv_col, a_inv_row, scale, inv_rows):
    f32 = jnp.float32
    shapes = [(2, PLANE, SIDE, CORES, PIECE, WIDTH)] * 2 + [(2, WIDTH, BLOCK), (2, BLOCK, WIDTH)] + [(2, BLOCK, BLOCK)] * 2
    hbm, vmem = pl.BlockSpec(memory_space=pl.ANY), pl.BlockSpec(memory_space=pltpu.VMEM)
    return pl.pallas_call(
        functools.partial(finish_kernel, scale, inv_rows),
        out_shape=[jax.ShapeDtypeStruct(shape, f32) for shape in shapes],
        in_specs=[hbm] * 2 + [vmem] * 4,
        out_specs=[hbm] * 4 + [vmem] * 2,
        scratch_shapes=[pltpu.VMEM((4, PLANE, SIDE, CORES, PIECE, FACTOR_COLS), f32), pltpu.VMEM((2, TRI - 1, SIDE, CORES, PIECE, BLOCK), f32), pltpu.VMEM(grads.shape, f32), pltpu.VMEM((2, WIDTH, BLOCK), f32), pltpu.VMEM((2, BLOCK, WIDTH), f32)] + [pltpu.SemaphoreType.DMA((num,)) for num in (SIDE * PLANE, 5, CORES, CORES, SIDE, SIDE)],
        compiler_params=pltpu.CompilerParams(vmem_limit_bytes=67043328),
        name='finish',
    )(fact, grads, s_old_col, a_old_row, s_inv_col, a_inv_row)


def solution(mesh):
    def shard_body(x_tokens, dy_tokens, w_col, w_row, a_old_col, s_old_col, a_old_row, s_old_row, a_inv_col, s_inv_col, a_inv_row, s_inv_row):
        inv_rows = 1.0 / (x_tokens.shape[0] * DATA_WAYS)
        scale = (1.0 - FACTOR_DECAY) * inv_rows
        fact, grads = step_call(x_tokens, dy_tokens, w_col, w_row, a_old_col, s_old_row, a_inv_col, s_inv_row, scale)
        a_new_col, s_new_row, u_col, u_row, s_new_col, a_new_row = finish_call(fact, grads, s_old_col, a_old_row, s_inv_col, a_inv_row, scale, inv_rows)
        return (u_col, u_row, a_new_col.reshape(2, WIDTH, WIDTH), s_new_col, a_new_row, s_new_row.reshape(2, WIDTH, WIDTH))

    batch_split = P('data', None)
    col_split = P(None, None, 'model')
    row_split = P(None, 'model', None)
    replicated = P()
    return jax.shard_map(
        shard_body,
        mesh=mesh,
        in_specs=(batch_split, batch_split, col_split, row_split, replicated, row_split, row_split, replicated, replicated, row_split, row_split, replicated),
        out_specs=(col_split, row_split, replicated, row_split, row_split, replicated),
        check_vma=False,
    )
```

```python
import contextlib
import functools
import math
import jax
import jax.numpy as jnp
from jax import lax
from jax.experimental import pallas as pl
from jax.experimental.pallas import tpu as pltpu
from jax.sharding import PartitionSpec as P

FACTOR_DECAY = 0.8
GELU_SCALE = math.sqrt(2.0 / math.pi)
GELU_CUBIC = 0.044715
EXACT = lax.Precision.HIGHEST
MESH = pl.DeviceIdType.MESH
SIDE = 4
PLANE = 16
DATA_WAYS = 8
WIDTH = 2048
BLOCK = 128
PIECE = 16
TRI = 9
ONLY = 0
CORES = 2
BOTH_WAYS = (1, -1)
ORDERS = (0, 1)
HALF = WIDTH // 2
SCOPED = False
FACTOR_COLS = TRI * BLOCK
GRAD_COLS = WIDTH + BLOCK
NT_DIMS = (((1,), (1,)), ((), ()))


def gelu_value(pre_act):
    tanh_arg = GELU_SCALE * (pre_act + GELU_CUBIC * pre_act * pre_act * pre_act)
    return 0.5 * pre_act * (1.0 + jnp.tanh(tanh_arg))


def gelu_slope(pre_act):
    tanh_arg = GELU_SCALE * (pre_act + GELU_CUBIC * pre_act * pre_act * pre_act)
    tanh_val = jnp.tanh(tanh_arg)
    return 0.5 * (1.0 + tanh_val) + 0.5 * pre_act * (1.0 - tanh_val * tanh_val) * GELU_SCALE * (1.0 + 3.0 * GELU_CUBIC * pre_act * pre_act)


def activate(pre_act):
    return gelu_value(pre_act.astype(jnp.float32)).astype(jnp.bfloat16)


def back_gate(grad_act, pre_act):
    return (grad_act.astype(jnp.float32) * gelu_slope(pre_act.astype(jnp.float32))).astype(jnp.bfloat16)


def matmul(left_mat, right_mat):
    return jnp.dot(left_mat, right_mat, preferred_element_type=jnp.float32)


def matmul_nt(left_mat, right_mat):
    return lax.dot_general(left_mat, right_mat, NT_DIMS, preferred_element_type=jnp.float32)


def exact_dot(left_mat, right_mat):
    return jnp.dot(left_mat, right_mat, precision=EXACT, preferred_element_type=jnp.float32)


def scope(name):
    return jax.named_scope(name) if SCOPED else contextlib.nullcontext()


def span_of(index, size):
    return pl.ds(pl.multiple_of(index * size, size), size)


class Place:
    def __init__(self):
        self.model, self.data = lax.axis_index('model'), lax.axis_index('data')
        self.core = lax.rem(self.data, 2)
        here = {'x': lax.div(self.data, 2), 'y': lax.rem(self.model, SIDE), 'z': lax.div(self.model, SIDE)}
        self.along = {dim: [at] + [lax.rem(at + step, SIDE) for step in range(1, SIDE)] for dim, at in here.items()}
        self.planes = [[z * SIDE + y for y in self.along['y']] for z in self.along['z']]
        self.lines = [x * 2 + self.core for x in self.along['x']]
        self.mate = (self.model, self.data + 1 - 2 * self.core)

    def at(self, dim, step):
        return self.along[dim][step % SIDE]

    def peer(self, z_step, y_step):
        return self.planes[z_step % SIDE][y_step % SIDE]

    def device(self, dim, step):
        if dim == 'x':
            return (self.model, self.lines[step % SIDE])
        return (self.peer(step, 0) if dim == 'z' else self.peer(0, step), self.data)


class Copies:
    def __init__(self, send_sems, recv_sems):
        self.send_sems, self.recv_sems = send_sems, recv_sems
        self.names, self.batches = {}, {}

    def start(self, batch, name, src, dst, device):
        num = self.names.setdefault((batch, name), len(self.names))
        out = self.batches.setdefault(batch, len(self.batches))
        pltpu.make_async_remote_copy(src_ref=src, dst_ref=dst, send_sem=self.send_sems.at[out], recv_sem=self.recv_sems.at[num], device_id=device, device_id_type=MESH).start()

    def wait(self, batch, name, ref):
        num = self.names.setdefault((batch, name), len(self.names))
        pltpu.make_async_copy(ref, ref, self.recv_sems.at[num]).wait()

    def left(self, batch, ref):
        pltpu.make_async_copy(ref, ref, self.send_sems.at[self.batches[batch]]).wait()


def call_out(devices):
    for device in devices:
        pl.semaphore_signal(pltpu.get_barrier_semaphore(), inc=1, device_id=device, device_id_type=MESH)


def all_here(devices):
    pl.semaphore_wait(pltpu.get_barrier_semaphore(), len(devices))


def plane_gather(copies, batch, place, region, like, on_piece):
    def steps(order, first, second):
        return (second, first) if order == 0 else (first, second)

    def send(order, name, k, part, first, second):
        z_step, y_step = steps(order, *k)
        ref = region(place.at('z', z_step), place.at('y', y_step), order, *part)
        copies.start(batch, name, ref, ref, (place.peer(*steps(order, first, second)), place.data))

    whole, low, high = (0, 2), (0, 1), (1, 2)

    def spread(order, k):
        for step in BOTH_WAYS:
            send(order, ('b', order, k), (k, 0), whole, 0, step)

    def pass_on(order, k):
        copies.wait(batch, ('b', order, k), like(4))
        for step, part in ((-1, low), (1, high)):
            send(order, ('end', k), (k, step), part, 0, -step)
            on_piece(order, *steps(order, k, step))

    for order in ORDERS:
        for step in BOTH_WAYS:
            send(order, 'a', (0, 0), whole, step, 0)
    for order in ORDERS:
        spread(order, 0)
    yield
    copies.wait(batch, 'a', like(8))
    for order in ORDERS:
        for step, part in ((-1, low), (1, high)):
            send(order, ('across', order), (step, 0), part, -step, 0)
            on_piece(order, *steps(order, step, 0))
    yield
    for step in BOTH_WAYS:
        for order in ORDERS:
            spread(order, step)
    yield
    for order in ORDERS:
        pass_on(order, 0)
        yield
    for order in ORDERS:
        copies.wait(batch, ('across', order), like(2))
        spread(order, 2)
        on_piece(order, *steps(order, 2, 0))
        yield
    for k in (-1, 1, 2):
        for order in ORDERS:
            pass_on(order, k)
            yield
    for k in (0, -1, 1, 2):
        copies.wait(batch, ('end', k), like(4))
        for order in ORDERS:
            on_piece(order, *steps(order, k, 2))
        yield


STEPS = [(a, b) for a in range(SIDE) for b in range(SIDE) if (a, b) != (0, 0)]


def line_reduce(copies, batch, place, src, near, far, store):
    core = place.core
    half = near.shape[1] // 2
    low, high = pl.ds(0, half), pl.ds(half, half)
    here, right, across, left = [place.at('x', step) for step in range(SIDE)]
    copies.start((batch, 'near'), ONLY, src.at[:, 1 - core], near, place.mate)
    yield
    copies.wait((batch, 'near'), ONLY, near)
    near[across] = near[across] + src[across, core]
    copies.start((batch, 'half'), 1, near.at[across, low], far.at[0, low], place.device('x', 1))
    copies.start((batch, 'half'), -1, near.at[across, high], far.at[0, high], place.device('x', -1))
    for there in (right, left, here):
        near[there] = near[there] + src[there, core]
    yield
    copies.wait((batch, 'half'), 1, far.at[0, low])
    near[right, low] = near[right, low] + far[0, low]
    copies.start((batch, 'full'), 1, near.at[right], far.at[1], place.device('x', 1))
    copies.wait((batch, 'half'), -1, far.at[0, high])
    near[left, high] = near[left, high] + far[0, high]
    copies.start((batch, 'full'), -1, near.at[left], far.at[2], place.device('x', -1))
    yield
    copies.wait((batch, 'full'), 1, far.at[1])
    copies.wait((batch, 'full'), -1, far.at[2])
    store(near[here] + far[1] + far[2])
    copies.left((batch, 'near'), near)
    copies.left((batch, 'half'), far.at[0])
    copies.left((batch, 'full'), far.at[pl.ds(1, 2)])
    yield


def line_gather(copies, batch, place, out):
    core = place.core
    half = out.shape[2] // 2
    here, right, across, left = [out.at[place.at('x', step), core] for step in range(SIDE)]

    def hand(ref):
        copies.start((batch, 'hand'), ONLY, ref, ref, place.mate)

    for step in BOTH_WAYS:
        copies.start((batch, 'all'), step, here, here, place.device('x', step))
    hand(here)
    yield
    for step, ref, span in ((1, left, pl.ds(0, half)), (-1, right, pl.ds(half, half))):
        copies.wait((batch, 'all'), step, ref)
        copies.start((batch, 'all'), 2 * step, ref.at[span], ref.at[span], place.device('x', step))
        hand(ref)
    yield
    for step, span in ((1, pl.ds(0, half)), (-1, pl.ds(half, half))):
        copies.wait((batch, 'all'), 2 * step, across.at[span])
    hand(across)
    yield
    copies.wait((batch, 'hand'), ONLY, out.at[:, 0])
    copies.left((batch, 'all'), out.at[0:3, 0])
    copies.left((batch, 'hand'), out.at[:, 0])
    yield


BALANCED = (('x', 'y', 'z'), ('y', 'z', 'x'), ('z', 'x', 'y'))
X_LAST = (('y', 'z', 'x'), ('z', 'y', 'x'))


def cube_gather(copies, batch, place, view, cuts, orders, one_way, owners=SIDE):
    core = place.core
    parts = [(order, pl.ds(start, end - start)) for order, start, end in zip(orders, cuts[:-1], cuts[1:])]
    every, low, high = (0, owners), (0, owners // 2), (owners // 2, owners // 2)

    def like(z, y, x):
        return view(0, *[pl.ds(0, num) if num > 1 else 0 for num in (z, y, x)], pl.ds(cuts[0], cuts[-1] - cuts[0]))

    def at(order, cols, places):
        where = dict(zip(order, places))
        return view(core, where['z'], where['y'], where['x'], cols)

    def single(order, cols):
        return at(order, cols, [place.at(dim, 0) for dim in order])

    def group(order, cols, a, b, span=every):
        return at(order, cols, (pl.ds(*span), place.at(order[1], a), place.at(order[2], b)))

    def hand(order, cols, a, b):
        ref = group(order, cols, a, b)
        copies.start((batch, 'mate'), ONLY, ref, ref, place.mate)

    def spread(order, cols, a):
        ref = group(order, cols, a, 0)
        for step in BOTH_WAYS:
            copies.start((batch, 'three'), a, ref, ref, place.device(order[2], step))
        hand(order, cols, a, 0)

    def ways(single_way, dim):
        return ((1, every),) if single_way and dim != 'x' else ((-1, low), (1, high))

    def pass_on(a):
        copies.wait((batch, 'three'), a, like(1, CORES, owners))
        for order, cols in parts:
            for step, span in ways(a in one_way, order[2]):
                half = group(order, cols, a, step, span)
                copies.start((batch, 'three'), ('end', a), half, half, place.device(order[2], -step))
            for step in BOTH_WAYS:
                hand(order, cols, a, step)

    def first_sends():
        for order, cols in parts:
            for step in (2, 1, -1):
                copies.start((batch, 'one'), ONLY, single(order, cols), single(order, cols), place.device(order[0], step))

    if owners == SIDE:
        first_sends()
        yield
        copies.wait((batch, 'one'), ONLY, like(1, 1, 3))
    else:
        pl.when(place.at('z', 0) < owners)(first_sends)
        yield
        pl.when(place.at('z', 0) < owners)(lambda: copies.wait((batch, 'one'), ONLY, like(1, 1, 1)))
        pl.when(place.at('z', 0) >= owners)(lambda: copies.wait((batch, 'one'), ONLY, like(1, 1, owners)))
    for order, cols in parts:
        for step in BOTH_WAYS:
            copies.start((batch, 'two'), ONLY, group(order, cols, 0, 0), group(order, cols, 0, 0), place.device(order[1], step))
    for order, cols in parts:
        spread(order, cols, 0)
    yield
    copies.wait((batch, 'two'), ONLY, like(1, CORES, owners))
    for order, cols in parts:
        for step, span in ways(len(one_way) > 2, order[1]):
            half = group(order, cols, step, 0, span)
            copies.start((batch, 'two'), 'end', half, half, place.device(order[1], -step))
    for order, cols in parts:
        for step in BOTH_WAYS:
            spread(order, cols, step)
    yield
    pass_on(0)
    yield
    copies.wait((batch, 'two'), 'end', like(1, 1, owners))
    for order, cols in parts:
        spread(order, cols, 2)
    yield
    for a in (-1, 1, 2):
        pass_on(a)
        yield
    for a in (0, -1, 1, 2):
        copies.wait((batch, 'three'), ('end', a), like(1, 1, owners))
        for order, cols in parts:
            hand(order, cols, a, 2)
        yield
    whole = like(SIDE, SIDE, owners)
    copies.wait((batch, 'mate'), ONLY, whole)
    copies.left((batch, 'mate'), whole)
    if owners == SIDE:
        copies.left((batch, 'one'), like(1, 1, 3))
    else:
        pl.when(place.at('z', 0) < owners)(lambda: copies.left((batch, 'one'), like(1, 1, 3)))
    copies.left((batch, 'two'), like(1, 3, owners))
    copies.left((batch, 'three'), like(3, SIDE, owners))
    yield


def pump(gen, name):
    with scope(name):
        next(gen, None)


def drain(gen, name):
    with scope(name):
        for _ in gen:
            pass


def step_kernel(scale, x_hbm, dy_hbm, w_col_hbm, w_row_hbm, a_old, s_old, a_inv, s_inv, fact, grads, w_col, w_row, x_buf, dy_buf, h_two, w_two, w_three, z_one, h_one, h_three,
                g_three, t_three, rows_buf, z_two, left, w_three_t, gram_src, gram_near, gram_far, old_buf, piece_buf, grad_src, grad_near,
                grad_far, grad_sum, grad_out, big_buf, load_sems, old_sems, big_sems, send_sems, recv_sems):
    place = Place()
    model_id, data_id, core = place.model, place.data, place.core
    spot, y_pos, z_pos = place.at('x', 0), place.at('y', 0), place.at('z', 0)
    copies = Copies(send_sems, recv_sems)
    my_rows = span_of(model_id, BLOCK)
    my_cols = span_of(model_id, BLOCK)
    my_part = pl.ds(pl.multiple_of(data_id * PIECE, PIECE), PIECE)
    g_one = t_three
    olds = [a_old.at[0], s_old.at[1], a_old.at[1], s_old.at[0]]
    chunk = 256
    n_chunks = WIDTH // chunk
    half_way = n_chunks // CORES
    met = [(place.peer(a, b), data_id) for a, b in STEPS] + [place.mate] + [place.device('x', step) for step in (1, 2, 3)]

    def load(src, dst, base, i):
        rows = span_of(i, chunk)
        return pltpu.make_async_copy(src.at[rows, :], dst.at[rows, :], load_sems.at[base + i])

    def load_x(i):
        return load(x_hbm, x_buf, 0, i)

    def load_dy(i):
        return load(dy_hbm, dy_buf, n_chunks, i)

    def load_old(mat, j):
        rows = pl.ds(pl.multiple_of(model_id * BLOCK + data_id * PIECE, PIECE), PIECE)
        cols = span_of(lax.rem(model_id + j, PLANE), BLOCK)
        return pltpu.make_async_copy(olds[mat].at[rows, cols], old_buf.at[mat, :, pl.ds(j * BLOCK, BLOCK)], old_sems.at[mat])

    def cols_of(buf, cols):
        return buf[:, cols] if len(buf.shape) == 2 else buf[:, :, :, :, :, cols].reshape(WIDTH, cols.size)

    def rows_of(buf, z_step, y_step):
        return buf[place.at('z', z_step), place.at('y', y_step)].reshape(BLOCK, WIDTH)

    call_out(met)
    own_w_two = pltpu.make_async_copy(w_row_hbm.at[0, my_part, :], w_two.at[z_pos, y_pos, spot, core], old_sems.at[4])
    own_w_two.start()
    load_w = [pltpu.make_async_copy(w_col_hbm, w_col, big_sems.at[0]), pltpu.make_async_copy(w_row_hbm, w_row, big_sems.at[1])]
    for move in load_w:
        move.start()
    for i in range(n_chunks):
        load_x(i).start()

    def z_one_step(i, carry):
        rows = span_of(i, chunk)
        load_x(i).wait()
        pre_act = matmul(x_buf[rows, :], w_col[0]).astype(jnp.bfloat16)
        z_one[rows, :] = pre_act
        h_one[rows, :] = activate(pre_act)
        return carry

    own_w_two.wait()
    with scope('greet'):
        all_here(met)

    def z_one_first():
        with scope('z1a'):
            for move in load_w:
                move.wait()
            w_three_t[...] = w_col[1].T
            w_three[z_pos, y_pos, spot, core] = w_three_t[my_part, :]
            lax.fori_loop(0, half_way, z_one_step, 0)
        for i in range(n_chunks):
            load_dy(i).start()
        for mat in range(4):
            for j in range(TRI):
                load_old(mat, j).start()

    def weight_thread(batch, buf, cuts, orders, one_way):
        def view(which, z, y, x, cols):
            return buf.at[z, y, x, which, :, cols]
        return cube_gather(copies, batch, place, view, cuts, orders, one_way)

    def z_one_rest():
        with scope('z1b'):
            lax.fori_loop(half_way, n_chunks, z_one_step, 0)

    def send_block(batch, cols_ref, a, b):
        peer = place.peer(a, b)
        copies.start(batch, ONLY, cols_ref.at[span_of(peer, BLOCK), :], rows_buf.at[:, my_cols], (peer, data_id))

    def wait_blocks(batch):
        others = rows_buf.at[:, 0:WIDTH - BLOCK]
        copies.wait(batch, ONLY, others)
        copies.left(batch, others)

    loaded = []

    def wait_dy():
        if not loaded:
            for i in range(n_chunks):
                load_dy(i).wait()
            loaded.append(True)

    def t_three_step(i, carry):
        rows = span_of(i, chunk)
        t_three[rows, :] = matmul_nt(dy_buf[rows, :], w_row[1]).astype(jnp.bfloat16)
        return carry

    def t_three_thread():
        wait_dy()
        for i in range(0, n_chunks, CORES):
            with scope('t3'):
                lax.fori_loop(i, i + CORES, t_three_step, 0)
            yield

    def turn(dst, src, cols):
        for i in range(4):
            rows = slice(i * 512, (i + 1) * 512)
            dst[:, rows] = (src[rows, cols] if len(src.shape) == 2 else src[i, :, :, :, :, cols].reshape(512, BLOCK)).T

    def gram_product(mat, lhs, right):
        def block_cols(j):
            return cols_of(right, span_of(lax.rem(model_id + j, PLANE), BLOCK))

        def gram_step(i, carry):
            block = matmul(lhs[...], jnp.concatenate([block_cols(2 * i), block_cols(2 * i + 1)], axis=1))
            gram_src[mat, :, :, :, span_of(i, chunk)] = block.reshape(SIDE, CORES, PIECE, chunk)
            return carry
        lax.fori_loop(0, TRI // 2, gram_step, 0)
        block = matmul(lhs[...], block_cols(TRI - 1))
        gram_src[mat, :, :, :, (TRI - 1) * BLOCK:] = block.reshape(SIDE, CORES, PIECE, BLOCK)

    def grad_product(lhs, right, same, slot):
        def grad_step(i, carry):
            cols = span_of(i, chunk)
            block = matmul(lhs[...], cols_of(right, cols))
            grad_src[slot, :, :, :, cols] = block.reshape(SIDE, CORES, PIECE, chunk)
            return carry
        lax.fori_loop(0, n_chunks, grad_step, 0)
        block = matmul(lhs[...], same[...])
        grad_src[slot, :, :, :, WIDTH:GRAD_COLS] = block.reshape(SIDE, CORES, PIECE, BLOCK)

    def store_factor(mat, total):
        pltpu.make_async_copy(old_buf.at[mat], old_buf.at[mat], old_sems.at[mat]).wait()
        mixed = FACTOR_DECAY * old_buf[mat] + scale * total
        piece_buf[mat] = mixed

    def sum_thread(mat):
        return line_reduce(copies, ('gram', mat), place, gram_src.at[mat], gram_near.at[mat], gram_far.at[mat], functools.partial(store_factor, mat))

    def factor_thread(first, count, cuts, orders, one_way, rest_order):
        mats = pl.ds(first, count)

        def view(which, z, y, x, cols):
            return fact.at[z, y, x, which, mats, :, cols]

        move = pltpu.make_async_copy(piece_buf.at[mats], fact.at[z_pos, y_pos, spot, core, mats], old_sems.at[4])
        move.start()
        move.wait()
        main = cube_gather(copies, ('fact', first), place, view, cuts, orders, one_way)
        rest = cube_gather(copies, ('rest', first), place, view, (TRI * BLOCK - BLOCK, FACTOR_COLS), (rest_order,), (), CORES)
        for _ in main:
            next(rest)
            yield


    def gram_job(mat, slot, right):
        if mat == 1:
            wait_dy()
        with scope('gram'):
            turn(left.at[slot], right, my_cols)
            gram_product(mat, left.at[slot], right)

    def grad_job(layer, slot, lhs, right):
        with scope('dW'):
            turn(left.at[slot], lhs, slice(0, BLOCK))
            grad_product(left.at[slot], right, lhs, layer % 2)
        if layer == 0:
            load_big(0, 0).start()
            load_big(0, 1).start()

    near_by = [(a, b) for a in range(SIDE) for b in range(SIDE) if 2 not in (a, b)]
    far_off = [where for where in [(0, 0)] + STEPS if where not in near_by]

    def picked(buf, places, cols):
        if len(buf.shape) == 2:
            parts = [buf[span_of(place.peer(a, b), BLOCK), cols] for a, b in places]
        else:
            parts = [buf[place.at('z', a), place.at('y', b), :, :, :, cols] for a, b in places]
        return [part.reshape(BLOCK, part.shape[-1]) for part in parts]

    def turn_picked(slot, buf, places, cols):
        for num, part in enumerate(picked(buf, places, cols)):
            left[slot, :, num * BLOCK:(num + 1) * BLOCK] = part.T

    def put(dst, cols, product, places):
        value = product.reshape(SIDE, CORES, PIECE, product.shape[-1])
        dst[:, :, :, cols] = value if places is near_by else dst[:, :, :, cols] + value

    def late_grad(layer, slot, lhs, right, places):
        def late_step(i, carry):
            cols = span_of(i, chunk)
            put(dst, cols, matmul(left[slot, :, :depth], jnp.concatenate(picked(right, places, cols), axis=0)), places)
            return carry

        dst, depth, block = grad_src.at[layer % 2], len(places) * BLOCK, slice(0, BLOCK)
        with scope('dW'):
            turn_picked(slot, lhs, places, block)
            lax.fori_loop(0, n_chunks, late_step, 0)
            put(dst, slice(WIDTH, GRAD_COLS), matmul(left[slot, :, :depth], jnp.concatenate(picked(lhs, places, block), axis=0)), places)

    def late_gram(mat, slot, right, places):
        def block_cols(j):
            return jnp.concatenate(picked(right, places, span_of(lax.rem(model_id + j, PLANE), BLOCK)), axis=0)

        def late_step(i, carry):
            put(dst, span_of(i, chunk), matmul(left[slot, :, :depth], jnp.concatenate([block_cols(2 * i), block_cols(2 * i + 1)], axis=1)), places)
            return carry

        dst, depth = gram_src.at[mat], len(places) * BLOCK
        with scope('gram'):
            turn_picked(slot, right, places, my_cols)
            lax.fori_loop(0, TRI // 2, late_step, 0)
            put(dst, slice((TRI - 1) * BLOCK, FACTOR_COLS), matmul(left[slot, :, :depth], block_cols(TRI - 1)), places)

    def swap_first():
        for a, b in STEPS:
            send_block('h1', h_one, a, b)
        rows_buf[:, my_cols] = h_one[my_rows, :]

    def z_two_step(i, carry):
        cols = span_of(i, chunk)
        pre_act = matmul(rows_buf[...], cols_of(w_two, cols)).astype(jnp.bfloat16)
        z_two[:, cols] = pre_act
        h_two[z_pos, y_pos, :, :, :, cols] = activate(pre_act).reshape(SIDE, CORES, PIECE, chunk)
        return carry

    def second_forward():
        drain(threads['w2'], 'w2_rest')
        with scope('wait_h1'):
            wait_blocks('h1')
        with scope('z2'):
            lax.fori_loop(0, n_chunks, z_two_step, 0)

    def forward_block(a, b):
        rows = span_of(place.peer(a, b), BLOCK)
        pre_act = matmul(rows_of(h_two, a, b), w_col[1]).astype(jnp.bfloat16)
        h_three[rows, :] = activate(pre_act)
        g_three[rows, :] = back_gate(t_three[rows, :], pre_act)
        if (a, b) != (0, 0):
            send_block('g3', g_three, a, b)

    def backward_block(a, b):
        rows = span_of(place.peer(a, b), BLOCK)
        grad = matmul_nt(rows_of(w_two, a, b), w_row[0]).astype(jnp.bfloat16)
        g_one[rows, :] = back_gate(grad, z_one[rows, :])

    def gather_tokens(tag, buf, block_step):
        seen = {}

        def on_piece(order, first, second):
            where = (first % SIDE, second % SIDE)
            seen[where] = seen.get(where, 0) + 1

        def region(z, y, order, lo, hi):
            return buf.at[z, y, pl.ds(2 * order + lo, hi - lo)]

        def like(quarters):
            return x_buf.at[0:quarters * BLOCK // 4, :]

        done = {(0, 0)}
        gen = plane_gather(copies, tag, place, region, like, on_piece)
        next(gen)
        with scope(tag + '_blocks'):
            block_step(0, 0)
        yield
        for _ in gen:
            ready = [where for where in sorted(seen) if seen[where] == 2 and where not in done]
            with scope(tag + '_blocks'):
                for where in ready:
                    block_step(*where)
            done.update(ready)
            yield
        copies.left(tag, x_buf.at[0:WIDTH - BLOCK, :])

    def split(value):
        high = value.astype(jnp.bfloat16)
        rest = value - high.astype(jnp.float32)
        middle = rest.astype(jnp.bfloat16)
        return high, middle, (rest - middle.astype(jnp.float32)).astype(jnp.bfloat16)

    inverses = [s_inv.at[1], a_inv.at[1], s_inv.at[0], a_inv.at[0]]
    big_rows = 2 * PIECE

    def load_big(layer, i):
        slot = lax.rem(i, CORES)
        return pltpu.make_async_copy(inverses[layer].at[span_of(i, chunk), span_of(core, HALF)], big_buf.at[slot], big_sems.at[slot])

    def grad_thread(layer):
        sum_ref, out_ref, tag = grad_sum.at[layer], grad_out.at[layer], ('grad', layer)

        def keep_sum(total):
            sum_ref[core] = total

        def big_step(i, carry):
            load_big(layer, i).wait()
            lhs = jnp.concatenate(split(sum_ref[:, :, span_of(i, chunk)].reshape(big_rows, chunk)), axis=0)
            high, middle, low = split(big_buf[lax.rem(i, CORES)])
            by_high, by_middle, by_low = matmul(lhs, high), matmul(lhs[:2 * big_rows], middle), matmul(lhs[:big_rows], low)
            small = by_high[2 * big_rows:] + by_middle[big_rows:] + by_low
            out_ref[:, :HALF] += by_high[:big_rows] + (by_high[big_rows:2 * big_rows] + by_middle[:big_rows] + small)

            @pl.when(i + 2 < n_chunks)
            def _():
                load_big(layer, i + 2).start()
            if layer < 3:
                @pl.when(i + 2 >= n_chunks)
                def _():
                    load_big(layer + 1, i + 2 - n_chunks).start()
            return carry

        yield from line_reduce(copies, tag, place, grad_src.at[layer % 2], grad_near.at[layer], grad_far.at[layer], keep_sum)
        copies.start(tag + ('pair',), ONLY, sum_ref.at[core], sum_ref.at[core], place.mate)
        yield
        copies.wait(tag + ('pair',), ONLY, sum_ref.at[1 - core])
        copies.left(tag + ('pair',), sum_ref.at[0])
        out_ref[...] = jnp.concatenate([jnp.zeros((big_rows, HALF), jnp.float32), sum_ref[:, :, WIDTH:].reshape(big_rows, BLOCK)], axis=1)
        with scope('X'):
            lax.fori_loop(0, half_way, big_step, 0)
        yield
        with scope('X'):
            lax.fori_loop(half_way, n_chunks, big_step, 0)
        move = pltpu.make_async_copy(out_ref, grads.at[layer, spot, core], old_sems.at[5])
        move.start()
        move.wait()
        yield from line_gather(copies, tag, place, grads.at[layer])

    def g_two_step(i, carry):
        cols = span_of(i, chunk)
        grad = matmul(rows_buf[...], cols_of(w_three, cols)).astype(jnp.bfloat16)
        w_two[z_pos, y_pos, :, :, :, cols] = back_gate(grad, z_two[:, cols]).reshape(SIDE, CORES, PIECE, chunk)
        return carry

    def second_backward():
        drain(threads['w3'], 'w3_rest')
        with scope('wait_g3'):
            wait_blocks('g3')
            rows_buf[:, my_cols] = g_three[my_rows, :]
        with scope('g2'):
            lax.fori_loop(0, n_chunks, g_two_step, 0)

    threads = dict(
        w2=weight_thread('w2', w_two, W_TWO_CUTS, BALANCED, W_TWO_WAYS),
        w3=weight_thread('w3', w_three, W_THREE_CUTS, MOSTLY_X, W_THREE_WAYS),
        h2=gather_tokens('h2', h_two, forward_block),
        g2=gather_tokens('g2', w_two, backward_block),
        pair=factor_thread(0, 2, PAIR_CUTS, MOSTLY_X, PAIR_WAYS, ('z', 'y', 'x')),
        fa3=factor_thread(2, 1, LATE_CUTS, BALANCED, LATE_WAYS, ('z', 'x', 'y')),
        fs2=factor_thread(3, 1, LATE_CUTS, BALANCED, LATE_WAYS, ('z', 'x', 'y')),
        sum0=sum_thread(0), sum1=sum_thread(1), sum2=sum_thread(2), sum3=sum_thread(3),
        t3=t_three_thread(),
        grad4=grad_thread(0), grad3=grad_thread(1), grad2=grad_thread(2), grad1=grad_thread(3),
    )
    steps = {name: functools.partial(pump, thread, name) for name, thread in threads.items()}
    steps.update(
        z0=z_one_first, z1=z_one_rest, swap=swap_first, z2=second_forward, back=second_backward,
        A1=functools.partial(gram_job, 0, 0, x_buf), S4=functools.partial(gram_job, 1, 1, dy_buf),
        A3=functools.partial(gram_job, 2, 0, h_two),
        S2a=functools.partial(late_gram, 3, 0, w_two, near_by), S2b=functools.partial(late_gram, 3, 0, w_two, far_off),
        dW4=functools.partial(grad_job, 0, 1, h_three, dy_buf), dW3=functools.partial(grad_job, 1, 0, g_three, h_two),
        dW2a=functools.partial(late_grad, 2, 0, h_one, w_two, near_by), dW2b=functools.partial(late_grad, 2, 0, h_one, w_two, far_off),
        dW1a=functools.partial(late_grad, 3, 1, g_one, x_buf, near_by), dW1b=functools.partial(late_grad, 3, 1, g_one, x_buf, far_off),
    )
    for step in plan(**steps):
        step()
    for name, thread in threads.items():
        drain(thread, name)
    assert len(copies.batches) == N_BATCHES and len(copies.names) == N_COPIES, (len(copies.batches), len(copies.names))


W_TWO_CUTS = (0, 640, 1408, 2048)
W_THREE_CUTS = (0, 640, 1920, 2048)
PAIR_CUTS = (0, 384, 896, 1024)
LATE_CUTS = (0, 512, 640, 1024)
W_TWO_WAYS = ()
W_THREE_WAYS = ()
PAIR_WAYS = (-1, 0)
LATE_WAYS = ()
MOSTLY_X = (('y', 'z', 'x'), ('z', 'y', 'x'), ('x', 'y', 'z'))


def plan(w2, w3, h2, g2, pair, fa3, fs2, sum0, sum1, sum2, sum3, grad4, grad3, grad2, grad1, z0, z1, swap, z2, back, A1, S4, A3, S2a, S2b, dW4, dW3, dW2a, dW2b, dW1a, dW1b, t3):
    return (
        w2, w2, z0, w3, z1, w2, A1, S4, sum0, w2, swap, sum0, sum1, w2, t3, t3, t3, t3, sum1, sum0, w2, sum1, sum0, w3, sum1, pair, w2, w2, w2, w3,
        w2, w3, w2, pair, w2, w2, w3, z2, h2, w3, h2, h2, w3, h2, w3, h2, w3, h2, h2, h2, h2, h2, h2, pair, h2, h2, h2, w3, h2, h2, h2, w3, pair,
        pair, dW4, w3, pair, w3, back, g2, grad4, dW3, grad3, grad4, A3, sum2, grad3, g2, g2, sum2, grad4, g2, grad3, g2, grad4, g2, sum2, pair,
        grad4, grad4, sum2, g2, g2, pair, grad3, g2, fa3, grad3, grad4, g2, g2, grad3, dW1a, grad3, g2, g2, pair, dW2a, fa3, S2a, g2, grad4, g2, g2,
        grad3, g2, S2b, dW2b, sum3, fa3, grad2, dW1b, grad1, sum3, grad2, grad1, sum3, grad2, fa3, sum3, fs2, fa3, fa3, grad3, fa3, pair, grad1,
        grad2, grad2, fs2, grad2, fa3, grad1, fa3, grad3, grad1, fa3, pair, grad2, fs2, grad1, fs2, grad1, fs2, fs2, pair, fa3, fs2, fa3, grad2,
        grad1, grad4, fs2, grad2, fs2, fs2, grad4, fs2, grad1, pair, fa3, fs2, grad2, grad1, fs2,
    )


N_BATCHES = 72
N_COPIES = 192


def step_call(x_tokens, dy_tokens, w_col, w_row, a_old, s_old, a_inv, s_inv, scale):
    f32, bf16 = jnp.float32, jnp.bfloat16
    tall, wide = (WIDTH, BLOCK), (BLOCK, WIDTH)
    cube = (SIDE, SIDE, SIDE, 2)
    rows = 2 * PIECE
    hbm = pl.BlockSpec(memory_space=pl.ANY)
    scratch = [pltpu.VMEM((2,) + tall, bf16), pltpu.VMEM((2,) + wide, bf16)] + [pltpu.VMEM((WIDTH, WIDTH), bf16)] * 2 + [pltpu.VMEM(cube + (PIECE, WIDTH), bf16)] * 3
    scratch += [pltpu.VMEM(tall, bf16)] * 5 + [pltpu.VMEM(wide, bf16)] * 2 + [pltpu.VMEM((2,) + wide, bf16), pltpu.VMEM(wide, bf16)]
    scratch += [pltpu.VMEM((SIDE, SIDE, CORES, PIECE, TRI * BLOCK), f32), pltpu.VMEM((SIDE, SIDE, PIECE, TRI * BLOCK), f32), pltpu.VMEM((4, 3, PIECE, TRI * BLOCK), f32)]
    scratch += [pltpu.VMEM((4, PIECE, TRI * BLOCK), f32), pltpu.VMEM((4, PIECE, FACTOR_COLS), f32)]
    scratch += [pltpu.VMEM((2, SIDE, CORES, PIECE, GRAD_COLS), f32), pltpu.VMEM((SIDE, SIDE, PIECE, GRAD_COLS), f32), pltpu.VMEM((4, 3, PIECE, GRAD_COLS), f32)]
    scratch += [pltpu.VMEM((4, 2, PIECE, GRAD_COLS), f32), pltpu.VMEM((4, rows, HALF + BLOCK), f32), pltpu.VMEM((2, 256, HALF), f32)]
    scratch += [pltpu.SemaphoreType.DMA((num,)) for num in (16, 6, 2, N_BATCHES, N_COPIES)]
    return pl.pallas_call(
        functools.partial(step_kernel, scale),
        out_shape=[jax.ShapeDtypeStruct(cube + (4, PIECE, FACTOR_COLS), f32), jax.ShapeDtypeStruct((4, SIDE, 2, rows, HALF + BLOCK), f32)],
        in_specs=[hbm] * 8,
        out_specs=[hbm, hbm],
        scratch_shapes=scratch,
        compiler_params=pltpu.CompilerParams(collective_id=0, has_side_effects=True, vmem_limit_bytes=67043328),
        name='step',
    )(x_tokens, dy_tokens, w_col, w_row, a_old, s_old, a_inv, s_inv)


def finish_kernel(scale, inv_rows, fact, grads, s_old_col, a_old_row, s_inv_col, a_inv_row, a_new, s_new, u_col, u_row, s_new_col, a_new_row, buf, turned, sums, u_col_buf, u_row_buf, load_sems, out_sems, turn_sems, far_sems, far_out_sems, small_sems):
    mid = PLANE // CORES
    outs = [(a_new, 0), (s_new, 1), (a_new, 1), (s_new, 0)]

    def load(mat, row):
        z, y = lax.div(row, SIDE), lax.rem(row, SIDE)
        return pltpu.make_async_copy(fact.at[z, y, :, :, mat], buf.at[mat, row], load_sems.at[mat * PLANE + row])

    def turn_done(slot):
        ref = turned.at[slot, pl.ds(0, TRI - 2)]
        return pltpu.make_async_copy(ref, ref, turn_sems.at[slot])

    def far_done(row):
        slot = lax.rem(row, CORES)
        ref = turned.at[slot, TRI - 2]
        return pltpu.make_async_copy(ref, ref, far_sems.at[slot])

    def start_load(mat):
        def body(row, carry):
            load(mat, row).start()
            return carry
        lax.fori_loop(0, PLANE, body, 0)

    load_sums = pltpu.make_async_copy(grads, sums, out_sems.at[4])
    load_sums.start()
    for mat in range(SIDE):
        start_load(mat)
    half = HALF

    def new_blocks():
        load_sums.wait()
        for layer in range(SIDE):
            block, num = scale * sums[layer, :, 0, :, half:].reshape(BLOCK, BLOCK), 1 - layer // 2
            if layer % 2 == 1:
                s_new_col[num] = FACTOR_DECAY * s_old_col[num] + block
            else:
                a_new_row[num] = FACTOR_DECAY * a_old_row[num] + block

    def move_small(batch):
        moves = [(u_col_buf, u_col), (u_row_buf, u_row)]
        return [pltpu.make_async_copy(src.at[1 - batch], dst.at[1 - batch], small_sems.at[2 * batch + num]) for num, (src, dst) in enumerate(moves)]

    chunk = 2 * BLOCK

    def small_product(layer, i):
        num = 1 - layer // 2
        core, cols, out = lax.div(i, SIDE), span_of(lax.rem(i, SIDE), chunk), span_of(i, chunk)
        product = sums[layer, :, core, :, cols].reshape(BLOCK, chunk)
        if layer % 2 == 1:
            u_col_buf[num, out, :] = exact_dot(product.T, s_inv_col[num]) * inv_rows
        else:
            u_row_buf[num, :, out] = exact_dot(a_inv_row[num], product) * inv_rows

    for mat, (out, num) in enumerate(outs):
        def row_step(row, carry):
            load(mat, row).wait()
            slot = lax.rem(row, CORES)
            if mat in (1, 2):
                @pl.when(row < mid)
                def _():
                    small_product(2 * mat - 2, row)

                @pl.when(row >= mid)
                def _():
                    small_product(2 * mat - 1, row - mid)
            far = TRI - 1
            def place_block(j, sem):
                cols = span_of(lax.rem(row + j, PLANE), BLOCK)
                pltpu.make_async_copy(buf.at[mat, row, :, :, :, pl.ds(j * BLOCK, BLOCK)], out.at[num, row, :, :, :, cols], sem).start()

            def place_turned(j, sem):
                block = buf[mat, row, :, :, :, j * BLOCK:(j + 1) * BLOCK].reshape(BLOCK, BLOCK).T
                turned[slot, j - 1] = block.reshape(SIDE, CORES, PIECE, BLOCK)
                pltpu.make_async_copy(turned.at[slot, j - 1], out.at[num, lax.rem(row + j, PLANE), :, :, :, span_of(row, BLOCK)], sem).start()

            for j in range(far):
                place_block(j, out_sems.at[mat])
            if mat > 0:
                turn_done(slot).wait()
            else:
                @pl.when(row >= 2)
                def _():
                    turn_done(slot).wait()
            for j in range(1, far):
                place_turned(j, turn_sems.at[slot])

            @pl.when(row < mid)
            def _():
                if mat > 0:
                    far_done(row).wait()
                else:
                    @pl.when(row >= 2)
                    def _():
                        far_done(row).wait()
                place_block(far, far_out_sems.at[mat])
                place_turned(far, far_sems.at[slot])
            return carry

        if mat == 1:
            new_blocks()
        lax.fori_loop(0, PLANE, row_step, 0)
        if mat in (1, 2):
            for move in move_small(mat - 1):
                move.start()
    for batch in range(CORES):
        for move in move_small(batch):
            move.wait()
    for slot in range(CORES):
        turn_done(slot).wait()
        far_done(slot).wait()
    for mat in range(SIDE):
        near, far = buf.at[mat, :, :, :, :, pl.ds(0, mid * BLOCK)], buf.at[mat, pl.ds(0, mid), :, :, :, pl.ds(0, BLOCK)]
        pltpu.make_async_copy(near, near, out_sems.at[mat]).wait()
        pltpu.make_async_copy(far, far, far_out_sems.at[mat]).wait()


def finish_call(fact, grads, s_old_col, a_old_row, s_inv_col, a_inv_row, scale, inv_rows):
    f32 = jnp.float32
    shapes = [(2, PLANE, SIDE, CORES, PIECE, WIDTH)] * 2 + [(2, WIDTH, BLOCK), (2, BLOCK, WIDTH)] + [(2, BLOCK, BLOCK)] * 2
    hbm, vmem = pl.BlockSpec(memory_space=pl.ANY), pl.BlockSpec(memory_space=pltpu.VMEM)
    return pl.pallas_call(
        functools.partial(finish_kernel, scale, inv_rows),
        out_shape=[jax.ShapeDtypeStruct(shape, f32) for shape in shapes],
        in_specs=[hbm] * 2 + [vmem] * 4,
        out_specs=[hbm] * 4 + [vmem] * 2,
        scratch_shapes=[pltpu.VMEM((4, PLANE, SIDE, CORES, PIECE, FACTOR_COLS), f32), pltpu.VMEM((2, TRI - 1, SIDE, CORES, PIECE, BLOCK), f32), pltpu.VMEM(grads.shape, f32), pltpu.VMEM((2, WIDTH, BLOCK), f32), pltpu.VMEM((2, BLOCK, WIDTH), f32)] + [pltpu.SemaphoreType.DMA((num,)) for num in (SIDE * PLANE, 5, CORES, CORES, SIDE, SIDE)],
        compiler_params=pltpu.CompilerParams(vmem_limit_bytes=67043328),
        name='finish',
    )(fact, grads, s_old_col, a_old_row, s_inv_col, a_inv_row)


def solution(mesh):
    def shard_body(x_tokens, dy_tokens, w_col, w_row, a_old_col, s_old_col, a_old_row, s_old_row, a_inv_col, s_inv_col, a_inv_row, s_inv_row):
        inv_rows = 1.0 / (x_tokens.shape[0] * DATA_WAYS)
        scale = (1.0 - FACTOR_DECAY) * inv_rows
        fact, grads = step_call(x_tokens, dy_tokens, w_col, w_row, a_old_col, s_old_row, a_inv_col, s_inv_row, scale)
        a_new_col, s_new_row, u_col, u_row, s_new_col, a_new_row = finish_call(fact, grads, s_old_col, a_old_row, s_inv_col, a_inv_row, scale, inv_rows)
        return (u_col, u_row, a_new_col.reshape(2, WIDTH, WIDTH), s_new_col, a_new_row, s_new_row.reshape(2, WIDTH, WIDTH))

    batch_split = P('data', None)
    col_split = P(None, None, 'model')
    row_split = P(None, 'model', None)
    replicated = P()
    return jax.shard_map(
        shard_body,
        mesh=mesh,
        in_specs=(batch_split, batch_split, col_split, row_split, replicated, row_split, row_split, replicated, replicated, row_split, row_split, replicated),
        out_specs=(col_split, row_split, replicated, row_split, row_split, replicated),
        check_vma=False,
    )
```

```python
import contextlib
import functools
import math
import jax
import jax.numpy as jnp
from jax import lax
from jax.experimental import pallas as pl
from jax.experimental.pallas import tpu as pltpu
from jax.sharding import PartitionSpec as P

FACTOR_DECAY = 0.8
GELU_SCALE = math.sqrt(2.0 / math.pi)
GELU_CUBIC = 0.044715
EXACT = lax.Precision.HIGHEST
MESH = pl.DeviceIdType.MESH
SIDE = 4
PLANE = 16
DATA_WAYS = 8
WIDTH = 2048
BLOCK = 128
PIECE = 16
TRI = 9
ONLY = 0
CORES = 2
BOTH_WAYS = (1, -1)
ORDERS = (0, 1)
HALF = WIDTH // 2
SCOPED = False
FACTOR_COLS = TRI * BLOCK
GRAD_COLS = WIDTH + BLOCK
NT_DIMS = (((1,), (1,)), ((), ()))


def gelu_value(pre_act):
    tanh_arg = GELU_SCALE * (pre_act + GELU_CUBIC * pre_act * pre_act * pre_act)
    return 0.5 * pre_act * (1.0 + jnp.tanh(tanh_arg))


def gelu_slope(pre_act):
    tanh_arg = GELU_SCALE * (pre_act + GELU_CUBIC * pre_act * pre_act * pre_act)
    tanh_val = jnp.tanh(tanh_arg)
    return 0.5 * (1.0 + tanh_val) + 0.5 * pre_act * (1.0 - tanh_val * tanh_val) * GELU_SCALE * (1.0 + 3.0 * GELU_CUBIC * pre_act * pre_act)


def activate(pre_act):
    return gelu_value(pre_act.astype(jnp.float32)).astype(jnp.bfloat16)


def back_gate(grad_act, pre_act):
    return (grad_act.astype(jnp.float32) * gelu_slope(pre_act.astype(jnp.float32))).astype(jnp.bfloat16)


def matmul(left_mat, right_mat):
    return jnp.dot(left_mat, right_mat, preferred_element_type=jnp.float32)


def matmul_nt(left_mat, right_mat):
    return lax.dot_general(left_mat, right_mat, NT_DIMS, preferred_element_type=jnp.float32)


def exact_dot(left_mat, right_mat):
    return jnp.dot(left_mat, right_mat, precision=EXACT, preferred_element_type=jnp.float32)


def scope(name):
    return jax.named_scope(name) if SCOPED else contextlib.nullcontext()


def span_of(index, size):
    return pl.ds(pl.multiple_of(index * size, size), size)


class Place:
    def __init__(self):
        self.model, self.data = lax.axis_index('model'), lax.axis_index('data')
        self.core = lax.rem(self.data, 2)
        here = {'x': lax.div(self.data, 2), 'y': lax.rem(self.model, SIDE), 'z': lax.div(self.model, SIDE)}
        self.along = {dim: [at] + [lax.rem(at + step, SIDE) for step in range(1, SIDE)] for dim, at in here.items()}
        self.planes = [[z * SIDE + y for y in self.along['y']] for z in self.along['z']]
        self.lines = [x * 2 + self.core for x in self.along['x']]
        self.mate = (self.model, self.data + 1 - 2 * self.core)

    def at(self, dim, step):
        return self.along[dim][step % SIDE]

    def peer(self, z_step, y_step):
        return self.planes[z_step % SIDE][y_step % SIDE]

    def device(self, dim, step):
        if dim == 'x':
            return (self.model, self.lines[step % SIDE])
        return (self.peer(step, 0) if dim == 'z' else self.peer(0, step), self.data)


class Copies:
    def __init__(self, send_sems, recv_sems):
        self.send_sems, self.recv_sems = send_sems, recv_sems
        self.names, self.batches = {}, {}

    def start(self, batch, name, src, dst, device):
        num = self.names.setdefault((batch, name), len(self.names))
        out = self.batches.setdefault(batch, len(self.batches))
        pltpu.make_async_remote_copy(src_ref=src, dst_ref=dst, send_sem=self.send_sems.at[out], recv_sem=self.recv_sems.at[num], device_id=device, device_id_type=MESH).start()

    def wait(self, batch, name, ref):
        num = self.names.setdefault((batch, name), len(self.names))
        pltpu.make_async_copy(ref, ref, self.recv_sems.at[num]).wait()

    def left(self, batch, ref):
        pltpu.make_async_copy(ref, ref, self.send_sems.at[self.batches[batch]]).wait()


def call_out(devices):
    for device in devices:
        pl.semaphore_signal(pltpu.get_barrier_semaphore(), inc=1, device_id=device, device_id_type=MESH)


def all_here(devices):
    pl.semaphore_wait(pltpu.get_barrier_semaphore(), len(devices))


def plane_gather(copies, batch, place, region, like, on_piece):
    def steps(order, first, second):
        return (second, first) if order == 0 else (first, second)

    def send(order, name, k, part, first, second):
        z_step, y_step = steps(order, *k)
        ref = region(place.at('z', z_step), place.at('y', y_step), order, *part)
        copies.start(batch, name, ref, ref, (place.peer(*steps(order, first, second)), place.data))

    whole, low, high = (0, 2), (0, 1), (1, 2)

    def spread(order, k):
        for step in BOTH_WAYS:
            send(order, ('b', order, k), (k, 0), whole, 0, step)

    def pass_on(order, k):
        copies.wait(batch, ('b', order, k), like(4))
        for step, part in ((-1, low), (1, high)):
            send(order, ('end', k), (k, step), part, 0, -step)
            on_piece(order, *steps(order, k, step))

    for order in ORDERS:
        for step in BOTH_WAYS:
            send(order, 'a', (0, 0), whole, step, 0)
    for order in ORDERS:
        spread(order, 0)
    yield
    copies.wait(batch, 'a', like(8))
    for order in ORDERS:
        for step, part in ((-1, low), (1, high)):
            send(order, ('across', order), (step, 0), part, -step, 0)
            on_piece(order, *steps(order, step, 0))
    yield
    for step in BOTH_WAYS:
        for order in ORDERS:
            spread(order, step)
    yield
    for order in ORDERS:
        pass_on(order, 0)
        yield
    for order in ORDERS:
        copies.wait(batch, ('across', order), like(2))
        spread(order, 2)
        on_piece(order, *steps(order, 2, 0))
        yield
    for k in (-1, 1, 2):
        for order in ORDERS:
            pass_on(order, k)
            yield
    for k in (0, -1, 1, 2):
        copies.wait(batch, ('end', k), like(4))
        for order in ORDERS:
            on_piece(order, *steps(order, k, 2))
        yield


STEPS = [(a, b) for a in range(SIDE) for b in range(SIDE) if (a, b) != (0, 0)]


def line_reduce(copies, batch, place, src, near, far, store):
    core = place.core
    half = near.shape[1] // 2
    low, high = pl.ds(0, half), pl.ds(half, half)
    here, right, across, left = [place.at('x', step) for step in range(SIDE)]
    copies.start((batch, 'near'), ONLY, src.at[:, 1 - core], near, place.mate)
    yield
    copies.wait((batch, 'near'), ONLY, near)
    near[across] = near[across] + src[across, core]
    copies.start((batch, 'half'), ONLY, near.at[across, low], far.at[0, low], place.device('x', 1))
    copies.start((batch, 'half'), ONLY, near.at[across, high], far.at[0, high], place.device('x', -1))
    for there in (right, left, here):
        near[there] = near[there] + src[there, core]
    yield
    copies.wait((batch, 'half'), ONLY, far.at[0])
    near[right, low] = near[right, low] + far[0, low]
    copies.start((batch, 'full'), ONLY, near.at[right], far.at[1], place.device('x', 1))
    near[left, high] = near[left, high] + far[0, high]
    copies.start((batch, 'full'), ONLY, near.at[left], far.at[2], place.device('x', -1))
    yield
    copies.wait((batch, 'full'), ONLY, far.at[pl.ds(1, 2)])
    store(near[here] + far[1] + far[2])
    copies.left((batch, 'near'), near)
    copies.left((batch, 'half'), far.at[0])
    copies.left((batch, 'full'), far.at[pl.ds(1, 2)])
    yield


def line_gather(copies, batch, place, out):
    core = place.core
    half = out.shape[2] // 2
    here, right, across, left = [out.at[place.at('x', step), core] for step in range(SIDE)]

    def hand(ref):
        copies.start((batch, 'hand'), ONLY, ref, ref, place.mate)

    for step in BOTH_WAYS:
        copies.start((batch, 'all'), ONLY, here, here, place.device('x', step))
    hand(here)
    yield
    copies.wait((batch, 'all'), ONLY, out.at[pl.ds(0, 2), 0])
    for step, ref, span in ((1, left, pl.ds(0, half)), (-1, right, pl.ds(half, half))):
        copies.start((batch, 'all'), 'end', ref.at[span], ref.at[span], place.device('x', step))
        hand(ref)
    yield
    copies.wait((batch, 'all'), 'end', out.at[0, 0])
    hand(across)
    yield
    copies.wait((batch, 'hand'), ONLY, out.at[:, 0])
    copies.left((batch, 'all'), out.at[0:3, 0])
    copies.left((batch, 'hand'), out.at[:, 0])
    yield


BALANCED = (('x', 'y', 'z'), ('y', 'z', 'x'), ('z', 'x', 'y'))
X_LAST = (('y', 'z', 'x'), ('z', 'y', 'x'))


def cube_gather(copies, batch, place, view, cuts, orders, one_way, owners=SIDE):
    core = place.core
    parts = [(order, pl.ds(start, end - start)) for order, start, end in zip(orders, cuts[:-1], cuts[1:])]
    every, low, high = (0, owners), (0, owners // 2), (owners // 2, owners // 2)

    def like(z, y, x):
        return view(0, *[pl.ds(0, num) if num > 1 else 0 for num in (z, y, x)], pl.ds(cuts[0], cuts[-1] - cuts[0]))

    def at(order, cols, places):
        where = dict(zip(order, places))
        return view(core, where['z'], where['y'], where['x'], cols)

    def single(order, cols):
        return at(order, cols, [place.at(dim, 0) for dim in order])

    def group(order, cols, a, b, span=every):
        return at(order, cols, (pl.ds(*span), place.at(order[1], a), place.at(order[2], b)))

    def hand(order, cols, a, b):
        ref = group(order, cols, a, b)
        copies.start((batch, 'mate'), ONLY, ref, ref, place.mate)

    def spread(order, cols, a):
        ref = group(order, cols, a, 0)
        for step in BOTH_WAYS:
            copies.start((batch, 'three'), a, ref, ref, place.device(order[2], step))
        hand(order, cols, a, 0)

    def ways(single_way, dim):
        return ((1, every),) if single_way and dim != 'x' else ((-1, low), (1, high))

    def pass_on(a):
        copies.wait((batch, 'three'), a, like(1, CORES, owners))
        for order, cols in parts:
            for step, span in ways(a in one_way, order[2]):
                half = group(order, cols, a, step, span)
                copies.start((batch, 'three'), ('end', a), half, half, place.device(order[2], -step))
            for step in BOTH_WAYS:
                hand(order, cols, a, step)

    def first_sends():
        for order, cols in parts:
            for step in (2, 1, -1):
                copies.start((batch, 'one'), ONLY, single(order, cols), single(order, cols), place.device(order[0], step))

    if owners == SIDE:
        first_sends()
        yield
        copies.wait((batch, 'one'), ONLY, like(1, 1, 3))
    else:
        pl.when(place.at('z', 0) < owners)(first_sends)
        yield
        pl.when(place.at('z', 0) < owners)(lambda: copies.wait((batch, 'one'), ONLY, like(1, 1, 1)))
        pl.when(place.at('z', 0) >= owners)(lambda: copies.wait((batch, 'one'), ONLY, like(1, 1, owners)))
    for order, cols in parts:
        for step in BOTH_WAYS:
            copies.start((batch, 'two'), ONLY, group(order, cols, 0, 0), group(order, cols, 0, 0), place.device(order[1], step))
    for order, cols in parts:
        spread(order, cols, 0)
    yield
    copies.wait((batch, 'two'), ONLY, like(1, CORES, owners))
    for order, cols in parts:
        for step, span in ways(len(one_way) > 2, order[1]):
            half = group(order, cols, step, 0, span)
            copies.start((batch, 'two'), 'end', half, half, place.device(order[1], -step))
    for order, cols in parts:
        for step in BOTH_WAYS:
            spread(order, cols, step)
    yield
    pass_on(0)
    yield
    copies.wait((batch, 'two'), 'end', like(1, 1, owners))
    for order, cols in parts:
        spread(order, cols, 2)
    yield
    for a in (-1, 1, 2):
        pass_on(a)
        yield
    for a in (0, -1, 1, 2):
        copies.wait((batch, 'three'), ('end', a), like(1, 1, owners))
        for order, cols in parts:
            hand(order, cols, a, 2)
        yield
    whole = like(SIDE, SIDE, owners)
    copies.wait((batch, 'mate'), ONLY, whole)
    copies.left((batch, 'mate'), whole)
    if owners == SIDE:
        copies.left((batch, 'one'), like(1, 1, 3))
    else:
        pl.when(place.at('z', 0) < owners)(lambda: copies.left((batch, 'one'), like(1, 1, 3)))
    copies.left((batch, 'two'), like(1, 3, owners))
    copies.left((batch, 'three'), like(3, SIDE, owners))
    yield


def pump(gen, name):
    with scope(name):
        next(gen, None)


def drain(gen, name):
    with scope(name):
        for _ in gen:
            pass


def step_kernel(scale, x_hbm, dy_hbm, w_col_hbm, w_row_hbm, a_old, s_old, a_inv, s_inv, fact, grads, w_col, w_row, x_buf, dy_buf, h_two, w_two, w_three, z_one, h_one, h_three,
                g_three, t_three, rows_buf, z_two, left, w_three_t, gram_src, gram_near, gram_far, old_buf, piece_buf, grad_src, grad_near,
                grad_far, grad_sum, grad_out, big_buf, load_sems, old_sems, big_sems, send_sems, recv_sems):
    place = Place()
    model_id, data_id, core = place.model, place.data, place.core
    spot, y_pos, z_pos = place.at('x', 0), place.at('y', 0), place.at('z', 0)
    copies = Copies(send_sems, recv_sems)
    my_rows = span_of(model_id, BLOCK)
    my_cols = span_of(model_id, BLOCK)
    my_part = pl.ds(pl.multiple_of(data_id * PIECE, PIECE), PIECE)
    g_one = t_three
    olds = [a_old.at[0], s_old.at[1], a_old.at[1], s_old.at[0]]
    chunk = 256
    n_chunks = WIDTH // chunk
    half_way = n_chunks // CORES
    met = [(place.peer(a, b), data_id) for a, b in STEPS] + [place.mate] + [place.device('x', step) for step in (1, 2, 3)]

    def load(src, dst, base, i):
        rows = span_of(i, chunk)
        return pltpu.make_async_copy(src.at[rows, :], dst.at[rows, :], load_sems.at[base + i])

    def load_x(i):
        return load(x_hbm, x_buf, 0, i)

    def load_dy(i):
        return load(dy_hbm, dy_buf, n_chunks, i)

    def load_old(mat, j):
        rows = pl.ds(pl.multiple_of(model_id * BLOCK + data_id * PIECE, PIECE), PIECE)
        cols = span_of(lax.rem(model_id + j, PLANE), BLOCK)
        return pltpu.make_async_copy(olds[mat].at[rows, cols], old_buf.at[mat, :, pl.ds(j * BLOCK, BLOCK)], old_sems.at[mat])

    def cols_of(buf, cols):
        return buf[:, cols] if len(buf.shape) == 2 else buf[:, :, :, :, :, cols].reshape(WIDTH, cols.size)

    def rows_of(buf, z_step, y_step):
        return buf[place.at('z', z_step), place.at('y', y_step)].reshape(BLOCK, WIDTH)

    call_out(met)
    own_w_two = pltpu.make_async_copy(w_row_hbm.at[0, my_part, :], w_two.at[z_pos, y_pos, spot, core], old_sems.at[4])
    own_w_two.start()
    load_w = [pltpu.make_async_copy(w_col_hbm, w_col, big_sems.at[0]), pltpu.make_async_copy(w_row_hbm, w_row, big_sems.at[1])]
    for move in load_w:
        move.start()
    for i in range(n_chunks):
        load_x(i).start()

    def z_one_step(i, carry):
        rows = span_of(i, chunk)
        load_x(i).wait()
        pre_act = matmul(x_buf[rows, :], w_col[0]).astype(jnp.bfloat16)
        z_one[rows, :] = pre_act
        h_one[rows, :] = activate(pre_act)
        return carry

    own_w_two.wait()
    with scope('greet'):
        all_here(met)

    def z_one_first():
        with scope('z1a'):
            for move in load_w:
                move.wait()
            w_three_t[...] = w_col[1].T
            w_three[z_pos, y_pos, spot, core] = w_three_t[my_part, :]
            lax.fori_loop(0, half_way, z_one_step, 0)
        for i in range(n_chunks):
            load_dy(i).start()
        for mat in range(4):
            for j in range(TRI):
                load_old(mat, j).start()

    def weight_thread(batch, buf, cuts, orders, one_way):
        def view(which, z, y, x, cols):
            return buf.at[z, y, x, which, :, cols]
        return cube_gather(copies, batch, place, view, cuts, orders, one_way)

    def z_one_rest():
        with scope('z1b'):
            lax.fori_loop(half_way, n_chunks, z_one_step, 0)

    def send_block(batch, cols_ref, a, b):
        peer = place.peer(a, b)
        copies.start(batch, ONLY, cols_ref.at[span_of(peer, BLOCK), :], rows_buf.at[:, my_cols], (peer, data_id))

    def wait_blocks(batch):
        others = rows_buf.at[:, 0:WIDTH - BLOCK]
        copies.wait(batch, ONLY, others)
        copies.left(batch, others)

    loaded = []

    def wait_dy():
        if not loaded:
            for i in range(n_chunks):
                load_dy(i).wait()
            loaded.append(True)

    def t_three_step(i, carry):
        rows = span_of(i, chunk)
        t_three[rows, :] = matmul_nt(dy_buf[rows, :], w_row[1]).astype(jnp.bfloat16)
        return carry

    def t_three_thread():
        wait_dy()
        for i in range(0, n_chunks, CORES):
            with scope('t3'):
                lax.fori_loop(i, i + CORES, t_three_step, 0)
            yield

    def turn(dst, src, cols):
        for i in range(4):
            rows = slice(i * 512, (i + 1) * 512)
            dst[:, rows] = (src[rows, cols] if len(src.shape) == 2 else src[i, :, :, :, :, cols].reshape(512, BLOCK)).T

    def gram_product(mat, lhs, right):
        def block_cols(j):
            return cols_of(right, span_of(lax.rem(model_id + j, PLANE), BLOCK))

        def gram_step(i, carry):
            block = matmul(lhs[...], jnp.concatenate([block_cols(2 * i), block_cols(2 * i + 1)], axis=1))
            gram_src[mat, :, :, :, span_of(i, chunk)] = block.reshape(SIDE, CORES, PIECE, chunk)
            return carry
        lax.fori_loop(0, TRI // 2, gram_step, 0)
        block = matmul(lhs[...], block_cols(TRI - 1))
        gram_src[mat, :, :, :, (TRI - 1) * BLOCK:] = block.reshape(SIDE, CORES, PIECE, BLOCK)

    def grad_product(lhs, right, same, slot):
        def grad_step(i, carry):
            cols = span_of(i, chunk)
            block = matmul(lhs[...], cols_of(right, cols))
            grad_src[slot, :, :, :, cols] = block.reshape(SIDE, CORES, PIECE, chunk)
            return carry
        lax.fori_loop(0, n_chunks, grad_step, 0)
        block = matmul(lhs[...], same[...])
        grad_src[slot, :, :, :, WIDTH:GRAD_COLS] = block.reshape(SIDE, CORES, PIECE, BLOCK)

    def store_factor(mat, total):
        pltpu.make_async_copy(old_buf.at[mat], old_buf.at[mat], old_sems.at[mat]).wait()
        mixed = FACTOR_DECAY * old_buf[mat] + scale * total
        piece_buf[mat] = mixed

    def sum_thread(mat):
        return line_reduce(copies, ('gram', mat), place, gram_src.at[mat], gram_near.at[mat], gram_far.at[mat], functools.partial(store_factor, mat))

    def factor_thread(first, count, cuts, orders, one_way, rest_order):
        mats = pl.ds(first, count)

        def view(which, z, y, x, cols):
            return fact.at[z, y, x, which, mats, :, cols]

        move = pltpu.make_async_copy(piece_buf.at[mats], fact.at[z_pos, y_pos, spot, core, mats], old_sems.at[4])
        move.start()
        move.wait()
        main = cube_gather(copies, ('fact', first), place, view, cuts, orders, one_way)
        rest = cube_gather(copies, ('rest', first), place, view, (TRI * BLOCK - BLOCK, FACTOR_COLS), (rest_order,), (), CORES)
        for _ in main:
            next(rest)
            yield


    def gram_job(mat, slot, right):
        if mat == 1:
            wait_dy()
        with scope('gram'):
            turn(left.at[slot], right, my_cols)
            gram_product(mat, left.at[slot], right)

    def grad_job(layer, slot, lhs, right):
        with scope('dW'):
            turn(left.at[slot], lhs, slice(0, BLOCK))
            grad_product(left.at[slot], right, lhs, layer % 2)
        if layer == 0:
            load_big(0, 0).start()
            load_big(0, 1).start()

    near_by = [(a, b) for a in range(SIDE) for b in range(SIDE) if 2 not in (a, b)]
    far_off = [where for where in [(0, 0)] + STEPS if where not in near_by]

    def picked(buf, places, cols):
        if len(buf.shape) == 2:
            parts = [buf[span_of(place.peer(a, b), BLOCK), cols] for a, b in places]
        else:
            parts = [buf[place.at('z', a), place.at('y', b), :, :, :, cols] for a, b in places]
        return [part.reshape(BLOCK, part.shape[-1]) for part in parts]

    def turn_picked(slot, buf, places, cols):
        for num, part in enumerate(picked(buf, places, cols)):
            left[slot, :, num * BLOCK:(num + 1) * BLOCK] = part.T

    def put(dst, cols, product, places):
        value = product.reshape(SIDE, CORES, PIECE, product.shape[-1])
        dst[:, :, :, cols] = value if places is near_by else dst[:, :, :, cols] + value

    def late_grad(layer, slot, lhs, right, places):
        def late_step(i, carry):
            cols = span_of(i, chunk)
            put(dst, cols, matmul(left[slot, :, :depth], jnp.concatenate(picked(right, places, cols), axis=0)), places)
            return carry

        dst, depth, block = grad_src.at[layer % 2], len(places) * BLOCK, slice(0, BLOCK)
        with scope('dW'):
            turn_picked(slot, lhs, places, block)
            lax.fori_loop(0, n_chunks, late_step, 0)
            put(dst, slice(WIDTH, GRAD_COLS), matmul(left[slot, :, :depth], jnp.concatenate(picked(lhs, places, block), axis=0)), places)

    def late_gram(mat, slot, right, places):
        def block_cols(j):
            return jnp.concatenate(picked(right, places, span_of(lax.rem(model_id + j, PLANE), BLOCK)), axis=0)

        def late_step(i, carry):
            put(dst, span_of(i, chunk), matmul(left[slot, :, :depth], jnp.concatenate([block_cols(2 * i), block_cols(2 * i + 1)], axis=1)), places)
            return carry

        dst, depth = gram_src.at[mat], len(places) * BLOCK
        with scope('gram'):
            turn_picked(slot, right, places, my_cols)
            lax.fori_loop(0, TRI // 2, late_step, 0)
            put(dst, slice((TRI - 1) * BLOCK, FACTOR_COLS), matmul(left[slot, :, :depth], block_cols(TRI - 1)), places)

    def swap_first():
        for a, b in STEPS:
            send_block('h1', h_one, a, b)
        rows_buf[:, my_cols] = h_one[my_rows, :]

    def z_two_step(i, carry):
        cols = span_of(i, chunk)
        pre_act = matmul(rows_buf[...], cols_of(w_two, cols)).astype(jnp.bfloat16)
        z_two[:, cols] = pre_act
        h_two[z_pos, y_pos, :, :, :, cols] = activate(pre_act).reshape(SIDE, CORES, PIECE, chunk)
        return carry

    def second_forward():
        drain(threads['w2'], 'w2_rest')
        with scope('wait_h1'):
            wait_blocks('h1')
        with scope('z2'):
            lax.fori_loop(0, n_chunks, z_two_step, 0)

    def forward_block(a, b):
        rows = span_of(place.peer(a, b), BLOCK)
        pre_act = matmul(rows_of(h_two, a, b), w_col[1]).astype(jnp.bfloat16)
        h_three[rows, :] = activate(pre_act)
        g_three[rows, :] = back_gate(t_three[rows, :], pre_act)
        if (a, b) != (0, 0):
            send_block('g3', g_three, a, b)

    def backward_block(a, b):
        rows = span_of(place.peer(a, b), BLOCK)
        grad = matmul_nt(rows_of(w_two, a, b), w_row[0]).astype(jnp.bfloat16)
        g_one[rows, :] = back_gate(grad, z_one[rows, :])

    def gather_tokens(tag, buf, block_step):
        seen = {}

        def on_piece(order, first, second):
            where = (first % SIDE, second % SIDE)
            seen[where] = seen.get(where, 0) + 1

        def region(z, y, order, lo, hi):
            return buf.at[z, y, pl.ds(2 * order + lo, hi - lo)]

        def like(quarters):
            return x_buf.at[0:quarters * BLOCK // 4, :]

        done = {(0, 0)}
        gen = plane_gather(copies, tag, place, region, like, on_piece)
        next(gen)
        with scope(tag + '_blocks'):
            block_step(0, 0)
        yield
        for _ in gen:
            ready = [where for where in sorted(seen) if seen[where] == 2 and where not in done]
            with scope(tag + '_blocks'):
                for where in ready:
                    block_step(*where)
            done.update(ready)
            yield
        copies.left(tag, x_buf.at[0:WIDTH - BLOCK, :])

    def split(value):
        high = value.astype(jnp.bfloat16)
        rest = value - high.astype(jnp.float32)
        middle = rest.astype(jnp.bfloat16)
        return high, middle, (rest - middle.astype(jnp.float32)).astype(jnp.bfloat16)

    inverses = [s_inv.at[1], a_inv.at[1], s_inv.at[0], a_inv.at[0]]
    big_rows = 2 * PIECE

    def load_big(layer, i):
        slot = lax.rem(i, CORES)
        return pltpu.make_async_copy(inverses[layer].at[span_of(i, chunk), span_of(core, HALF)], big_buf.at[slot], big_sems.at[slot])

    def grad_thread(layer):
        sum_ref, out_ref, tag = grad_sum.at[layer], grad_out.at[layer], ('grad', layer)

        def keep_sum(total):
            sum_ref[core] = total

        def big_step(i, carry):
            load_big(layer, i).wait()
            lhs = jnp.concatenate(split(sum_ref[:, :, span_of(i, chunk)].reshape(big_rows, chunk)), axis=0)
            high, middle, low = split(big_buf[lax.rem(i, CORES)])
            by_high, by_middle, by_low = matmul(lhs, high), matmul(lhs[:2 * big_rows], middle), matmul(lhs[:big_rows], low)
            small = by_high[2 * big_rows:] + by_middle[big_rows:] + by_low
            out_ref[:, :HALF] += by_high[:big_rows] + (by_high[big_rows:2 * big_rows] + by_middle[:big_rows] + small)

            @pl.when(i + 2 < n_chunks)
            def _():
                load_big(layer, i + 2).start()
            if layer < 3:
                @pl.when(i + 2 >= n_chunks)
                def _():
                    load_big(layer + 1, i + 2 - n_chunks).start()
            return carry

        yield from line_reduce(copies, tag, place, grad_src.at[layer % 2], grad_near.at[layer], grad_far.at[layer], keep_sum)
        copies.start(tag + ('pair',), ONLY, sum_ref.at[core], sum_ref.at[core], place.mate)
        yield
        copies.wait(tag + ('pair',), ONLY, sum_ref.at[1 - core])
        copies.left(tag + ('pair',), sum_ref.at[0])
        out_ref[...] = jnp.concatenate([jnp.zeros((big_rows, HALF), jnp.float32), sum_ref[:, :, WIDTH:].reshape(big_rows, BLOCK)], axis=1)
        with scope('X'):
            lax.fori_loop(0, half_way, big_step, 0)
        yield
        with scope('X'):
            lax.fori_loop(half_way, n_chunks, big_step, 0)
        move = pltpu.make_async_copy(out_ref, grads.at[layer, spot, core], old_sems.at[5])
        move.start()
        move.wait()
        yield from line_gather(copies, tag, place, grads.at[layer])

    def g_two_step(i, carry):
        cols = span_of(i, chunk)
        grad = matmul(rows_buf[...], cols_of(w_three, cols)).astype(jnp.bfloat16)
        w_two[z_pos, y_pos, :, :, :, cols] = back_gate(grad, z_two[:, cols]).reshape(SIDE, CORES, PIECE, chunk)
        return carry

    def second_backward():
        drain(threads['w3'], 'w3_rest')
        with scope('wait_g3'):
            wait_blocks('g3')
            rows_buf[:, my_cols] = g_three[my_rows, :]
        with scope('g2'):
            lax.fori_loop(0, n_chunks, g_two_step, 0)

    threads = dict(
        w2=weight_thread('w2', w_two, W_TWO_CUTS, BALANCED, W_TWO_WAYS),
        w3=weight_thread('w3', w_three, W_THREE_CUTS, MOSTLY_X, W_THREE_WAYS),
        h2=gather_tokens('h2', h_two, forward_block),
        g2=gather_tokens('g2', w_two, backward_block),
        pair=factor_thread(0, 2, PAIR_CUTS, MOSTLY_X, PAIR_WAYS, ('z', 'y', 'x')),
        fa3=factor_thread(2, 1, LATE_CUTS, BALANCED, LATE_WAYS, ('z', 'x', 'y')),
        fs2=factor_thread(3, 1, LATE_CUTS, BALANCED, LATE_WAYS, ('z', 'x', 'y')),
        sum0=sum_thread(0), sum1=sum_thread(1), sum2=sum_thread(2), sum3=sum_thread(3),
        t3=t_three_thread(),
        grad4=grad_thread(0), grad3=grad_thread(1), grad2=grad_thread(2), grad1=grad_thread(3),
    )
    steps = {name: functools.partial(pump, thread, name) for name, thread in threads.items()}
    steps.update(
        z0=z_one_first, z1=z_one_rest, swap=swap_first, z2=second_forward, back=second_backward,
        A1=functools.partial(gram_job, 0, 0, x_buf), S4=functools.partial(gram_job, 1, 1, dy_buf),
        A3=functools.partial(gram_job, 2, 0, h_two),
        S2a=functools.partial(late_gram, 3, 0, w_two, near_by), S2b=functools.partial(late_gram, 3, 0, w_two, far_off),
        dW4=functools.partial(grad_job, 0, 1, h_three, dy_buf), dW3=functools.partial(grad_job, 1, 0, g_three, h_two),
        dW2a=functools.partial(late_grad, 2, 0, h_one, w_two, near_by), dW2b=functools.partial(late_grad, 2, 0, h_one, w_two, far_off),
        dW1a=functools.partial(late_grad, 3, 1, g_one, x_buf, near_by), dW1b=functools.partial(late_grad, 3, 1, g_one, x_buf, far_off),
    )
    for step in plan(**steps):
        step()
    for name, thread in threads.items():
        drain(thread, name)
    assert len(copies.batches) == N_BATCHES and len(copies.names) == N_COPIES, (len(copies.batches), len(copies.names))


W_TWO_CUTS = (0, 640, 1408, 2048)
W_THREE_CUTS = (0, 640, 1920, 2048)
PAIR_CUTS = (0, 384, 896, 1024)
LATE_CUTS = (0, 512, 640, 1024)
W_TWO_WAYS = ()
W_THREE_WAYS = ()
PAIR_WAYS = (2,)
LATE_WAYS = ()
MOSTLY_X = (('y', 'z', 'x'), ('z', 'y', 'x'), ('x', 'y', 'z'))


def plan(w2, w3, h2, g2, pair, fa3, fs2, sum0, sum1, sum2, sum3, grad4, grad3, grad2, grad1, z0, z1, swap, z2, back, A1, S4, A3, S2a, S2b, dW4, dW3, dW2a, dW2b, dW1a, dW1b, t3):
    return (
        w2, z0, w2, z1, w3, A1, w2, S4, sum0, t3, t3, sum1, w2, sum0, sum1, swap, w2, sum0, sum1, t3, w3, sum0, sum1, pair, w2, w2, w2, w2, t3, w3,
        w2, w3, pair, w2, w2, w3, w2, z2, h2, h2, w3, h2, w3, h2, w3, pair, h2, h2, h2, w3, h2, h2, h2, w3, w3, w3, h2, h2, w3, h2, h2, h2, h2, h2,
        pair, A3, dW4, pair, sum2, back, g2, grad4, dW3, grad3, grad4, g2, sum2, g2, grad3, grad4, sum2, pair, g2, grad4, grad4, g2, grad4, grad3,
        sum2, g2, grad4, pair, g2, grad3, g2, g2, grad3, fa3, g2, grad4, grad3, grad3, g2, g2, pair, dW2a, S2a, pair, g2, g2, dW1a, fa3, pair, g2,
        grad3, g2, g2, S2b, sum3, pair, sum3, fa3, dW2b, grad2, sum3, dW1b, grad1, grad2, fa3, grad1, sum3, grad3, fs2, grad2, fa3, grad1, grad3,
        fs2, fa3, grad2, grad2, fa3, grad2, fa3, grad4, grad1, grad1, grad2, fs2, grad1, fs2, grad1, fa3, fa3, fs2, fa3, fa3, grad2, fs2, fs2, grad1,
        pair, fs2, fs2, fa3, fs2, fs2, grad2, grad4, pair, grad1, fs2, grad2, grad1, fs2,
    )


N_BATCHES = 72
N_COPIES = 168


def step_call(x_tokens, dy_tokens, w_col, w_row, a_old, s_old, a_inv, s_inv, scale):
    f32, bf16 = jnp.float32, jnp.bfloat16
    tall, wide = (WIDTH, BLOCK), (BLOCK, WIDTH)
    cube = (SIDE, SIDE, SIDE, 2)
    rows = 2 * PIECE
    hbm = pl.BlockSpec(memory_space=pl.ANY)
    scratch = [pltpu.VMEM((2,) + tall, bf16), pltpu.VMEM((2,) + wide, bf16)] + [pltpu.VMEM((WIDTH, WIDTH), bf16)] * 2 + [pltpu.VMEM(cube + (PIECE, WIDTH), bf16)] * 3
    scratch += [pltpu.VMEM(tall, bf16)] * 5 + [pltpu.VMEM(wide, bf16)] * 2 + [pltpu.VMEM((2,) + wide, bf16), pltpu.VMEM(wide, bf16)]
    scratch += [pltpu.VMEM((SIDE, SIDE, CORES, PIECE, TRI * BLOCK), f32), pltpu.VMEM((SIDE, SIDE, PIECE, TRI * BLOCK), f32), pltpu.VMEM((4, 3, PIECE, TRI * BLOCK), f32)]
    scratch += [pltpu.VMEM((4, PIECE, TRI * BLOCK), f32), pltpu.VMEM((4, PIECE, FACTOR_COLS), f32)]
    scratch += [pltpu.VMEM((2, SIDE, CORES, PIECE, GRAD_COLS), f32), pltpu.VMEM((SIDE, SIDE, PIECE, GRAD_COLS), f32), pltpu.VMEM((4, 3, PIECE, GRAD_COLS), f32)]
    scratch += [pltpu.VMEM((4, 2, PIECE, GRAD_COLS), f32), pltpu.VMEM((4, rows, HALF + BLOCK), f32), pltpu.VMEM((2, 256, HALF), f32)]
    scratch += [pltpu.SemaphoreType.DMA((num,)) for num in (16, 6, 2, N_BATCHES, N_COPIES)]
    return pl.pallas_call(
        functools.partial(step_kernel, scale),
        out_shape=[jax.ShapeDtypeStruct(cube + (4, PIECE, FACTOR_COLS), f32), jax.ShapeDtypeStruct((4, SIDE, 2, rows, HALF + BLOCK), f32)],
        in_specs=[hbm] * 8,
        out_specs=[hbm, hbm],
        scratch_shapes=scratch,
        compiler_params=pltpu.CompilerParams(collective_id=0, has_side_effects=True, vmem_limit_bytes=67043328),
        name='step',
    )(x_tokens, dy_tokens, w_col, w_row, a_old, s_old, a_inv, s_inv)


def finish_kernel(scale, inv_rows, fact, grads, s_old_col, a_old_row, s_inv_col, a_inv_row, a_new, s_new, u_col, u_row, s_new_col, a_new_row, buf, turned, sums, u_col_buf, u_row_buf, load_sems, out_sems, turn_sems, far_sems, far_out_sems, small_sems):
    mid = PLANE // CORES
    outs = [(a_new, 0), (s_new, 1), (a_new, 1), (s_new, 0)]

    def load(mat, row):
        z, y = lax.div(row, SIDE), lax.rem(row, SIDE)
        return pltpu.make_async_copy(fact.at[z, y, :, :, mat], buf.at[mat, row], load_sems.at[mat * PLANE + row])

    def turn_done(slot):
        ref = turned.at[slot, pl.ds(0, TRI - 2)]
        return pltpu.make_async_copy(ref, ref, turn_sems.at[slot])

    def far_done(row):
        slot = lax.rem(row, CORES)
        ref = turned.at[slot, TRI - 2]
        return pltpu.make_async_copy(ref, ref, far_sems.at[slot])

    def start_load(mat):
        def body(row, carry):
            load(mat, row).start()
            return carry
        lax.fori_loop(0, PLANE, body, 0)

    load_sums = pltpu.make_async_copy(grads, sums, out_sems.at[4])
    load_sums.start()
    for mat in range(SIDE):
        start_load(mat)
    half = HALF

    def new_blocks():
        load_sums.wait()
        for layer in range(SIDE):
            block, num = scale * sums[layer, :, 0, :, half:].reshape(BLOCK, BLOCK), 1 - layer // 2
            if layer % 2 == 1:
                s_new_col[num] = FACTOR_DECAY * s_old_col[num] + block
            else:
                a_new_row[num] = FACTOR_DECAY * a_old_row[num] + block

    def move_small(batch):
        moves = [(u_col_buf, u_col), (u_row_buf, u_row)]
        return [pltpu.make_async_copy(src.at[1 - batch], dst.at[1 - batch], small_sems.at[2 * batch + num]) for num, (src, dst) in enumerate(moves)]

    chunk = 2 * BLOCK

    def small_product(layer, i):
        num = 1 - layer // 2
        core, cols, out = lax.div(i, SIDE), span_of(lax.rem(i, SIDE), chunk), span_of(i, chunk)
        product = sums[layer, :, core, :, cols].reshape(BLOCK, chunk)
        if layer % 2 == 1:
            u_col_buf[num, out, :] = exact_dot(product.T, s_inv_col[num]) * inv_rows
        else:
            u_row_buf[num, :, out] = exact_dot(a_inv_row[num], product) * inv_rows

    for mat, (out, num) in enumerate(outs):
        def row_step(row, carry):
            load(mat, row).wait()
            slot = lax.rem(row, CORES)
            if mat in (1, 2):
                @pl.when(row < mid)
                def _():
                    small_product(2 * mat - 2, row)

                @pl.when(row >= mid)
                def _():
                    small_product(2 * mat - 1, row - mid)
            far = TRI - 1
            def place_block(j, sem):
                cols = span_of(lax.rem(row + j, PLANE), BLOCK)
                pltpu.make_async_copy(buf.at[mat, row, :, :, :, pl.ds(j * BLOCK, BLOCK)], out.at[num, row, :, :, :, cols], sem).start()

            def place_turned(j, sem):
                block = buf[mat, row, :, :, :, j * BLOCK:(j + 1) * BLOCK].reshape(BLOCK, BLOCK).T
                turned[slot, j - 1] = block.reshape(SIDE, CORES, PIECE, BLOCK)
                pltpu.make_async_copy(turned.at[slot, j - 1], out.at[num, lax.rem(row + j, PLANE), :, :, :, span_of(row, BLOCK)], sem).start()

            for j in range(far):
                place_block(j, out_sems.at[mat])
            if mat > 0:
                turn_done(slot).wait()
            else:
                @pl.when(row >= 2)
                def _():
                    turn_done(slot).wait()
            for j in range(1, far):
                place_turned(j, turn_sems.at[slot])

            @pl.when(row < mid)
            def _():
                if mat > 0:
                    far_done(row).wait()
                else:
                    @pl.when(row >= 2)
                    def _():
                        far_done(row).wait()
                place_block(far, far_out_sems.at[mat])
                place_turned(far, far_sems.at[slot])
            return carry

        if mat == 1:
            new_blocks()
        lax.fori_loop(0, PLANE, row_step, 0)
        if mat in (1, 2):
            for move in move_small(mat - 1):
                move.start()
    for batch in range(CORES):
        for move in move_small(batch):
            move.wait()
    for slot in range(CORES):
        turn_done(slot).wait()
        far_done(slot).wait()
    for mat in range(SIDE):
        near, far = buf.at[mat, :, :, :, :, pl.ds(0, mid * BLOCK)], buf.at[mat, pl.ds(0, mid), :, :, :, pl.ds(0, BLOCK)]
        pltpu.make_async_copy(near, near, out_sems.at[mat]).wait()
        pltpu.make_async_copy(far, far, far_out_sems.at[mat]).wait()


def finish_call(fact, grads, s_old_col, a_old_row, s_inv_col, a_inv_row, scale, inv_rows):
    f32 = jnp.float32
    shapes = [(2, PLANE, SIDE, CORES, PIECE, WIDTH)] * 2 + [(2, WIDTH, BLOCK), (2, BLOCK, WIDTH)] + [(2, BLOCK, BLOCK)] * 2
    hbm, vmem = pl.BlockSpec(memory_space=pl.ANY), pl.BlockSpec(memory_space=pltpu.VMEM)
    return pl.pallas_call(
        functools.partial(finish_kernel, scale, inv_rows),
        out_shape=[jax.ShapeDtypeStruct(shape, f32) for shape in shapes],
        in_specs=[hbm] * 2 + [vmem] * 4,
        out_specs=[hbm] * 4 + [vmem] * 2,
        scratch_shapes=[pltpu.VMEM((4, PLANE, SIDE, CORES, PIECE, FACTOR_COLS), f32), pltpu.VMEM((2, TRI - 1, SIDE, CORES, PIECE, BLOCK), f32), pltpu.VMEM(grads.shape, f32), pltpu.VMEM((2, WIDTH, BLOCK), f32), pltpu.VMEM((2, BLOCK, WIDTH), f32)] + [pltpu.SemaphoreType.DMA((num,)) for num in (SIDE * PLANE, 5, CORES, CORES, SIDE, SIDE)],
        compiler_params=pltpu.CompilerParams(vmem_limit_bytes=67043328),
        name='finish',
    )(fact, grads, s_old_col, a_old_row, s_inv_col, a_inv_row)


def solution(mesh):
    def shard_body(x_tokens, dy_tokens, w_col, w_row, a_old_col, s_old_col, a_old_row, s_old_row, a_inv_col, s_inv_col, a_inv_row, s_inv_row):
        inv_rows = 1.0 / (x_tokens.shape[0] * DATA_WAYS)
        scale = (1.0 - FACTOR_DECAY) * inv_rows
        fact, grads = step_call(x_tokens, dy_tokens, w_col, w_row, a_old_col, s_old_row, a_inv_col, s_inv_row, scale)
        a_new_col, s_new_row, u_col, u_row, s_new_col, a_new_row = finish_call(fact, grads, s_old_col, a_old_row, s_inv_col, a_inv_row, scale, inv_rows)
        return (u_col, u_row, a_new_col.reshape(2, WIDTH, WIDTH), s_new_col, a_new_row, s_new_row.reshape(2, WIDTH, WIDTH))

    batch_split = P('data', None)
    col_split = P(None, None, 'model')
    row_split = P(None, 'model', None)
    replicated = P()
    return jax.shard_map(
        shard_body,
        mesh=mesh,
        in_specs=(batch_split, batch_split, col_split, row_split, replicated, row_split, row_split, replicated, replicated, row_split, row_split, replicated),
        out_specs=(col_split, row_split, replicated, row_split, row_split, replicated),
        check_vma=False,
    )
```
